32 devices in a mesh: dp: 1 (over z), col: 4 (over y), row: 8 (over x, core).
Axes of the slice: x: 4, y: 4, z: 1, core: 2. Of those that a mesh axis runs over, the one named last changes fastest.
The devices are a block of a 4x4x8 slice.
Arguments:
- hidden: bfloat16 [64, 4096], P('dp', 'row')
- cache_len: int32 [64], P('dp')
- k_cache: bfloat16 [2, 64, 32, 256, 128], P(None, 'dp', ('col', 'row'))
- v_cache: bfloat16 [2, 64, 32, 256, 128], P(None, 'dp', ('col', 'row'))
- ln1_g: bfloat16 [2, 4096], P(None, 'row')
- ln1_b: bfloat16 [2, 4096], P(None, 'row')
- w_q: bfloat16 [2, 4096, 4096], P(None, 'row', 'col')
- b_q: bfloat16 [2, 4096], P(None, 'col')
- w_k: bfloat16 [2, 4096, 4096], P(None, 'row', 'col')
- b_k: bfloat16 [2, 4096], P(None, 'col')
- w_v: bfloat16 [2, 4096, 4096], P(None, 'row', 'col')
- b_v: bfloat16 [2, 4096], P(None, 'col')
- w_o: bfloat16 [2, 4096, 4096], P(None, 'col', 'row')
- b_o: bfloat16 [2, 4096], P(None, 'row')
- ln2_g: bfloat16 [2, 4096], P(None, 'row')
- ln2_b: bfloat16 [2, 4096], P(None, 'row')
- w_fc1: bfloat16 [2, 4096, 16384], P(None, 'row', 'col')
- b_fc1: bfloat16 [2, 16384], P(None, 'col')
- w_fc2: bfloat16 [2, 16384, 4096], P(None, 'col', 'row')
- b_fc2: bfloat16 [2, 4096], P(None, 'row')
Outputs:
- output 1: bfloat16 [64, 4096], P('dp', 'row')
- output 2: bfloat16 [2, 64, 32, 128], P(None, 'dp', ('col', 'row'))
- output 3: bfloat16 [2, 64, 32, 128], P(None, 'dp', ('col', 'row'))
All inputs are finite; a program needn't handle non-finite values.
Results may differ from the reference program's by a relative error of at most 0.02.
Values are sent between devices in bfloat16 or wider.
A program may use at most 768 MiB of HBM per device.

```python
import jax
import jax.numpy as jnp
from jax import lax

BATCH = 64
D_MODEL = 4096
HEADS = 32
S_MAX = 256
LAYERS = 2
HEAD_DIM = D_MODEL // HEADS
FF_DIM = 4 * D_MODEL
EPS_LN = 1e-5


def setup_inputs(seed: int = 0, part: int = 0) -> dict:
    shared_key = jax.random.key(seed)
    part_key = jax.random.fold_in(shared_key, part)
    part_keys = jax.random.split(part_key, 6)
    weight_keys = jax.random.split(shared_key, 16)

    def normal(rng_key, shape):
        return jax.random.normal(rng_key, shape, jnp.float32)

    def weight(rng_key, shape, fan_in, gain):
        return (gain * fan_in ** -0.5 * normal(rng_key, shape)).astype(jnp.bfloat16)

    def vector(rng_key, shape, center, spread):
        return (center + spread * normal(rng_key, shape)).astype(jnp.bfloat16)

    hidden = normal(part_keys[0], (BATCH, D_MODEL)) + 0.7 * normal(part_keys[1], (BATCH, 1))
    lengths = jax.random.randint(part_keys[2], (BATCH,), 0, S_MAX)
    lengths = lengths.at[0].set(S_MAX - 1).at[1].set(0)
    cache_shape = (LAYERS, BATCH, HEADS, S_MAX, HEAD_DIM)
    k_cache = 1.5 * normal(part_keys[3], cache_shape)
    v_cache = normal(part_keys[4], cache_shape) + 0.8 * normal(part_keys[5], (LAYERS, BATCH, HEADS, 1, HEAD_DIM))
    vec_shape = (LAYERS, D_MODEL)
    square_shape = (LAYERS, D_MODEL, D_MODEL)
    return {
        "hidden": hidden.astype(jnp.bfloat16),
        "cache_len": lengths.astype(jnp.int32),
        "k_cache": k_cache.astype(jnp.bfloat16),
        "v_cache": v_cache.astype(jnp.bfloat16),
        "ln1_g": vector(weight_keys[0], vec_shape, 1.0, 0.3),
        "ln1_b": vector(weight_keys[1], vec_shape, 0.0, 0.3),
        "w_q": weight(weight_keys[2], square_shape, D_MODEL, 1.5),
        "b_q": vector(weight_keys[3], vec_shape, 0.0, 0.5),
        "w_k": weight(weight_keys[4], square_shape, D_MODEL, 1.0),
        "b_k": vector(weight_keys[5], vec_shape, 0.0, 0.5),
        "w_v": weight(weight_keys[6], square_shape, D_MODEL, 1.0),
        "b_v": vector(weight_keys[7], vec_shape, 0.0, 0.5),
        "w_o": weight(weight_keys[8], square_shape, D_MODEL, 1.0),
        "b_o": vector(weight_keys[9], vec_shape, 0.0, 0.3),
        "ln2_g": vector(weight_keys[10], vec_shape, 1.0, 0.3),
        "ln2_b": vector(weight_keys[11], vec_shape, 0.0, 0.3),
        "w_fc1": weight(weight_keys[12], (LAYERS, D_MODEL, FF_DIM), D_MODEL, 1.0),
        "b_fc1": vector(weight_keys[13], (LAYERS, FF_DIM), 0.0, 0.5),
        "w_fc2": weight(weight_keys[14], (LAYERS, FF_DIM, D_MODEL), FF_DIM, 1.0),
        "b_fc2": vector(weight_keys[15], vec_shape, 0.0, 0.3),
    }


def layer_norm(state, gain, shift):
    state_f32 = state.astype(jnp.float32)
    mean_val = jnp.sum(state_f32, axis=-1, keepdims=True) / D_MODEL
    mean_sq = jnp.sum(state_f32 * state_f32, axis=-1, keepdims=True) / D_MODEL
    variance = mean_sq - mean_val * mean_val
    normed = (state_f32 - mean_val) * lax.rsqrt(variance + EPS_LN) * gain.astype(jnp.float32) + shift.astype(jnp.float32)
    return normed.astype(jnp.bfloat16)


def project(normed, weight, bias):
    return jnp.dot(normed, weight, preferred_element_type=jnp.float32) + bias.astype(jnp.float32)


def attend_row(row_args):
    q_row, k_row, v_row, k_fresh, v_fresh, length = row_args
    positions = jnp.arange(S_MAX)
    at_new = (positions == length)[None, :, None]
    keys_all = jnp.where(at_new, k_fresh[:, None, :], k_row)
    values_all = jnp.where(at_new, v_fresh[:, None, :], v_row)
    scores = jnp.einsum("hd,hsd->hs", q_row.astype(jnp.float32), keys_all.astype(jnp.float32))
    scores = jnp.where((positions <= length)[None, :], scores, -jnp.inf)
    probs = jax.nn.softmax(scores, axis=-1).astype(jnp.bfloat16)
    mixed = jnp.einsum("hs,hsd->hd", probs.astype(jnp.float32), values_all.astype(jnp.float32))
    return mixed.astype(jnp.bfloat16)


def reference(hidden, cache_len, k_cache, v_cache, ln1_g, ln1_b, w_q, b_q, w_k, b_k, w_v, b_v, w_o, b_o, ln2_g, ln2_b, w_fc1, b_fc1, w_fc2, b_fc2):
    scale = HEAD_DIM ** -0.5

    def layer_step(state, layer_args):
        (k_layer, v_layer, gain_one, shift_one, wq_layer, bq_layer, wk_layer, bk_layer, wv_layer, bv_layer,
         wo_layer, bo_layer, gain_two, shift_two, fc1_layer, bfc1_layer, fc2_layer, bfc2_layer) = layer_args
        normed = layer_norm(state, gain_one, shift_one)
        q_all = (project(normed, wq_layer, bq_layer) * scale).astype(jnp.bfloat16).reshape(BATCH, HEADS, HEAD_DIM)
        k_all = project(normed, wk_layer, bk_layer).astype(jnp.bfloat16).reshape(BATCH, HEADS, HEAD_DIM)
        v_all = project(normed, wv_layer, bv_layer).astype(jnp.bfloat16).reshape(BATCH, HEADS, HEAD_DIM)
        attended = lax.map(attend_row, (q_all, k_layer, v_layer, k_all, v_all, cache_len))
        state_mid = (state.astype(jnp.float32) + project(attended.reshape(BATCH, D_MODEL), wo_layer, bo_layer)).astype(jnp.bfloat16)
        normed_two = layer_norm(state_mid, gain_two, shift_two)
        inner = jnp.maximum(project(normed_two, fc1_layer, bfc1_layer).astype(jnp.bfloat16), 0)
        state_out = (state_mid.astype(jnp.float32) + project(inner, fc2_layer, bfc2_layer)).astype(jnp.bfloat16)
        return state_out, (k_all, v_all)

    layer_inputs = (k_cache, v_cache, ln1_g, ln1_b, w_q, b_q, w_k, b_k, w_v, b_v, w_o, b_o, ln2_g, ln2_b, w_fc1, b_fc1, w_fc2, b_fc2)
    state_final, fresh_rows = lax.scan(layer_step, hidden, layer_inputs)
    return state_final, fresh_rows[0], fresh_rows[1]
```

```python
import functools

import jax
import jax.numpy as jnp
from jax import lax
from jax.experimental import pallas as pl
from jax.experimental.pallas import tpu as pltpu
from jax.sharding import PartitionSpec as P

EPS_LN = 1e-5
MESH = pl.DeviceIdType.MESH
F32 = jnp.float32
BF16 = jnp.bfloat16


class Sems:
    def __init__(self):
        self.count = 0

    def take(self, n):
        base = self.count
        self.count += n
        return base


def layout(n_chip, n_row, n_col):
    sems = Sems()
    names = dict(st1=n_row, st2=n_row, qd=3 * n_chip, qi=3 * n_chip, ag=n_row, wo=n_col,
                 fd=n_chip, fi=n_chip, ug=n_row, fo=n_col)
    table = {name: sems.take(n) for name, n in names.items()}
    return table, sems.count


def kernel(dims, hid_hbm, len_hbm, kc_hbm, vc_hbm, g1_hbm, b1_hbm, wq_hbm, bq_hbm, wk_hbm, bk_hbm, wv_hbm, bv_hbm,
           wo_hbm, bo_hbm, g2_hbm, b2_hbm, w1_hbm, bf1_hbm, w2_hbm, bf2_hbm,
           h_out, k_out, v_out,
           hid_v, len_v, kc, vc, g1, b1, wq, bq, wk, bk, wv, bv, wo, bo, g2, b2, w1, bf1, w2, bf2,
           state, st_send, st_recv, qd_send, qd_recv, q_mine, qi_send, qi_recv, ag_send, ag_recv, wo_recv,
           fd_send, fd_recv, f_mine, fi_send, fi_recv, ug_recv, fo_recv,
           small_sem, big_sem, ssem, rsem):
    n_layer, n_row, n_col, table = dims
    n_chip = n_row // 2
    row = lax.axis_index("row")
    col = lax.axis_index("col")
    chip = row // 2
    par = row % 2
    partner = row + 1 - 2 * par
    batch, width = hid_v.shape
    full = width * n_row
    hd = kc.shape[-1]
    keys = kc.shape[2]
    ffb = fd_send.shape[-1]
    offs = [2, 1, 3, 0]

    small = [(hid_hbm, hid_v), (len_hbm, len_v), (g1_hbm, g1), (b1_hbm, b1), (bq_hbm, bq), (bk_hbm, bk),
             (bv_hbm, bv), (bo_hbm, bo), (g2_hbm, g2), (b2_hbm, b2), (bf1_hbm, bf1), (bf2_hbm, bf2)]
    small_copies = [pltpu.make_async_copy(s, d, small_sem.at[i]) for i, (s, d) in enumerate(small)]
    for c in small_copies:
        c.start()

    bigs = [(wq_hbm, wq), (wk_hbm, wk), (wv_hbm, wv), (kc_hbm, kc), (vc_hbm, vc), (wo_hbm, wo), (w1_hbm, w1),
            (w2_hbm, w2)]
    WQ, WK, WV, KC, VC, WO, W1, W2 = range(8)

    def big_copy(i, l):
        s, d = bigs[i]
        src = s.at[l, :, 0] if i in (KC, VC) else s.at[l]
        return pltpu.make_async_copy(src, d.at[l], big_sem.at[l, i])

    for l in range(n_layer):
        for i in range(8):
            big_copy(i, l).start()

    barrier = pltpu.get_barrier_semaphore()
    for t in range(1, n_row):
        pl.semaphore_signal(barrier, inc=1, device_id={"row": lax.rem(row + t, n_row)}, device_id_type=MESH)
    for t in range(1, n_col):
        pl.semaphore_signal(barrier, inc=1, device_id={"col": lax.rem(col + t, n_col)}, device_id_type=MESH)
    for c in small_copies:
        c.wait()
    state[...] = hid_v[...]
    pl.semaphore_wait(barrier, n_row - 1 + n_col - 1)

    def remote(l, name, i_send, i_recv, src, dst, axis, target):
        return pltpu.make_async_remote_copy(
            src_ref=src, dst_ref=dst, send_sem=ssem.at[l, table[name] + i_send], recv_sem=rsem.at[l, table[name] + i_recv],
            device_id={axis: target}, device_id_type=MESH)

    def pick(ref, l):
        rows = ref[...].astype(F32)
        out = rows[0:1]
        for i in range(1, n_layer):
            out = jnp.where(l == i, rows[i:i + 1], out)
        return out

    def pick_slice(ref, l, start, size):
        rows = ref[:, pl.ds(pl.multiple_of(start, size), size)].astype(F32)
        out = rows[0:1]
        for i in range(1, n_layer):
            out = jnp.where(l == i, rows[i:i + 1], out)
        return out

    eye = lax.broadcasted_iota(jnp.int32, (batch, 128), 0) == lax.broadcasted_iota(jnp.int32, (batch, 128), 1)
    lens = jnp.sum(jnp.where(eye, jnp.pad(len_v[...], ((0, 0), (0, 128 - batch))), 0), axis=1, keepdims=True)

    row_order = []
    for off in offs[:-1]:
        k = lax.rem(chip + off, n_chip)
        row_order += [2 * k + par, 2 * k + 1 - par]
    row_order.append(partner)

    def layer_norm(l, name, which, gain, shift):
        x = state[...].astype(F32)
        s1 = jnp.sum(x, axis=1, keepdims=True)
        s2 = jnp.sum(x * x, axis=1, keepdims=True)
        r1 = jnp.sum(jnp.where(eye, s1, 0.0), axis=0, keepdims=True)
        r2 = jnp.sum(jnp.where(eye, s2, 0.0), axis=0, keepdims=True)
        sub = lax.broadcasted_iota(jnp.int32, (8, 128), 0)
        tile = jnp.where(sub == 0, r1, jnp.where(sub == 1, r2, 0.0))
        st_send[l, which] = tile
        st_recv[l, which, row] = tile
        for t, j in enumerate(row_order):
            remote(l, name, t, row, st_send.at[l, which], st_recv.at[l, which, row], "row", j).start()
        for t, j in enumerate(row_order):
            remote(l, name, t, j, st_send.at[l, which], st_recv.at[l, which, j], "row", j).wait_recv()
        tot = jnp.sum(st_recv[l, which], axis=0)
        m = jnp.sum(jnp.where(eye, tot[0:1], 0.0), axis=1, keepdims=True) / full
        var = jnp.sum(jnp.where(eye, tot[1:2], 0.0), axis=1, keepdims=True) / full - m * m
        y = (x - m) * lax.rsqrt(var + EPS_LN) * pick(gain, l) + pick(shift, l)
        return y.astype(BF16)

    def ar_col(l, name, part, buf, bias):
        buf[l, col] = part.astype(BF16)
        for t in (2, 1, 3):
            j = lax.rem(col + t, n_col)
            remote(l, name, t, col, buf.at[l, col], buf.at[l, col], "col", j).start()
        for t in (1, 3, 2):
            j = lax.rem(col + t, n_col)
            remote(l, name, t, j, buf.at[l, col], buf.at[l, j], "col", j).wait_recv()
        total = buf[l, 0].astype(F32)
        for j in range(1, n_col):
            total = total + buf[l, j].astype(F32)
        state[...] = (state[...].astype(F32) + (total + bias)).astype(BF16)

    def layer(l, carry):
        y = layer_norm(l, "st1", 0, g1, b1)

        def project(w, i_big, wref):
            big_copy(i_big, l).wait()
            for off in offs:
                k = lax.rem(chip + off, n_chip)
                res = jnp.dot(y, wref[l, :, pl.ds(pl.multiple_of(k * 2 * hd, 2 * hd), 2 * hd)],
                              preferred_element_type=F32)
                lo, hi = res[:, :hd], res[:, hd:]
                qd_send[l, w, k] = jnp.where(par == 0, hi, lo).astype(BF16)
                q_mine[w, k] = jnp.where(par == 0, lo, hi)
                remote(l, "qd", w * n_chip + k, w * n_chip + k, qd_send.at[l, w, k], qd_recv.at[l, w, k],
                       "row", partner).start()

        def forward(w):
            for off in offs:
                k = lax.rem(chip + off, n_chip)
                remote(l, "qd", w * n_chip + k, w * n_chip + k, qd_send.at[l, w, k], qd_recv.at[l, w, k],
                       "row", partner).wait_recv()
                both = q_mine[w, k] + qd_recv[l, w, k].astype(F32)
                if off:
                    qi_send[l, w, k] = both.astype(BF16)
                    remote(l, "qi", w * n_chip + k, w * n_chip + chip, qi_send.at[l, w, k], qi_recv.at[l, w, chip],
                           "row", 2 * k + par).start()
                else:
                    q_mine[w, k] = both

        def collect(w, bias):
            total = q_mine[w, chip]
            for off in (1, 3, 2):
                k = lax.rem(chip + off, n_chip)
                remote(l, "qi", w * n_chip + k, w * n_chip + k, qi_send.at[l, w, k], qi_recv.at[l, w, k],
                       "row", 2 * k + par).wait_recv()
                total = total + qi_recv[l, w, k].astype(F32)
            return total + pick_slice(bias, l, row * hd, hd)

        project(0, WQ, wq)
        project(1, WK, wk)
        forward(0)
        project(2, WV, wv)
        forward(1)
        forward(2)
        q = (collect(0, bq) * (hd ** -0.5)).astype(BF16).astype(F32)

        group = 16
        rowi = lax.broadcasted_iota(jnp.int32, (group, 1), 0)
        big_copy(KC, l).wait()
        parts = []
        for g in range(batch // group):
            q_g = q[g * group:(g + 1) * group]
            lhs = jnp.concatenate([jnp.where(rowi == i, q_g, 0.0) for i in range(group)], axis=1).astype(BF16)
            k_g = jnp.concatenate([kc[l, g * group + i] for i in range(group)], axis=1)
            parts.append(lax.dot_general(lhs, k_g, (((1,), (1,)), ((), ())), preferred_element_type=F32))
        scores = jnp.concatenate(parts, axis=0)
        scores = jnp.where(lax.broadcasted_iota(jnp.int32, (batch, keys), 1) < lens, scores, -jnp.inf)
        k_new = collect(1, bk).astype(BF16)
        k_out[l] = k_new
        s_new = jnp.sum(q * k_new.astype(F32), axis=1, keepdims=True)
        peak = jnp.maximum(jnp.max(scores, axis=1, keepdims=True), s_new)
        e = jnp.exp(scores - peak)
        e_new = jnp.exp(s_new - peak)
        mass = jnp.sum(e, axis=1, keepdims=True) + e_new
        prob = (e / mass).astype(BF16).astype(F32)
        prob_new = (e_new / mass).astype(BF16).astype(F32)
        big_copy(VC, l).wait()
        outs = []
        for g in range(batch // group):
            p_g = prob[g * group:(g + 1) * group]
            lhs = jnp.concatenate([jnp.where(rowi // 2 == i, p_g, 0.0) for i in range(group // 2)],
                                  axis=1).astype(BF16)
            v_g = jnp.concatenate([jnp.concatenate([vc[l, g * group + 2 * i], vc[l, g * group + 2 * i + 1]], axis=1)
                                   for i in range(group // 2)], axis=0)
            out = jnp.dot(lhs, v_g, preferred_element_type=F32)
            outs.append(jnp.where(rowi % 2 == 0, out[:, :hd], out[:, hd:]))
        v_new = collect(2, bv).astype(BF16)
        v_out[l] = v_new
        mixed = jnp.concatenate(outs, axis=0) + prob_new * v_new.astype(F32)

        ag_recv[l, row] = mixed.astype(BF16)
        for t, j in enumerate(row_order):
            remote(l, "ag", t, row, ag_recv.at[l, row], ag_recv.at[l, row], "row", j).start()
        big_copy(WO, l).wait()
        for t, j in enumerate(row_order):
            remote(l, "ag", t, j, ag_recv.at[l, row], ag_recv.at[l, j], "row", j).wait_recv()
        gathered = jnp.concatenate([ag_recv[l, j] for j in range(n_row)], axis=1)
        ar_col(l, "wo", jnp.dot(gathered, wo[l], preferred_element_type=F32), wo_recv, pick(bo, l))

        y2 = layer_norm(l, "st2", 1, g2, b2)
        big_copy(W1, l).wait()

        def fc1_block(j):
            return jnp.dot(y2, w1[l, :, pl.ds(pl.multiple_of(j * ffb, ffb), ffb)], preferred_element_type=F32)

        for off in offs:
            k = lax.rem(chip + off, n_chip)
            fd_send[l, k] = fc1_block(2 * k + 1 - par).astype(BF16)
            remote(l, "fd", k, k, fd_send.at[l, k], fd_recv.at[l, k], "row", partner).start()
        for off in offs:
            k = lax.rem(chip + off, n_chip)
            f_mine[k] = fc1_block(2 * k + par)
        for off in offs:
            k = lax.rem(chip + off, n_chip)
            remote(l, "fd", k, k, fd_send.at[l, k], fd_recv.at[l, k], "row", partner).wait_recv()
            both = f_mine[k] + fd_recv[l, k].astype(F32)
            if off:
                fi_send[l, k] = both.astype(BF16)
                remote(l, "fi", k, chip, fi_send.at[l, k], fi_recv.at[l, chip], "row", 2 * k + par).start()
            else:
                f_mine[k] = both
        total = f_mine[chip]
        for off in (1, 3, 2):
            k = lax.rem(chip + off, n_chip)
            remote(l, "fi", k, k, fi_send.at[l, k], fi_recv.at[l, k], "row", 2 * k + par).wait_recv()
            total = total + fi_recv[l, k].astype(F32)
        u = jnp.maximum((total + pick_slice(bf1, l, row * ffb, ffb)).astype(BF16), 0)

        ug_recv[l, row] = u
        for off in offs[:-1]:
            k = lax.rem(chip + off, n_chip)
            remote(l, "ug", 2 * k + par, row, ug_recv.at[l, row], ug_recv.at[l, row], "row", 2 * k + par).start()
        remote(l, "ug", row, row, ug_recv.at[l, row], ug_recv.at[l, row], "row", partner).start()
        big_copy(W2, l).wait()

        def fc2_block(j, u_j):
            return jnp.dot(u_j, w2[l, pl.ds(pl.multiple_of(j * ffb, ffb), ffb), :], preferred_element_type=F32)

        acc = fc2_block(row, u)

        def got(j, target):
            remote(l, "ug", j, j, ug_recv.at[l, row], ug_recv.at[l, j], "row", target).wait_recv()

        got(partner, partner)
        acc = acc + fc2_block(partner, ug_recv[l, partner])
        for off in (1, 3, 2):
            k = lax.rem(chip + off, n_chip)
            j = 2 * k + par
            got(j, j)
            remote(l, "ug", 2 * k + 1 - par, j, ug_recv.at[l, j], ug_recv.at[l, j], "row", partner).start()
            acc = acc + fc2_block(j, ug_recv[l, j])
        for off in (1, 3, 2):
            k = lax.rem(chip + off, n_chip)
            j = 2 * k + 1 - par
            got(j, partner)
            acc = acc + fc2_block(j, ug_recv[l, j])
        ar_col(l, "fo", acc, fo_recv, pick(bf2, l))
        return carry

    lax.fori_loop(0, n_layer, layer, 0)
    h_out[...] = state[...]

    def drain(l, carry):
        def done(name, i, src, axis, target):
            remote(l, name, i, i, src, src, axis, target).wait_send()

        for t, j in enumerate(row_order):
            done("st1", t, st_send.at[l, 0], "row", j)
            done("st2", t, st_send.at[l, 1], "row", j)
            done("ag", t, ag_recv.at[l, row], "row", j)
        for t in (1, 2, 3):
            j = lax.rem(col + t, n_col)
            done("wo", t, wo_recv.at[l, col], "col", j)
            done("fo", t, fo_recv.at[l, col], "col", j)
        for off in offs:
            k = lax.rem(chip + off, n_chip)
            for w in range(3):
                done("qd", w * n_chip + k, qd_send.at[l, w, k], "row", partner)
                if off:
                    done("qi", w * n_chip + k, qi_send.at[l, w, k], "row", 2 * k + par)
            done("fd", k, fd_send.at[l, k], "row", partner)
            if off:
                done("fi", k, fi_send.at[l, k], "row", 2 * k + par)
                done("ug", 2 * k + par, ug_recv.at[l, row], "row", 2 * k + par)
                done("ug", 2 * k + 1 - par, ug_recv.at[l, 2 * k + par], "row", partner)
            else:
                done("ug", row, ug_recv.at[l, row], "row", partner)
        return carry

    lax.fori_loop(0, n_layer, drain, 0)


def solution(mesh):
    n_row, n_col = mesh.shape["row"], mesh.shape["col"]
    n_chip = n_row // 2
    act_spec = P("dp", "row")
    cache_spec = P(None, "dp", ("col", "row"), None, None)
    fresh_spec = P(None, "dp", ("col", "row"), None)
    in_weight = P(None, "row", "col")
    out_weight = P(None, "col", "row")
    col_vec = P(None, "col")
    row_vec = P(None, "row")
    in_specs = (act_spec, P("dp"), cache_spec, cache_spec, row_vec, row_vec,
                in_weight, col_vec, in_weight, col_vec, in_weight, col_vec,
                out_weight, row_vec, row_vec, row_vec, in_weight, col_vec, out_weight, row_vec)

    def local_step(hidden, cache_len, k_cache, v_cache, ln1_g, ln1_b, w_q, b_q, w_k, b_k, w_v, b_v,
                   w_o, b_o, ln2_g, ln2_b, w_fc1, b_fc1, w_fc2, b_fc2):
        batch, width = hidden.shape
        n_layer, _, _, keys, hd = k_cache.shape
        ff = w_fc1.shape[2]
        ffb = ff // n_row
        table, n_sem = layout(n_chip, n_row, n_col)
        args = (hidden, cache_len.reshape(1, batch), k_cache, v_cache, ln1_g, ln1_b, w_q, b_q, w_k, b_k, w_v, b_v,
                w_o, b_o, ln2_g, ln2_b, w_fc1, b_fc1, w_fc2, b_fc2)

        def vm(shape, dtype=BF16):
            return pltpu.VMEM(shape, dtype)

        local = [vm(a.shape, a.dtype) for a in args]
        local[2] = local[3] = vm((n_layer, batch, keys, hd))
        scratch = local + [
            vm((batch, width)),
            vm((n_layer, 2, 8, 128), F32), vm((n_layer, 2, n_row, 8, 128), F32),
            vm((n_layer, 3, n_chip, batch, hd)), vm((n_layer, 3, n_chip, batch, hd)),
            vm((3, n_chip, batch, hd), F32),
            vm((n_layer, 3, n_chip, batch, hd)), vm((n_layer, 3, n_chip, batch, hd)),
            vm((8, 128)), vm((n_layer, n_row, batch, hd)),
            vm((n_layer, n_col, batch, width)),
            vm((n_layer, n_chip, batch, ffb)), vm((n_layer, n_chip, batch, ffb)), vm((n_chip, batch, ffb), F32),
            vm((n_layer, n_chip, batch, ffb)), vm((n_layer, n_chip, batch, ffb)),
            vm((n_layer, n_row, batch, ffb)),
            vm((n_layer, n_col, batch, width)),
            pltpu.SemaphoreType.DMA((12,)), pltpu.SemaphoreType.DMA((n_layer, 8)),
            pltpu.SemaphoreType.DMA((n_layer, n_sem)), pltpu.SemaphoreType.DMA((n_layer, n_sem)),
        ]
        out_shape = (jax.ShapeDtypeStruct((batch, width), BF16),
                     jax.ShapeDtypeStruct((n_layer, batch, hd), BF16),
                     jax.ShapeDtypeStruct((n_layer, batch, hd), BF16))
        h_out, k_new, v_new = pl.pallas_call(
            functools.partial(kernel, (n_layer, n_row, n_col, table)),
            out_shape=out_shape,
            in_specs=[pl.BlockSpec(memory_space=pl.ANY)] * len(args),
            out_specs=[pl.BlockSpec(memory_space=pltpu.VMEM)] * 3,
            scratch_shapes=scratch,
            compiler_params=pltpu.CompilerParams(collective_id=0, has_side_effects=True,
                                                 vmem_limit_bytes=66 * 1000 * 1000),
        )(*args)
        return h_out, k_new[:, :, None, :], v_new[:, :, None, :]

    return jax.shard_map(local_step, mesh=mesh, in_specs=in_specs,
                         out_specs=(act_spec, fresh_spec, fresh_spec), check_vma=False)
```

```python
import functools

import jax
import jax.numpy as jnp
from jax import lax
from jax.experimental import pallas as pl
from jax.experimental.pallas import tpu as pltpu
from jax.sharding import PartitionSpec as P

EPS_LN = 1e-5
MESH = pl.DeviceIdType.MESH
F32 = jnp.float32
BF16 = jnp.bfloat16


class Sems:
    def __init__(self):
        self.count = 0

    def take(self, n):
        base = self.count
        self.count += n
        return base


def layout(n_chip, n_row, n_col):
    sems = Sems()
    names = dict(st1=n_row, st2=n_row, qd=3, qi=3 * n_chip, ag=n_row, wo=n_col,
                 fd=n_chip, fi=n_chip, ug=n_row, fo=n_col)
    table = {name: sems.take(n) for name, n in names.items()}
    return table, sems.count


def kernel(dims, hid_hbm, len_hbm, kc_hbm, vc_hbm, g1_hbm, b1_hbm, wq_hbm, bq_hbm, wk_hbm, bk_hbm, wv_hbm, bv_hbm,
           wo_hbm, bo_hbm, g2_hbm, b2_hbm, w1_hbm, bf1_hbm, w2_hbm, bf2_hbm,
           h_out, k_out, v_out,
           hid_v, len_v, kc, vc, g1, b1, wq, bq, wk, bk, wv, bv, wo, bo, g2, b2, w1, bf1, w2, bf2,
           state, st_send, st_recv, qd_send, qd_recv, q_mine, q_own, qi_send, qi_recv, k_stage, v_stage, ag_recv, wo_recv,
           fd_send, fd_recv, f_mine, f_own, fi_send, fi_recv, ug_recv, fo_recv,
           small_sem, big_sem, out_sem, ssem, rsem):
    n_layer, n_row, n_col, table = dims
    n_chip = n_row // 2
    row = lax.axis_index("row")
    col = lax.axis_index("col")
    chip = row // 2
    par = row % 2
    partner = row + 1 - 2 * par
    batch, width = hid_v.shape
    hd = kc.shape[-1]
    keys = kc.shape[2]
    ffb = fd_send.shape[-1]
    offs = [2, 1, 3, 0]

    small = [(hid_hbm, hid_v), (len_hbm, len_v), (g1_hbm, g1), (b1_hbm, b1), (bq_hbm, bq), (bk_hbm, bk),
             (bv_hbm, bv), (bo_hbm, bo), (g2_hbm, g2), (b2_hbm, b2), (bf1_hbm, bf1), (bf2_hbm, bf2)]
    small_copies = [pltpu.make_async_copy(s, d, small_sem.at[i]) for i, (s, d) in enumerate(small)]
    for c in small_copies:
        c.start()

    bigs = [(wq_hbm, wq), (wk_hbm, wk), (wv_hbm, wv), (kc_hbm, kc), (vc_hbm, vc), (wo_hbm, wo), (w1_hbm, w1),
            (w2_hbm, w2)]
    WQ, WK, WV, KC, VC, WO, W1, W2 = range(8)

    def big_copy(i, l):
        s, d = bigs[i]
        src = s.at[l, :, 0] if i in (KC, VC) else s.at[l]
        return pltpu.make_async_copy(src, d.at[l], big_sem.at[l, i])

    for i in (WQ, WK, WV):
        big_copy(i, 0).start()

    barrier = pltpu.get_barrier_semaphore()
    for t in range(1, n_row):
        pl.semaphore_signal(barrier, inc=1, device_id={"row": lax.rem(row + t, n_row)}, device_id_type=MESH)
    for t in range(1, n_col):
        pl.semaphore_signal(barrier, inc=1, device_id={"col": lax.rem(col + t, n_col)}, device_id_type=MESH)
    for c in small_copies:
        c.wait()
    state[...] = hid_v[...]
    for i in (KC, VC, WO, W1, W2):
        big_copy(i, 0).start()
    for l in range(1, n_layer):
        for i in range(8):
            big_copy(i, l).start()
    pl.semaphore_wait(barrier, n_row - 1 + n_col - 1)

    def remote(l, name, i_send, i_recv, src, dst, axis, target):
        return pltpu.make_async_remote_copy(
            src_ref=src, dst_ref=dst, send_sem=ssem.at[l, table[name] + i_send], recv_sem=rsem.at[l, table[name] + i_recv],
            device_id={axis: target}, device_id_type=MESH)

    def pick(ref, l):
        rows = ref[...].astype(F32)
        out = rows[0:1]
        for i in range(1, n_layer):
            out = jnp.where(l == i, rows[i:i + 1], out)
        return out

    def pick_slice(ref, l, start, size):
        rows = ref[:, pl.ds(pl.multiple_of(start, size), size)].astype(F32)
        out = rows[0:1]
        for i in range(1, n_layer):
            out = jnp.where(l == i, rows[i:i + 1], out)
        return out

    eye = lax.broadcasted_iota(jnp.int32, (batch, 128), 0) == lax.broadcasted_iota(jnp.int32, (batch, 128), 1)
    lens = jnp.sum(jnp.where(eye, jnp.pad(len_v[...], ((0, 0), (0, 128 - batch))), 0), axis=1, keepdims=True)

    row_order = []
    for off in offs[:-1]:
        k = lax.rem(chip + off, n_chip)
        row_order += [2 * k + par, 2 * k + 1 - par]
    row_order.append(partner)

    def to_row(column):
        return jnp.sum(jnp.where(eye, column, 0.0), axis=0, keepdims=True)

    def to_column(line):
        return jnp.sum(jnp.where(eye, line, 0.0), axis=1, keepdims=True)

    def local_norm(l, name, which, gain, shift):
        x = state[...].astype(F32)
        c = jnp.sum(x, axis=1, keepdims=True) / width
        xc = x - c
        v = jnp.sum(xc * xc, axis=1, keepdims=True) / width
        sub = lax.broadcasted_iota(jnp.int32, (8, 128), 0)
        tile = jnp.where(sub == 0, to_row(c), jnp.where(sub == 1, to_row(v), 0.0))
        st_send[l, which] = tile
        st_recv[l, which, row] = tile
        for t, j in enumerate(row_order):
            remote(l, name, t, row, st_send.at[l, which], st_recv.at[l, which, row], "row", j).start()
        g, b = pick(gain, l), pick(shift, l)
        y = xc * lax.rsqrt(v + EPS_LN) * g
        extra = lax.broadcasted_iota(jnp.int32, (16, 1), 0)
        extra = jnp.where(extra == 0, g, jnp.where(extra == 1, b, 0.0))
        return jnp.concatenate([y.astype(BF16), extra.astype(BF16)], axis=0)

    def global_norm(l, name, which):
        for t, j in enumerate(row_order):
            remote(l, name, t, j, st_send.at[l, which], st_recv.at[l, which, j], "row", j).wait_recv()
        m = jnp.zeros((1, 128), F32)
        for j in range(n_row):
            m = m + st_recv[l, which, j][0:1]
        m = m / n_row
        var = jnp.zeros((1, 128), F32)
        for j in range(n_row):
            tile = st_recv[l, which, j]
            var = var + (tile[1:2] + (tile[0:1] - m) * (tile[0:1] - m))
        r = lax.rsqrt(var / n_row + EPS_LN)

        def coefficients(tile):
            local = tile[1:2] + EPS_LN
            return to_column(r * (local * lax.rsqrt(local))), to_column(r * (tile[0:1] - m))

        mine = coefficients(st_recv[l, which, row])
        other = coefficients(st_recv[l, which, partner])

        def combine(own, got):
            got = got.astype(F32)
            return ((mine[0] * own[:batch] + other[0] * got[:batch])
                    + (mine[1] * own[batch:batch + 1] + other[1] * got[batch:batch + 1])
                    + (own[batch + 1:batch + 2] + got[batch + 1:batch + 2]))

        return combine

    def ar_col(l, name, part, buf, bias):
        buf[l, col] = part.astype(BF16)
        for t in (2, 1, 3):
            j = lax.rem(col + t, n_col)
            remote(l, name, t, col, buf.at[l, col], buf.at[l, col], "col", j).start()
        for t in (1, 3, 2):
            j = lax.rem(col + t, n_col)
            remote(l, name, t, j, buf.at[l, col], buf.at[l, j], "col", j).wait_recv()
        total = buf[l, 0].astype(F32)
        for j in range(1, n_col):
            total = total + buf[l, j].astype(F32)
        state[...] = (state[...].astype(F32) + (total + bias)).astype(BF16)

    def layer(l, carry):
        y = local_norm(l, "st1", 0, g1, b1)

        def pair(w):
            return remote(l, "qd", w, w, qd_send.at[l, w], qd_recv.at[l, w], "row", partner)

        def project(w, i_big, wref):
            big_copy(i_big, l).wait()
            res = jnp.dot(y, wref[l], preferred_element_type=F32)
            even = jnp.concatenate([res[:, 2 * k * hd:(2 * k + 1) * hd] for k in range(n_chip)], axis=1)
            odd = jnp.concatenate([res[:, (2 * k + 1) * hd:(2 * k + 2) * hd] for k in range(n_chip)], axis=1)
            qd_send[l, w] = jnp.where(par == 0, odd, even).astype(BF16)
            pair(w).start()
            q_mine[w] = jnp.where(par == 0, even, odd)

        def forward(w):
            pair(w).wait_recv()
            both = combine(q_mine[w], qd_recv[l, w])
            own = both[:, :hd]
            for k in range(n_chip):
                block = both[:, k * hd:(k + 1) * hd]
                own = jnp.where(chip == k, block, own)
                qi_send[l, w, k] = block.astype(BF16)
            for off in offs[:-1]:
                k = lax.rem(chip + off, n_chip)
                remote(l, "qi", w * n_chip + k, w * n_chip + chip, qi_send.at[l, w, k], qi_recv.at[l, w, chip],
                       "row", 2 * k + par).start()
            q_own[w] = own

        def collect(w, bias):
            total = q_own[w]
            for off in (1, 3, 2):
                k = lax.rem(chip + off, n_chip)
                remote(l, "qi", w * n_chip + k, w * n_chip + k, qi_send.at[l, w, k], qi_recv.at[l, w, k],
                       "row", 2 * k + par).wait_recv()
                total = total + qi_recv[l, w, k].astype(F32)
            return total + pick_slice(bias, l, row * hd, hd)

        project(0, WQ, wq)
        project(1, WK, wk)
        project(2, WV, wv)
        combine = global_norm(l, "st1", 0)
        forward(0)
        forward(1)
        forward(2)
        q = (collect(0, bq) * (hd ** -0.5)).astype(BF16).astype(F32)

        group = 16
        rowi = lax.broadcasted_iota(jnp.int32, (group, 1), 0)
        big_copy(KC, l).wait()
        parts = []
        for g in range(batch // group):
            q_g = q[g * group:(g + 1) * group]
            lhs = jnp.concatenate([jnp.where(rowi == i, q_g, 0.0) for i in range(group)], axis=1).astype(BF16)
            k_g = jnp.concatenate([kc[l, g * group + i] for i in range(group)], axis=1)
            parts.append(lax.dot_general(lhs, k_g, (((1,), (1,)), ((), ())), preferred_element_type=F32))
        scores = jnp.concatenate(parts, axis=0)
        scores = jnp.where(lax.broadcasted_iota(jnp.int32, (batch, keys), 1) < lens, scores, -jnp.inf)
        k_new = collect(1, bk).astype(BF16)
        k_stage[l] = k_new
        pltpu.make_async_copy(k_stage.at[l], k_out.at[l], out_sem.at[l, 0]).start()
        s_new = jnp.sum(q * k_new.astype(F32), axis=1, keepdims=True)
        peak = jnp.maximum(jnp.max(scores, axis=1, keepdims=True), s_new)
        e = jnp.exp(scores - peak)
        e_new = jnp.exp(s_new - peak)
        mass = jnp.sum(e, axis=1, keepdims=True) + e_new
        prob = (e / mass).astype(BF16).astype(F32)
        prob_new = (e_new / mass).astype(BF16).astype(F32)
        big_copy(VC, l).wait()
        outs = []
        for g in range(batch // group):
            p_g = prob[g * group:(g + 1) * group]
            lhs = jnp.concatenate([jnp.where(rowi // 2 == i, p_g, 0.0) for i in range(group // 2)],
                                  axis=1).astype(BF16)
            v_g = jnp.concatenate([jnp.concatenate([vc[l, g * group + 2 * i], vc[l, g * group + 2 * i + 1]], axis=1)
                                   for i in range(group // 2)], axis=0)
            out = jnp.dot(lhs, v_g, preferred_element_type=F32)
            outs.append(jnp.where(rowi % 2 == 0, out[:, :hd], out[:, hd:]))
        v_new = collect(2, bv).astype(BF16)
        v_stage[l] = v_new
        pltpu.make_async_copy(v_stage.at[l], v_out.at[l], out_sem.at[l, 1]).start()
        mixed = jnp.concatenate(outs, axis=0) + prob_new * v_new.astype(F32)

        ag_recv[l, row] = mixed.astype(BF16)
        for t, j in enumerate(row_order):
            remote(l, "ag", t, row, ag_recv.at[l, row], ag_recv.at[l, row], "row", j).start()
        big_copy(WO, l).wait()
        for t, j in enumerate(row_order):
            remote(l, "ag", t, j, ag_recv.at[l, row], ag_recv.at[l, j], "row", j).wait_recv()
        gathered = jnp.concatenate([ag_recv[l, j] for j in range(n_row)], axis=1)
        ar_col(l, "wo", jnp.dot(gathered, wo[l], preferred_element_type=F32), wo_recv, pick(bo, l))

        y2 = local_norm(l, "st2", 1, g2, b2)
        big_copy(W1, l).wait()

        def fc1_block(j):
            return jnp.dot(y2, w1[l, :, pl.ds(pl.multiple_of(j * ffb, ffb), ffb)], preferred_element_type=F32)

        for off in offs:
            k = lax.rem(chip + off, n_chip)
            fd_send[l, k] = fc1_block(2 * k + 1 - par).astype(BF16)
            remote(l, "fd", k, k, fd_send.at[l, k], fd_recv.at[l, k], "row", partner).start()
        for off in offs:
            k = lax.rem(chip + off, n_chip)
            f_mine[k] = fc1_block(2 * k + par)
        combine = global_norm(l, "st2", 1)
        for off in offs:
            k = lax.rem(chip + off, n_chip)
            remote(l, "fd", k, k, fd_send.at[l, k], fd_recv.at[l, k], "row", partner).wait_recv()
            both = combine(f_mine[k], fd_recv[l, k])
            if off:
                fi_send[l, k] = both.astype(BF16)
                remote(l, "fi", k, chip, fi_send.at[l, k], fi_recv.at[l, chip], "row", 2 * k + par).start()
            else:
                f_own[...] = both
        total = f_own[...]
        for off in (1, 3, 2):
            k = lax.rem(chip + off, n_chip)
            remote(l, "fi", k, k, fi_send.at[l, k], fi_recv.at[l, k], "row", 2 * k + par).wait_recv()
            total = total + fi_recv[l, k].astype(F32)
        u = jnp.maximum((total + pick_slice(bf1, l, row * ffb, ffb)).astype(BF16), 0)

        ug_recv[l, row] = u
        for off in offs[:-1]:
            k = lax.rem(chip + off, n_chip)
            remote(l, "ug", 2 * k + par, row, ug_recv.at[l, row], ug_recv.at[l, row], "row", 2 * k + par).start()
        remote(l, "ug", row, row, ug_recv.at[l, row], ug_recv.at[l, row], "row", partner).start()
        big_copy(W2, l).wait()

        def fc2_block(j, u_j):
            return jnp.dot(u_j, w2[l, pl.ds(pl.multiple_of(j * ffb, ffb), ffb), :], preferred_element_type=F32)

        acc = fc2_block(row, u)

        def got(j, target):
            remote(l, "ug", j, j, ug_recv.at[l, row], ug_recv.at[l, j], "row", target).wait_recv()

        got(partner, partner)
        acc = acc + fc2_block(partner, ug_recv[l, partner])
        for off in (1, 3, 2):
            k = lax.rem(chip + off, n_chip)
            j = 2 * k + par
            got(j, j)
            remote(l, "ug", 2 * k + 1 - par, j, ug_recv.at[l, j], ug_recv.at[l, j], "row", partner).start()
            acc = acc + fc2_block(j, ug_recv[l, j])
        for off in (1, 3, 2):
            k = lax.rem(chip + off, n_chip)
            j = 2 * k + 1 - par
            got(j, partner)
            acc = acc + fc2_block(j, ug_recv[l, j])
        ar_col(l, "fo", acc, fo_recv, pick(bf2, l))
        return carry

    lax.fori_loop(0, n_layer, layer, 0)
    pltpu.make_async_copy(state, h_out, out_sem.at[0, 2]).start()

    def drain(l, carry):
        def done(name, i, src, axis, target):
            remote(l, name, i, i, src, src, axis, target).wait_send()

        for t, j in enumerate(row_order):
            done("st1", t, st_send.at[l, 0], "row", j)
            done("st2", t, st_send.at[l, 1], "row", j)
            done("ag", t, ag_recv.at[l, row], "row", j)
        for t in (1, 2, 3):
            j = lax.rem(col + t, n_col)
            done("wo", t, wo_recv.at[l, col], "col", j)
            done("fo", t, fo_recv.at[l, col], "col", j)
        for w in range(3):
            done("qd", w, qd_send.at[l, w], "row", partner)
        pltpu.make_async_copy(k_stage.at[l], k_out.at[l], out_sem.at[l, 0]).wait()
        pltpu.make_async_copy(v_stage.at[l], v_out.at[l], out_sem.at[l, 1]).wait()
        for off in offs:
            k = lax.rem(chip + off, n_chip)
            for w in range(3):
                if off:
                    done("qi", w * n_chip + k, qi_send.at[l, w, k], "row", 2 * k + par)
            done("fd", k, fd_send.at[l, k], "row", partner)
            if off:
                done("fi", k, fi_send.at[l, k], "row", 2 * k + par)
                done("ug", 2 * k + par, ug_recv.at[l, row], "row", 2 * k + par)
                done("ug", 2 * k + 1 - par, ug_recv.at[l, 2 * k + par], "row", partner)
            else:
                done("ug", row, ug_recv.at[l, row], "row", partner)
        return carry

    lax.fori_loop(0, n_layer, drain, 0)
    pltpu.make_async_copy(state, h_out, out_sem.at[0, 2]).wait()


def solution(mesh):
    n_row, n_col = mesh.shape["row"], mesh.shape["col"]
    n_chip = n_row // 2
    act_spec = P("dp", "row")
    cache_spec = P(None, "dp", ("col", "row"), None, None)
    fresh_spec = P(None, "dp", ("col", "row"), None)
    in_weight = P(None, "row", "col")
    out_weight = P(None, "col", "row")
    col_vec = P(None, "col")
    row_vec = P(None, "row")
    in_specs = (act_spec, P("dp"), cache_spec, cache_spec, row_vec, row_vec,
                in_weight, col_vec, in_weight, col_vec, in_weight, col_vec,
                out_weight, row_vec, row_vec, row_vec, in_weight, col_vec, out_weight, row_vec)

    def local_step(hidden, cache_len, k_cache, v_cache, ln1_g, ln1_b, w_q, b_q, w_k, b_k, w_v, b_v,
                   w_o, b_o, ln2_g, ln2_b, w_fc1, b_fc1, w_fc2, b_fc2):
        batch, width = hidden.shape
        n_layer, _, _, keys, hd = k_cache.shape
        ff = w_fc1.shape[2]
        ffb = ff // n_row
        table, n_sem = layout(n_chip, n_row, n_col)
        args = (hidden, cache_len.reshape(1, batch), k_cache, v_cache, ln1_g, ln1_b, w_q, b_q, w_k, b_k, w_v, b_v,
                w_o, b_o, ln2_g, ln2_b, w_fc1, b_fc1, w_fc2, b_fc2)

        def vm(shape, dtype=BF16):
            return pltpu.VMEM(shape, dtype)

        local = [vm(a.shape, a.dtype) for a in args]
        local[2] = local[3] = vm((n_layer, batch, keys, hd))
        scratch = local + [
            vm((batch, width)),
            vm((n_layer, 2, 8, 128), F32), vm((n_layer, 2, n_row, 8, 128), F32),
            vm((n_layer, 3, batch + 16, n_chip * hd)), vm((n_layer, 3, batch + 16, n_chip * hd)),
            vm((3, batch + 16, n_chip * hd), F32), vm((3, batch, hd), F32),
            vm((n_layer, 3, n_chip, batch, hd)), vm((n_layer, 3, n_chip, batch, hd)),
            vm((n_layer, batch, hd)), vm((n_layer, batch, hd)), vm((n_layer, n_row, batch, hd)),
            vm((n_layer, n_col, batch, width)),
            vm((n_layer, n_chip, batch + 16, ffb)), vm((n_layer, n_chip, batch + 16, ffb)),
            vm((n_chip, batch + 16, ffb), F32), vm((batch, ffb), F32),
            vm((n_layer, n_chip, batch, ffb)), vm((n_layer, n_chip, batch, ffb)),
            vm((n_layer, n_row, batch, ffb)),
            vm((n_layer, n_col, batch, width)),
            pltpu.SemaphoreType.DMA((12,)), pltpu.SemaphoreType.DMA((n_layer, 8)), pltpu.SemaphoreType.DMA((n_layer, 3)),
            pltpu.SemaphoreType.DMA((n_layer, n_sem)), pltpu.SemaphoreType.DMA((n_layer, n_sem)),
        ]
        out_shape = (jax.ShapeDtypeStruct((batch, width), BF16),
                     jax.ShapeDtypeStruct((n_layer, batch, hd), BF16),
                     jax.ShapeDtypeStruct((n_layer, batch, hd), BF16))
        h_out, k_new, v_new = pl.pallas_call(
            functools.partial(kernel, (n_layer, n_row, n_col, table)),
            out_shape=out_shape,
            in_specs=[pl.BlockSpec(memory_space=pl.ANY)] * len(args),
            out_specs=[pl.BlockSpec(memory_space=pl.ANY)] * 3,
            scratch_shapes=scratch,
            compiler_params=pltpu.CompilerParams(collective_id=0, has_side_effects=True,
                                                 vmem_limit_bytes=66 * 1000 * 1000),
        )(*args)
        return h_out, k_new[:, :, None, :], v_new[:, :, None, :]

    return jax.shard_map(local_step, mesh=mesh, in_specs=in_specs,
                         out_specs=(act_spec, fresh_spec, fresh_spec), check_vma=False)
```

```python
import functools

import jax
import jax.numpy as jnp
from jax import lax
from jax.experimental import pallas as pl
from jax.experimental.pallas import tpu as pltpu
from jax.sharding import PartitionSpec as P

EPS_LN = 1e-5
MESH = pl.DeviceIdType.MESH
F32 = jnp.float32
BF16 = jnp.bfloat16


class Sems:
    def __init__(self):
        self.count = 0

    def take(self, n):
        base = self.count
        self.count += n
        return base


def layout(n_chip, n_row, n_col):
    sems = Sems()
    names = dict(st1=n_row, st2=n_row, qi=3 * n_row, ag=n_row, wo=n_col,
                 fd=n_chip, fi=n_chip, fg=n_chip, ug=n_row, fo=n_col)
    table = {name: sems.take(n) for name, n in names.items()}
    return table, sems.count


def kernel(dims, hid_hbm, len_hbm, kc_hbm, vc_hbm, g1_hbm, b1_hbm, wq_hbm, bq_hbm, wk_hbm, bk_hbm, wv_hbm, bv_hbm,
           wo_hbm, bo_hbm, g2_hbm, b2_hbm, w1_hbm, bf1_hbm, w2_hbm, bf2_hbm,
           h_out, k_out, v_out,
           hid_v, len_v, kc, vc, g1, b1, wq, bq, wk, bk, wv, bv, wo, bo, g2, b2, w1, bf1, w2, bf2,
           state, st_send, st_recv, qi_send, qi_recv, k_stage, v_stage, ag_recv, wo_recv,
           fd_send, fd_recv, f_mine, f_own, fi_send, fi_recv, fg_send, fg_recv, ug_recv, fo_recv,
           small_sem, big_sem, out_sem, ssem, rsem):
    n_layer, n_row, n_col, table = dims
    n_chip = n_row // 2
    row = lax.axis_index("row")
    col = lax.axis_index("col")
    chip = row // 2
    par = row % 2
    partner = row + 1 - 2 * par
    batch, width = hid_v.shape
    hd = kc.shape[-1]
    keys = kc.shape[2]
    ffb = fd_send.shape[-1]
    offs = [2, 1, 3, 0]

    barrier = pltpu.get_barrier_semaphore()
    for t in range(1, n_row):
        pl.semaphore_signal(barrier, inc=1, device_id={"row": lax.rem(row + t, n_row)}, device_id_type=MESH)
    for t in range(1, n_col):
        pl.semaphore_signal(barrier, inc=1, device_id={"col": lax.rem(col + t, n_col)}, device_id_type=MESH)

    small = [(hid_hbm, hid_v), (len_hbm, len_v), (g1_hbm, g1), (b1_hbm, b1), (bq_hbm, bq), (bk_hbm, bk),
             (bv_hbm, bv), (bo_hbm, bo), (g2_hbm, g2), (b2_hbm, b2), (bf1_hbm, bf1), (bf2_hbm, bf2)]
    small_copies = [pltpu.make_async_copy(s, d, small_sem.at[i]) for i, (s, d) in enumerate(small)]
    for c in small_copies:
        c.start()

    bigs = [(wq_hbm, wq), (wk_hbm, wk), (wv_hbm, wv), (kc_hbm, kc), (vc_hbm, vc), (wo_hbm, wo), (w1_hbm, w1),
            (w2_hbm, w2)]
    WQ, WK, WV, KC, VC, WO, W1, W2 = range(8)

    def big_copy(i, l):
        s, d = bigs[i]
        src = s.at[l, :, 0] if i in (KC, VC) else s.at[l]
        return pltpu.make_async_copy(src, d.at[l], big_sem.at[l, i])

    for i in (WQ, WK, WV):
        big_copy(i, 0).start()

    for c in small_copies:
        c.wait()
    state[...] = hid_v[...]
    for i in (KC, VC, WO, W1, W2):
        big_copy(i, 0).start()
    for l in range(1, n_layer):
        for i in range(8):
            big_copy(i, l).start()
    pl.semaphore_wait(barrier, n_row - 1 + n_col - 1)

    def remote(l, name, i_send, i_recv, src, dst, axis, target):
        return pltpu.make_async_remote_copy(
            src_ref=src, dst_ref=dst, send_sem=ssem.at[l, table[name] + i_send], recv_sem=rsem.at[l, table[name] + i_recv],
            device_id={axis: target}, device_id_type=MESH)

    def pick(ref, l):
        rows = ref[...].astype(F32)
        out = rows[0:1]
        for i in range(1, n_layer):
            out = jnp.where(l == i, rows[i:i + 1], out)
        return out

    def pick_slice(ref, l, start, size):
        rows = ref[:, pl.ds(pl.multiple_of(start, size), size)].astype(F32)
        out = rows[0:1]
        for i in range(1, n_layer):
            out = jnp.where(l == i, rows[i:i + 1], out)
        return out

    eye = lax.broadcasted_iota(jnp.int32, (batch, 128), 0) == lax.broadcasted_iota(jnp.int32, (batch, 128), 1)
    lens = jnp.sum(jnp.where(eye, jnp.pad(len_v[...], ((0, 0), (0, 128 - batch))), 0), axis=1, keepdims=True)

    row_order = []
    for off in offs[:-1]:
        k = lax.rem(chip + off, n_chip)
        row_order += [2 * k + par, 2 * k + 1 - par]
    row_order.append(partner)

    def to_row(column):
        return jnp.sum(jnp.where(eye, column, 0.0), axis=0, keepdims=True)

    def to_column(line):
        return jnp.sum(jnp.where(eye, line, 0.0), axis=1, keepdims=True)

    def local_norm(l, name, which, gain, shift):
        x = state[...].astype(F32)
        c = jnp.sum(x, axis=1, keepdims=True) / width
        xc = x - c
        v = jnp.sum(xc * xc, axis=1, keepdims=True) / width
        sub = lax.broadcasted_iota(jnp.int32, (8, 128), 0)
        tile = jnp.where(sub == 0, to_row(c), jnp.where(sub == 1, to_row(v), 0.0))
        st_send[l, which] = tile
        st_recv[l, which, row] = tile
        for t, j in enumerate(row_order):
            remote(l, name, t, row, st_send.at[l, which], st_recv.at[l, which, row], "row", j).start()
        g, b = pick(gain, l), pick(shift, l)
        y = xc * lax.rsqrt(v + EPS_LN) * g
        extra = lax.broadcasted_iota(jnp.int32, (16, 1), 0)
        extra = jnp.where(extra == 0, g, jnp.where(extra == 1, b, 0.0))
        return jnp.concatenate([y.astype(BF16), extra.astype(BF16)], axis=0)

    def wait_stats(l, name, which, sources):
        for j in sources:
            remote(l, name, 0, j, st_send.at[l, which], st_recv.at[l, which, j], "row", j).wait_recv()

    def scale_of(v):
        return (v + EPS_LN) * lax.rsqrt(v + EPS_LN)

    def global_norm(parts):
        m = sum(c for c, _ in parts) / len(parts)
        var = sum(v + (c - m) * (c - m) for c, v in parts) / len(parts)
        r = lax.rsqrt(var + EPS_LN)
        return [(to_column(r * scale_of(v)), to_column(r * (c - m))) for c, v in parts]

    def stats(l, which, j):
        tile = st_recv[l, which, j]
        return tile[0:1], tile[1:2]

    def merge(one, two):
        half = 0.5 * (one[0] - two[0])
        return 0.5 * (one[0] + two[0]), 0.5 * (one[1] + two[1]) + half * half

    def ar_col(l, name, part, buf, bias):
        buf[l, col] = part.astype(BF16)
        for t in (2, 1, 3):
            j = lax.rem(col + t, n_col)
            remote(l, name, t, col, buf.at[l, col], buf.at[l, col], "col", j).start()
        for t in (1, 3, 2):
            j = lax.rem(col + t, n_col)
            remote(l, name, t, j, buf.at[l, col], buf.at[l, j], "col", j).wait_recv()
        total = buf[l, 0].astype(F32)
        for j in range(1, n_col):
            total = total + buf[l, j].astype(F32)
        state[...] = (state[...].astype(F32) + (total + bias)).astype(BF16)

    def layer(l, carry):
        y = local_norm(l, "st1", 0, g1, b1)

        def project(w, i_big, wref):
            big_copy(i_big, l).wait()
            res = jnp.dot(y, wref[l], preferred_element_type=F32).astype(BF16)
            for j in range(n_row):
                qi_send[l, w, j] = res[:, j * hd:(j + 1) * hd]
            for j in row_order:
                remote(l, "qi", w * n_row + j, w * n_row + row, qi_send.at[l, w, j], qi_recv.at[l, w, row],
                       "row", j).start()
            qi_recv[l, w, row] = qi_send[l, w, row]

        def collect(w, bias):
            for j in row_order:
                remote(l, "qi", w * n_row + j, w * n_row + j, qi_send.at[l, w, j], qi_recv.at[l, w, j],
                       "row", j).wait_recv()
            total = pick_slice(bias, l, row * hd, hd)
            for j in range(n_row):
                got = qi_recv[l, w, j].astype(F32)
                total = total + (coef[j][0] * got[:batch]
                                 + (coef[j][1] * got[batch:batch + 1] + got[batch + 1:batch + 2]))
            return total

        project(0, WQ, wq)
        project(1, WK, wk)
        project(2, WV, wv)
        wait_stats(l, "st1", 0, row_order)
        coef = global_norm([stats(l, 0, j) for j in range(n_row)])
        q = (collect(0, bq) * (hd ** -0.5)).astype(BF16).astype(F32)

        group = 16
        rowi = lax.broadcasted_iota(jnp.int32, (group, 1), 0)
        big_copy(KC, l).wait()
        parts = []
        for g in range(batch // group):
            q_g = q[g * group:(g + 1) * group]
            lhs = jnp.concatenate([jnp.where(rowi == i, q_g, 0.0) for i in range(group)], axis=1).astype(BF16)
            k_g = jnp.concatenate([kc[l, g * group + i] for i in range(group)], axis=1)
            parts.append(lax.dot_general(lhs, k_g, (((1,), (1,)), ((), ())), preferred_element_type=F32))
        scores = jnp.concatenate(parts, axis=0)
        scores = jnp.where(lax.broadcasted_iota(jnp.int32, (batch, keys), 1) < lens, scores, -jnp.inf)
        k_new = collect(1, bk).astype(BF16)
        k_stage[l] = k_new
        pltpu.make_async_copy(k_stage.at[l], k_out.at[l], out_sem.at[l, 0]).start()
        s_new = jnp.sum(q * k_new.astype(F32), axis=1, keepdims=True)
        peak = jnp.maximum(jnp.max(scores, axis=1, keepdims=True), s_new)
        e = jnp.exp(scores - peak)
        e_new = jnp.exp(s_new - peak)
        mass = jnp.sum(e, axis=1, keepdims=True) + e_new
        prob = (e / mass).astype(BF16).astype(F32)
        prob_new = (e_new / mass).astype(BF16).astype(F32)
        big_copy(VC, l).wait()
        outs = []
        for g in range(batch // group):
            p_g = prob[g * group:(g + 1) * group]
            lhs = jnp.concatenate([jnp.where(rowi // 2 == i, p_g, 0.0) for i in range(group // 2)],
                                  axis=1).astype(BF16)
            v_g = jnp.concatenate([jnp.concatenate([vc[l, g * group + 2 * i], vc[l, g * group + 2 * i + 1]], axis=1)
                                   for i in range(group // 2)], axis=0)
            out = jnp.dot(lhs, v_g, preferred_element_type=F32)
            outs.append(jnp.where(rowi % 2 == 0, out[:, :hd], out[:, hd:]))
        v_new = collect(2, bv).astype(BF16)
        v_stage[l] = v_new
        pltpu.make_async_copy(v_stage.at[l], v_out.at[l], out_sem.at[l, 1]).start()
        mixed = jnp.concatenate(outs, axis=0) + prob_new * v_new.astype(F32)

        ag_recv[l, row] = mixed.astype(BF16)
        for t, j in enumerate(row_order):
            remote(l, "ag", t, row, ag_recv.at[l, row], ag_recv.at[l, row], "row", j).start()
        big_copy(WO, l).wait()
        for t, j in enumerate(row_order):
            remote(l, "ag", t, j, ag_recv.at[l, row], ag_recv.at[l, j], "row", j).wait_recv()
        gathered = jnp.concatenate([ag_recv[l, j] for j in range(n_row)], axis=1)
        ar_col(l, "wo", jnp.dot(gathered, wo[l], preferred_element_type=F32), wo_recv, pick(bo, l))

        y2 = local_norm(l, "st2", 1, g2, b2)
        big_copy(W1, l).wait()

        def fc1_block(j):
            return jnp.dot(y2, w1[l, :, pl.ds(pl.multiple_of(j * ffb, ffb), ffb)], preferred_element_type=F32)

        for off in offs:
            k = lax.rem(chip + off, n_chip)
            fd_send[l, k] = fc1_block(2 * k + 1 - par).astype(BF16)
            remote(l, "fd", k, k, fd_send.at[l, k], fd_recv.at[l, k], "row", partner).start()
        for off in offs:
            k = lax.rem(chip + off, n_chip)
            f_mine[k] = fc1_block(2 * k + par)
        wait_stats(l, "st2", 1, [partner])
        here, there = stats(l, 1, row), stats(l, 1, partner)
        c_pair, v_pair = merge(here, there)
        r_pair = lax.rsqrt(v_pair + EPS_LN)
        a_own, a_got = to_column(r_pair * scale_of(here[1])), to_column(r_pair * scale_of(there[1]))
        d_own = to_column(r_pair * (here[0] - c_pair))
        lanes = ffb // 128
        for off in offs:
            k = lax.rem(chip + off, n_chip)
            remote(l, "fd", k, k, fd_send.at[l, k], fd_recv.at[l, k], "row", partner).wait_recv()
            own, got = f_mine[k], fd_recv[l, k].astype(F32)
            g_own, g_got = own[batch:batch + 1], got[batch:batch + 1]
            both = (a_own * own[:batch] + a_got * got[:batch]) + d_own * (g_own - g_got)
            rows_gb = jnp.concatenate([g_own + g_got, own[batch + 1:batch + 2] + got[batch + 1:batch + 2]], axis=1)
            tile = jnp.concatenate([rows_gb[:, i * 128:(i + 1) * 128] for i in range(2 * lanes)], axis=0)
            if off:
                fi_send[l, k] = both.astype(BF16)
                fg_send[l, k] = tile
                remote(l, "fi", k, chip, fi_send.at[l, k], fi_recv.at[l, chip], "row", 2 * k + par).start()
                remote(l, "fg", k, chip, fg_send.at[l, k], fg_recv.at[l, chip], "row", 2 * k + par).start()
            else:
                f_own[...] = both
                fg_recv[l, k] = tile
        wait_stats(l, "st2", 1, row_order[:-1])
        pairs = [merge(stats(l, 1, 2 * k), stats(l, 1, 2 * k + 1)) for k in range(n_chip)]
        coef = global_norm(pairs)
        total = pick_slice(bf1, l, row * ffb, ffb)
        for k in range(n_chip):
            if k == 0:
                scale_own, shift_own = coef[0]
            else:
                scale_own = jnp.where(chip == k, coef[k][0], scale_own)
                shift_own = jnp.where(chip == k, coef[k][1], shift_own)

        def add(total, k, part, scale, shift):
            tile = fg_recv[l, k]
            g = jnp.concatenate([tile[i:i + 1] for i in range(lanes)], axis=1)
            b = jnp.concatenate([tile[lanes + i:lanes + i + 1] for i in range(lanes)], axis=1)
            return total + (scale * part + (shift * g + b))

        total = add(total, chip, f_own[...], scale_own, shift_own)
        for off in (1, 3, 2):
            k = lax.rem(chip + off, n_chip)
            remote(l, "fi", k, k, fi_send.at[l, k], fi_recv.at[l, k], "row", 2 * k + par).wait_recv()
            remote(l, "fg", k, k, fg_send.at[l, k], fg_recv.at[l, k], "row", 2 * k + par).wait_recv()
            scale, shift = coef[0]
            for i in range(1, n_chip):
                scale = jnp.where(k == i, coef[i][0], scale)
                shift = jnp.where(k == i, coef[i][1], shift)
            total = add(total, k, fi_recv[l, k].astype(F32), scale, shift)
        u = jnp.maximum(total.astype(BF16), 0)

        ug_recv[l, row] = u
        for off in offs[:-1]:
            k = lax.rem(chip + off, n_chip)
            remote(l, "ug", 2 * k + par, row, ug_recv.at[l, row], ug_recv.at[l, row], "row", 2 * k + par).start()
        remote(l, "ug", row, row, ug_recv.at[l, row], ug_recv.at[l, row], "row", partner).start()
        big_copy(W2, l).wait()

        def fc2_block(j, u_j):
            return jnp.dot(u_j, w2[l, pl.ds(pl.multiple_of(j * ffb, ffb), ffb), :], preferred_element_type=F32)

        acc = fc2_block(row, u)

        def got(j, target):
            remote(l, "ug", j, j, ug_recv.at[l, row], ug_recv.at[l, j], "row", target).wait_recv()

        got(partner, partner)
        acc = acc + fc2_block(partner, ug_recv[l, partner])
        for off in (1, 3, 2):
            k = lax.rem(chip + off, n_chip)
            j = 2 * k + par
            got(j, j)
            remote(l, "ug", 2 * k + 1 - par, j, ug_recv.at[l, j], ug_recv.at[l, j], "row", partner).start()
            acc = acc + fc2_block(j, ug_recv[l, j])
        for off in (1, 3, 2):
            k = lax.rem(chip + off, n_chip)
            j = 2 * k + 1 - par
            got(j, partner)
            acc = acc + fc2_block(j, ug_recv[l, j])
        ar_col(l, "fo", acc, fo_recv, pick(bf2, l))
        return carry

    lax.fori_loop(0, n_layer, layer, 0)
    pltpu.make_async_copy(state, h_out, out_sem.at[0, 2]).start()

    def drain(l, carry):
        def done(name, i, src, axis, target):
            remote(l, name, i, i, src, src, axis, target).wait_send()

        for t, j in enumerate(row_order):
            done("st1", t, st_send.at[l, 0], "row", j)
            done("st2", t, st_send.at[l, 1], "row", j)
            done("ag", t, ag_recv.at[l, row], "row", j)
        for t in (1, 2, 3):
            j = lax.rem(col + t, n_col)
            done("wo", t, wo_recv.at[l, col], "col", j)
            done("fo", t, fo_recv.at[l, col], "col", j)
        for w in range(3):
            for j in row_order:
                done("qi", w * n_row + j, qi_send.at[l, w, j], "row", j)
        pltpu.make_async_copy(k_stage.at[l], k_out.at[l], out_sem.at[l, 0]).wait()
        pltpu.make_async_copy(v_stage.at[l], v_out.at[l], out_sem.at[l, 1]).wait()
        for off in offs:
            k = lax.rem(chip + off, n_chip)
            done("fd", k, fd_send.at[l, k], "row", partner)
            if off:
                done("fi", k, fi_send.at[l, k], "row", 2 * k + par)
                done("fg", k, fg_send.at[l, k], "row", 2 * k + par)
                done("ug", 2 * k + par, ug_recv.at[l, row], "row", 2 * k + par)
                done("ug", 2 * k + 1 - par, ug_recv.at[l, 2 * k + par], "row", partner)
            else:
                done("ug", row, ug_recv.at[l, row], "row", partner)
        return carry

    lax.fori_loop(0, n_layer, drain, 0)
    pltpu.make_async_copy(state, h_out, out_sem.at[0, 2]).wait()


def solution(mesh):
    n_row, n_col = mesh.shape["row"], mesh.shape["col"]
    n_chip = n_row // 2
    act_spec = P("dp", "row")
    cache_spec = P(None, "dp", ("col", "row"), None, None)
    fresh_spec = P(None, "dp", ("col", "row"), None)
    in_weight = P(None, "row", "col")
    out_weight = P(None, "col", "row")
    col_vec = P(None, "col")
    row_vec = P(None, "row")
    in_specs = (act_spec, P("dp"), cache_spec, cache_spec, row_vec, row_vec,
                in_weight, col_vec, in_weight, col_vec, in_weight, col_vec,
                out_weight, row_vec, row_vec, row_vec, in_weight, col_vec, out_weight, row_vec)

    def local_step(hidden, cache_len, k_cache, v_cache, ln1_g, ln1_b, w_q, b_q, w_k, b_k, w_v, b_v,
                   w_o, b_o, ln2_g, ln2_b, w_fc1, b_fc1, w_fc2, b_fc2):
        batch, width = hidden.shape
        n_layer, _, _, keys, hd = k_cache.shape
        ff = w_fc1.shape[2]
        ffb = ff // n_row
        table, n_sem = layout(n_chip, n_row, n_col)
        args = (hidden, cache_len.reshape(1, batch), k_cache, v_cache, ln1_g, ln1_b, w_q, b_q, w_k, b_k, w_v, b_v,
                w_o, b_o, ln2_g, ln2_b, w_fc1, b_fc1, w_fc2, b_fc2)

        def vm(shape, dtype=BF16):
            return pltpu.VMEM(shape, dtype)

        local = [vm(a.shape, a.dtype) for a in args]
        local[2] = local[3] = vm((n_layer, batch, keys, hd))
        scratch = local + [
            vm((batch, width)),
            vm((n_layer, 2, 8, 128), F32), vm((n_layer, 2, n_row, 8, 128), F32),
            vm((n_layer, 3, n_row, batch + 16, hd)), vm((n_layer, 3, n_row, batch + 16, hd)),
            vm((n_layer, batch, hd)), vm((n_layer, batch, hd)), vm((n_layer, n_row, batch, hd)),
            vm((n_layer, n_col, batch, width)),
            vm((n_layer, n_chip, batch + 16, ffb)), vm((n_layer, n_chip, batch + 16, ffb)),
            vm((n_chip, batch + 16, ffb), F32), vm((batch, ffb), F32),
            vm((n_layer, n_chip, batch, ffb)), vm((n_layer, n_chip, batch, ffb)),
            vm((n_layer, n_chip, 2 * ffb // 128, 128), F32), vm((n_layer, n_chip, 2 * ffb // 128, 128), F32),
            vm((n_layer, n_row, batch, ffb)),
            vm((n_layer, n_col, batch, width)),
            pltpu.SemaphoreType.DMA((12,)), pltpu.SemaphoreType.DMA((n_layer, 8)), pltpu.SemaphoreType.DMA((n_layer, 3)),
            pltpu.SemaphoreType.DMA((n_layer, n_sem)), pltpu.SemaphoreType.DMA((n_layer, n_sem)),
        ]
        out_shape = (jax.ShapeDtypeStruct((batch, width), BF16),
                     jax.ShapeDtypeStruct((n_layer, batch, hd), BF16),
                     jax.ShapeDtypeStruct((n_layer, batch, hd), BF16))
        h_out, k_new, v_new = pl.pallas_call(
            functools.partial(kernel, (n_layer, n_row, n_col, table)),
            out_shape=out_shape,
            in_specs=[pl.BlockSpec(memory_space=pl.ANY)] * len(args),
            out_specs=[pl.BlockSpec(memory_space=pl.ANY)] * 3,
            scratch_shapes=scratch,
            compiler_params=pltpu.CompilerParams(collective_id=0, has_side_effects=True,
                                                 vmem_limit_bytes=66 * 1000 * 1000),
        )(*args)
        return h_out, k_new[:, :, None, :], v_new[:, :, None, :]

    return jax.shard_map(local_step, mesh=mesh, in_specs=in_specs,
                         out_specs=(act_spec, fresh_spec, fresh_spec), check_vma=False)
```

```python
import functools

import jax
import jax.numpy as jnp
from jax import lax
from jax.experimental import pallas as pl
from jax.experimental.pallas import tpu as pltpu
from jax.sharding import PartitionSpec as P

EPS_LN = 1e-5
VLIM = 66 * 1000 * 1000
MESH = pl.DeviceIdType.MESH
F32 = jnp.float32
BF16 = jnp.bfloat16


class Sems:
    def __init__(self):
        self.count = 0

    def take(self, n):
        base = self.count
        self.count += n
        return base


def layout():
    sems = Sems()
    names = dict(st1=1, st1p=1, st2=1, st2p=1, q=1, kd=1, vd=1, k=1, v=1, ag=1, wo=1, fd=4, fi=1, fg=1, ug=8, fo=1)
    table = {name: sems.take(n) for name, n in names.items()}
    return table, sems.count


def kernel(dims, hid_hbm, len_hbm, kc_hbm, vc_hbm, g1_hbm, b1_hbm, wq_hbm, bq_hbm, wk_hbm, bk_hbm, wv_hbm, bv_hbm,
           wo_hbm, bo_hbm, g2_hbm, b2_hbm, w1_hbm, bf1_hbm, w2_hbm, bf2_hbm,
           h_out, k_out, v_out,
           hid_v, len_v, kc, vc, g1, b1, wq, bq, wk, bk, wv, bv, wo, bo, g2, b2, w1, bf1, w2, bf2,
           state, st_send, st_recv, q_send, q_recv, kd_send, kd_recv, k_mine, k_send, k_recv, k_stage, v_stage,
           ag_recv, wo_recv, fd_send, fd_recv, f_mine, f_own, fi_send, fi_recv, fg_send, fg_recv, ug_recv, fo_recv,
           small_sem, big_sem, out_sem, ssem, rsem):
    n_layer, n_row, n_col, table = dims
    n_chip = n_row // 2
    row = lax.axis_index("row")
    col = lax.axis_index("col")
    chip = row // 2
    par = row % 2
    partner = row + 1 - 2 * par
    batch, width = hid_v.shape
    hd = kc.shape[-1]
    keys = kc.shape[2]
    ffb = fd_send.shape[-1]
    offs = [2, 1, 3, 0]
    chips = {off: lax.rem(chip + off, n_chip) for off in offs}
    row_order = []
    for off in offs[:-1]:
        row_order += [2 * chips[off] + par, 2 * chips[off] + 1 - par]

    barrier = pltpu.get_barrier_semaphore()
    for t in range(1, n_row):
        pl.semaphore_signal(barrier, inc=1, device_id={"row": lax.rem(row + t, n_row)}, device_id_type=MESH)
    for t in range(1, n_col):
        pl.semaphore_signal(barrier, inc=1, device_id={"col": lax.rem(col + t, n_col)}, device_id_type=MESH)

    small = [(hid_hbm, hid_v), (len_hbm, len_v), (g1_hbm, g1), (b1_hbm, b1), (bq_hbm, bq), (bk_hbm, bk),
             (bv_hbm, bv), (bo_hbm, bo), (g2_hbm, g2), (b2_hbm, b2), (bf1_hbm, bf1), (bf2_hbm, bf2)]
    small_copies = [pltpu.make_async_copy(s, d, small_sem.at[i]) for i, (s, d) in enumerate(small)]
    for c in small_copies:
        c.start()

    bigs = [(wq_hbm, wq), (wk_hbm, wk), (wv_hbm, wv), (kc_hbm, kc), (vc_hbm, vc), (wo_hbm, wo), (w1_hbm, w1),
            (w2_hbm, w2)]
    WQ, WK, WV, KC, VC, WO, W1, W2 = range(8)

    def big_copy(i, l):
        s, d = bigs[i]
        src = s.at[l, :, 0] if i in (KC, VC) else s.at[l]
        return pltpu.make_async_copy(src, d.at[l], big_sem.at[l, i])

    for i in (WQ, WK, WV):
        big_copy(i, 0).start()

    small_copies[0].wait()
    state[...] = hid_v[...]

    def enter():
        pl.semaphore_wait(barrier, n_row - 1 + n_col - 1)

    def rest_of_loads():
        for i in (KC, VC, WO, W1, W2):
            big_copy(i, 0).start()
        for l in range(1, n_layer):
            for i in range(8):
                big_copy(i, l).start()
        for c in small_copies[1:]:
            c.wait()

    def remote(name, i, src, dst, axis, target):
        sem = table[name] + i
        return pltpu.make_async_remote_copy(src_ref=src, dst_ref=dst, send_sem=ssem.at[sem], recv_sem=rsem.at[sem],
                                            device_id={axis: target}, device_id_type=MESH)

    def got(name, i, ref, axis="row"):
        remote(name, i, ref, ref, axis, partner if axis == "row" else lax.rem(col + 1, n_col)).wait_recv()

    def sent(name, i, ref, axis="row"):
        remote(name, i, ref, ref, axis, partner if axis == "row" else lax.rem(col + 1, n_col)).wait_send()

    def pick(ref, l):
        rows = ref[...].astype(F32)
        out = rows[0:1]
        for i in range(1, n_layer):
            out = jnp.where(l == i, rows[i:i + 1], out)
        return out

    def pick_slice(ref, l, start, size):
        rows = ref[:, pl.ds(pl.multiple_of(start, size), size)].astype(F32)
        out = rows[0:1]
        for i in range(1, n_layer):
            out = jnp.where(l == i, rows[i:i + 1], out)
        return out

    eye = lax.broadcasted_iota(jnp.int32, (batch, 128), 0) == lax.broadcasted_iota(jnp.int32, (batch, 128), 1)

    def to_row(column):
        return jnp.sum(jnp.where(eye, column, 0.0), axis=0, keepdims=True)

    def to_column(line):
        return jnp.sum(jnp.where(eye, line, 0.0), axis=1, keepdims=True)

    def local_norm(l, name, which, gain, shift):
        x = state[...].astype(F32)
        c = jnp.sum(x, axis=1, keepdims=True) / width
        xc = x - c
        v = jnp.sum(xc * xc, axis=1, keepdims=True) / width
        sub = lax.broadcasted_iota(jnp.int32, (8, 128), 0)
        tile = jnp.where(sub == 0, to_row(c), jnp.where(sub == 1, to_row(v), 0.0))
        st_send[l, which] = tile
        if which == 0:
            pl.when(l == 0)(enter)
        for j in row_order:
            remote(name, 0, st_send.at[l, which], st_recv.at[l, which, row], "row", j).start()
        remote(name + "p", 0, st_send.at[l, which], st_recv.at[l, which, row], "row", partner).start()
        st_recv[l, which, row] = tile
        if which == 0:
            pl.when(l == 0)(rest_of_loads)
        g, b = pick(gain, l), pick(shift, l)
        y = xc * lax.rsqrt(v + EPS_LN) * g
        extra = lax.broadcasted_iota(jnp.int32, (16, 1), 0)
        extra = jnp.where(extra == 0, g, jnp.where(extra == 1, b, 0.0))
        return jnp.concatenate([y.astype(BF16), extra.astype(BF16)], axis=0)

    def scale_of(v):
        return (v + EPS_LN) * lax.rsqrt(v + EPS_LN)

    def global_norm(parts):
        m = sum(c for c, _ in parts) / len(parts)
        var = sum(v + (c - m) * (c - m) for c, v in parts) / len(parts)
        r = lax.rsqrt(var + EPS_LN)
        return [(to_column(r * scale_of(v)), to_column(r * (c - m))) for c, v in parts]

    def stats(l, which, j):
        tile = st_recv[l, which, j]
        return tile[0:1], tile[1:2]

    def merge(one, two):
        half = 0.5 * (one[0] - two[0])
        return 0.5 * (one[0] + two[0]), 0.5 * (one[1] + two[1]) + half * half

    def pair_merge(l, which):
        here, there = stats(l, which, row), stats(l, which, partner)
        c_pair, v_pair = merge(here, there)
        r_pair = lax.rsqrt(v_pair + EPS_LN)
        a_own, a_got = to_column(r_pair * scale_of(here[1])), to_column(r_pair * scale_of(there[1]))
        d_own = to_column(r_pair * (here[0] - c_pair))

        def rows(own, got_rows):
            return ((a_own * own[:batch] + a_got * got_rows[:batch])
                    + d_own * (own[batch:batch + 1] - got_rows[batch:batch + 1]))

        return rows

    def pair_coefficients(l, which):
        return global_norm([merge(stats(l, which, 2 * k), stats(l, which, 2 * k + 1)) for k in range(n_chip)])

    def ar_col(l, name, part, buf, bias):
        buf[l, col] = part.astype(BF16)
        for t in (2, 1, 3):
            remote(name, 0, buf.at[l, col], buf.at[l, col], "col", lax.rem(col + t, n_col)).start()
        if name == "fo":
            drain(l)
        got(name, 0, buf.at[l, pl.ds(0, n_col - 1)], "col")
        total = buf[l, 0].astype(F32)
        for j in range(1, n_col):
            total = total + buf[l, j].astype(F32)
        state[...] = (state[...].astype(F32) + (total + bias)).astype(BF16)
        sent(name, 0, buf.at[l, pl.ds(0, n_col - 1)], "col")

    def drain(l):
        for which, name in ((0, "st1"), (1, "st2")):
            sent(name, 0, st_recv.at[l, which, pl.ds(0, n_row - 2)])
            sent(name + "p", 0, st_recv.at[l, which, 0])
        sent("q", 0, q_recv.at[l, pl.ds(0, n_row - 1)])
        for w, (d, i) in enumerate((("kd", "k"), ("vd", "v"))):
            sent(d, 0, kd_send.at[l, w])
            sent(i, 0, k_send.at[l, w, pl.ds(0, n_chip - 1)])
        sent("ag", 0, ag_recv.at[l, pl.ds(0, n_row - 1)])
        for k in range(n_chip):
            sent("fd", k, fd_send.at[l, k])
        sent("fi", 0, fi_send.at[l, pl.ds(0, n_chip - 1)])
        sent("fg", 0, fg_send.at[l, pl.ds(0, n_chip - 1)])
        for j in range(n_row - 1):
            sent("ug", j, ug_recv.at[l, j])

    def layer(l, carry):
        y = local_norm(l, "st1", 0, g1, b1)

        big_copy(WQ, l).wait()
        res = jnp.dot(y, wq[l], preferred_element_type=F32).astype(BF16)
        for j in range(n_row):
            q_send[l, j] = res[:, j * hd:(j + 1) * hd]
        for j in row_order + [partner]:
            remote("q", 0, q_send.at[l, j], q_recv.at[l, row], "row", j).start()
        q_recv[l, row] = q_send[l, row]

        for i_big, w_ref in ((WK, wk), (WV, wv)):
            big_copy(i_big, l).wait()
        for w, (name, w_ref) in enumerate((("kd", wk), ("vd", wv))):
            res = jnp.dot(y, w_ref[l], preferred_element_type=F32)
            even = jnp.concatenate([res[:, 2 * k * hd:(2 * k + 1) * hd] for k in range(n_chip)], axis=1)
            odd = jnp.concatenate([res[:, (2 * k + 1) * hd:(2 * k + 2) * hd] for k in range(n_chip)], axis=1)
            kd_send[l, w] = jnp.where(par == 0, odd, even).astype(BF16)
            remote(name, 0, kd_send.at[l, w], kd_recv.at[l, w], "row", partner).start()
            k_mine[w] = jnp.where(par == 0, even, odd)

        got("st1p", 0, st_recv.at[l, 0, 0])
        merged = pair_merge(l, 0)
        for w, (d_name, name) in enumerate((("kd", "k"), ("vd", "v"))):
            got(d_name, 0, kd_recv.at[l, w])
            own, other = k_mine[w], kd_recv[l, w].astype(F32)
            both = jnp.concatenate([merged(own, other), own[batch:] + other[batch:]], axis=0).astype(BF16)
            for k in range(n_chip):
                k_send[l, w, k] = both[:, k * hd:(k + 1) * hd]
            for off in offs[:-1]:
                k = chips[off]
                remote(name, 0, k_send.at[l, w, k], k_recv.at[l, w, chip], "row", 2 * k + par).start()
            k_recv[l, w, chip] = k_send[l, w, chip]

        def collect(parts, coefs, bias):
            total = pick_slice(bias, l, row * hd, hd)
            for part, (scale, shift) in zip(parts, coefs):
                part = part.astype(F32)
                total = total + (scale * part[:batch] + (shift * part[batch:batch + 1] + part[batch + 1:batch + 2]))
            return total

        got("st1", 0, st_recv.at[l, 0, pl.ds(0, n_row - 2)])
        coef = global_norm([stats(l, 0, j) for j in range(n_row)])
        coef_pair = pair_coefficients(l, 0)
        got("q", 0, q_recv.at[l, pl.ds(0, n_row - 1)])
        q = collect([q_recv[l, j] for j in range(n_row)], coef, bq)
        q = (q * (hd ** -0.5)).astype(BF16).astype(F32)

        group = 16
        rowi = lax.broadcasted_iota(jnp.int32, (group, 1), 0)
        big_copy(KC, l).wait()
        parts = []
        for g in range(batch // group):
            q_g = q[g * group:(g + 1) * group]
            lhs = jnp.concatenate([jnp.where(rowi == i, q_g, 0.0) for i in range(group)], axis=1).astype(BF16)
            k_g = jnp.concatenate([kc[l, g * group + i] for i in range(group)], axis=1)
            parts.append(lax.dot_general(lhs, k_g, (((1,), (1,)), ((), ())), preferred_element_type=F32))
        scores = jnp.concatenate(parts, axis=0)
        lens = jnp.sum(jnp.where(eye, jnp.pad(len_v[...], ((0, 0), (0, 128 - batch))), 0), axis=1, keepdims=True)
        scores = jnp.where(lax.broadcasted_iota(jnp.int32, (batch, keys), 1) < lens, scores, -jnp.inf)
        got("k", 0, k_recv.at[l, 0, pl.ds(0, n_chip - 1)])
        k_new = collect([k_recv[l, 0, k] for k in range(n_chip)], coef_pair, bk).astype(BF16)
        k_stage[l] = k_new
        pltpu.make_async_copy(k_stage.at[l], k_out.at[l], out_sem.at[l, 0]).start()
        s_new = jnp.sum(q * k_new.astype(F32), axis=1, keepdims=True)
        peak = jnp.maximum(jnp.max(scores, axis=1, keepdims=True), s_new)
        e = jnp.exp(scores - peak)
        e_new = jnp.exp(s_new - peak)
        mass = jnp.sum(e, axis=1, keepdims=True) + e_new
        prob = (e / mass).astype(BF16).astype(F32)
        prob_new = (e_new / mass).astype(BF16).astype(F32)
        big_copy(VC, l).wait()
        outs = []
        for g in range(batch // group):
            p_g = prob[g * group:(g + 1) * group]
            lhs = jnp.concatenate([jnp.where(rowi // 2 == i, p_g, 0.0) for i in range(group // 2)],
                                  axis=1).astype(BF16)
            v_g = jnp.concatenate([jnp.concatenate([vc[l, g * group + 2 * i], vc[l, g * group + 2 * i + 1]], axis=1)
                                   for i in range(group // 2)], axis=0)
            out = jnp.dot(lhs, v_g, preferred_element_type=F32)
            outs.append(jnp.where(rowi % 2 == 0, out[:, :hd], out[:, hd:]))
        got("v", 0, k_recv.at[l, 1, pl.ds(0, n_chip - 1)])
        v_new = collect([k_recv[l, 1, k] for k in range(n_chip)], coef_pair, bv).astype(BF16)
        mixed = jnp.concatenate(outs, axis=0) + prob_new * v_new.astype(F32)

        ag_recv[l, row] = mixed.astype(BF16)
        for j in row_order + [partner]:
            remote("ag", 0, ag_recv.at[l, row], ag_recv.at[l, row], "row", j).start()
        v_stage[l] = v_new
        pltpu.make_async_copy(v_stage.at[l], v_out.at[l], out_sem.at[l, 1]).start()
        big_copy(WO, l).wait()
        got("ag", 0, ag_recv.at[l, pl.ds(0, n_row - 1)])
        gathered = jnp.concatenate([ag_recv[l, j] for j in range(n_row)], axis=1)
        ar_col(l, "wo", jnp.dot(gathered, wo[l], preferred_element_type=F32), wo_recv, pick(bo, l))

        y2 = local_norm(l, "st2", 1, g2, b2)
        big_copy(W1, l).wait()

        def fc1_block(j):
            return jnp.dot(y2, w1[l, :, pl.ds(pl.multiple_of(j * ffb, ffb), ffb)], preferred_element_type=F32)

        for some in (offs[:2], offs[2:]):
            blocks = [fc1_block(2 * chips[off] + 1 - par).astype(BF16) for off in some]
            for off, block in zip(some, blocks):
                fd_send[l, chips[off]] = block
            for off in some:
                k = chips[off]
                remote("fd", k, fd_send.at[l, k], fd_recv.at[l, k], "row", partner).start()
        blocks = [fc1_block(2 * chips[off] + par) for off in offs]
        for off, block in zip(offs, blocks):
            f_mine[chips[off]] = block
        got("st2p", 0, st_recv.at[l, 1, 0])
        merged = pair_merge(l, 1)
        lanes = ffb // 128
        for off in offs:
            k = chips[off]
            got("fd", k, fd_recv.at[l, k])
            own, other = f_mine[k], fd_recv[l, k].astype(F32)
            both = merged(own, other)
            gb = own[batch:] + other[batch:]
            gb = jnp.concatenate([gb[0:1], gb[1:2]], axis=1)
            tile = jnp.concatenate([gb[:, i * 128:(i + 1) * 128] for i in range(2 * lanes)], axis=0)
            if off:
                fi_send[l, k] = both.astype(BF16)
                fg_send[l, k] = tile
                remote("fi", 0, fi_send.at[l, k], fi_recv.at[l, chip], "row", 2 * k + par).start()
                remote("fg", 0, fg_send.at[l, k], fg_recv.at[l, chip], "row", 2 * k + par).start()
            else:
                fi_recv[l, k] = both.astype(BF16)
                fg_recv[l, k] = tile
        got("st2", 0, st_recv.at[l, 1, pl.ds(0, n_row - 2)])
        coef = pair_coefficients(l, 1)
        total = pick_slice(bf1, l, row * ffb, ffb)
        got("fg", 0, fg_recv.at[l, pl.ds(0, n_chip - 1)])
        got("fi", 0, fi_recv.at[l, pl.ds(0, n_chip - 1)])
        for k in range(n_chip):
            tile = fg_recv[l, k]
            g = jnp.concatenate([tile[i:i + 1] for i in range(lanes)], axis=1)
            b = jnp.concatenate([tile[lanes + i:lanes + i + 1] for i in range(lanes)], axis=1)
            total = total + (coef[k][0] * fi_recv[l, k].astype(F32) + (coef[k][1] * g + b))
        u = jnp.maximum(total.astype(BF16), 0)

        ug_recv[l, row] = u
        for off in offs[:-1]:
            remote("ug", n_chip - off, ug_recv.at[l, row], ug_recv.at[l, row], "row", 2 * chips[off] + par).start()
        remote("ug", 0, ug_recv.at[l, row], ug_recv.at[l, row], "row", partner).start()
        big_copy(W2, l).wait()

        def fc2_block(j):
            return jnp.dot(ug_recv[l, j], w2[l, pl.ds(pl.multiple_of(j * ffb, ffb), ffb), :],
                           preferred_element_type=F32)

        acc = jnp.dot(u, w2[l, pl.ds(pl.multiple_of(row * ffb, ffb), ffb), :], preferred_element_type=F32)
        got("ug", 0, ug_recv.at[l, partner])
        acc = acc + fc2_block(partner)

        def same(off):
            return 2 * chips[off] + par

        def cross(off):
            return 2 * chips[off] + 1 - par

        def pass_on(off):
            got("ug", off, ug_recv.at[l, same(off)])
            remote("ug", n_chip - 1 + off, ug_recv.at[l, same(off)], ug_recv.at[l, same(off)], "row", partner).start()

        pass_on(1)
        pass_on(3)
        acc = acc + (fc2_block(same(1)) + fc2_block(same(3)))
        pass_on(2)
        got("ug", n_chip, ug_recv.at[l, cross(1)])
        got("ug", n_chip + 2, ug_recv.at[l, cross(3)])
        acc = acc + (fc2_block(same(2)) + fc2_block(cross(1)) + fc2_block(cross(3)))
        got("ug", n_chip + 1, ug_recv.at[l, cross(2)])
        ar_col(l, "fo", acc + fc2_block(cross(2)), fo_recv, pick(bf2, l))
        return carry

    lax.fori_loop(0, n_layer, layer, 0)
    pltpu.make_async_copy(state, h_out, out_sem.at[0, 2]).start()
    for l in range(n_layer):
        pltpu.make_async_copy(k_stage.at[l], k_out.at[l], out_sem.at[l, 0]).wait()
        pltpu.make_async_copy(v_stage.at[l], v_out.at[l], out_sem.at[l, 1]).wait()
    pltpu.make_async_copy(state, h_out, out_sem.at[0, 2]).wait()


def finish(h, k, v, h_out, k_out, v_out, h_v, k_v, v_v, sem_in, sem_out):
    loads = [pltpu.make_async_copy(s, d, sem_in.at[i]) for i, (s, d) in enumerate(((h, h_v), (k, k_v), (v, v_v)))]
    stores = [pltpu.make_async_copy(s, d, sem_out.at[i])
              for i, (s, d) in enumerate(((h_v, h_out), (k_v, k_out), (v_v, v_out)))]
    for c in loads:
        c.start()
    for c, d in zip(loads, stores):
        c.wait()
        d.start()
    for d in stores:
        d.wait()


def solution(mesh):
    n_row, n_col = mesh.shape["row"], mesh.shape["col"]
    n_chip = n_row // 2
    act_spec = P("dp", "row")
    cache_spec = P(None, "dp", ("col", "row"), None, None)
    fresh_spec = P(None, "dp", ("col", "row"), None)
    in_weight = P(None, "row", "col")
    out_weight = P(None, "col", "row")
    col_vec = P(None, "col")
    row_vec = P(None, "row")
    in_specs = (act_spec, P("dp"), cache_spec, cache_spec, row_vec, row_vec,
                in_weight, col_vec, in_weight, col_vec, in_weight, col_vec,
                out_weight, row_vec, row_vec, row_vec, in_weight, col_vec, out_weight, row_vec)

    def local_step(hidden, cache_len, k_cache, v_cache, ln1_g, ln1_b, w_q, b_q, w_k, b_k, w_v, b_v,
                   w_o, b_o, ln2_g, ln2_b, w_fc1, b_fc1, w_fc2, b_fc2):
        batch, width = hidden.shape
        n_layer, _, _, keys, hd = k_cache.shape
        ff = w_fc1.shape[2]
        ffb = ff // n_row
        table, n_sem = layout()
        args = (hidden, cache_len.reshape(1, batch), k_cache, v_cache, ln1_g, ln1_b, w_q, b_q, w_k, b_k, w_v, b_v,
                w_o, b_o, ln2_g, ln2_b, w_fc1, b_fc1, w_fc2, b_fc2)

        def vm(shape, dtype=BF16):
            return pltpu.VMEM(shape, dtype)

        local = [vm(a.shape, a.dtype) for a in args]
        local[2] = local[3] = vm((n_layer, batch, keys, hd))
        scratch = local + [
            vm((batch, width)),
            vm((n_layer, 2, 8, 128), F32), vm((n_layer, 2, n_row, 8, 128), F32),
            vm((n_layer, n_row, batch + 16, hd)), vm((n_layer, n_row, batch + 16, hd)),
            vm((n_layer, 2, batch + 16, n_chip * hd)), vm((n_layer, 2, batch + 16, n_chip * hd)),
            vm((2, batch + 16, n_chip * hd), F32),
            vm((n_layer, 2, n_chip, batch + 16, hd)), vm((n_layer, 2, n_chip, batch + 16, hd)),
            vm((n_layer, batch, hd)), vm((n_layer, batch, hd)),
            vm((n_layer, n_row, batch, hd)), vm((n_layer, n_col, batch, width)),
            vm((n_layer, n_chip, batch + 16, ffb)), vm((n_layer, n_chip, batch + 16, ffb)),
            vm((n_chip, batch + 16, ffb), F32), vm((batch, ffb), F32),
            vm((n_layer, n_chip, batch, ffb)), vm((n_layer, n_chip, batch, ffb)),
            vm((n_layer, n_chip, 2 * ffb // 128, 128), F32), vm((n_layer, n_chip, 2 * ffb // 128, 128), F32),
            vm((n_layer, n_row, batch, ffb)), vm((n_layer, n_col, batch, width)),
            pltpu.SemaphoreType.DMA((12,)), pltpu.SemaphoreType.DMA((n_layer, 8)), pltpu.SemaphoreType.DMA((n_layer, 3)),
            pltpu.SemaphoreType.DMA((n_sem,)), pltpu.SemaphoreType.DMA((n_sem,)),
        ]
        out_shape = (jax.ShapeDtypeStruct((batch, width), BF16),
                     jax.ShapeDtypeStruct((n_layer, batch, hd), BF16),
                     jax.ShapeDtypeStruct((n_layer, batch, hd), BF16))
        h_out, k_new, v_new = pl.pallas_call(
            functools.partial(kernel, (n_layer, n_row, n_col, table)),
            out_shape=out_shape,
            in_specs=[pl.BlockSpec(memory_space=pl.ANY)] * len(args),
            out_specs=[pl.BlockSpec(memory_space=pl.ANY)] * 3,
            scratch_shapes=scratch,
            compiler_params=pltpu.CompilerParams(collective_id=0, has_side_effects=True,
                                                 vmem_limit_bytes=VLIM),
        )(*args)
        h_out, k_new, v_new = pl.pallas_call(
            finish, out_shape=out_shape,
            in_specs=[pl.BlockSpec(memory_space=pl.ANY)] * 3, out_specs=[pl.BlockSpec(memory_space=pl.ANY)] * 3,
            scratch_shapes=[vm(o.shape) for o in out_shape] + [pltpu.SemaphoreType.DMA((3,))] * 2,
        )(h_out, k_new, v_new)
        return h_out, k_new[:, :, None, :], v_new[:, :, None, :]

    return jax.shard_map(local_step, mesh=mesh, in_specs=in_specs,
                         out_specs=(act_spec, fresh_spec, fresh_spec), check_vma=False)
```

```python
import functools

import jax
import jax.numpy as jnp
from jax import lax
from jax.experimental import pallas as pl
from jax.experimental.pallas import tpu as pltpu
from jax.sharding import PartitionSpec as P

EPS_LN = 1e-5
VLIM = 66 * 1000 * 1000
MESH = pl.DeviceIdType.MESH
F32 = jnp.float32
BF16 = jnp.bfloat16


class Sems:
    def __init__(self):
        self.count = 0

    def take(self, n):
        base = self.count
        self.count += n
        return base


HALVES = 2


def layout(n_chip):
    sems = Sems()
    names = dict(st1=1, st1p=1, st2=1, st2p=1, q=1, kd=1, vd=1, k=1, v=1, ag=1, wo=1, fd=n_chip, fi=1, fg=1,
                 ug=2 * n_chip - 1, fo=1)
    table = [{name: sems.take(n) for name, n in names.items()} for _ in range(HALVES)]
    return table, sems.count


def kernel(dims, hid_hbm, len_hbm, kc_hbm, vc_hbm, g1_hbm, b1_hbm, wq_hbm, bq_hbm, wk_hbm, bk_hbm, wv_hbm, bv_hbm,
           wo_hbm, bo_hbm, g2_hbm, b2_hbm, w1_hbm, bf1_hbm, w2_hbm, bf2_hbm,
           h_out, k_out, v_out, local, halves, state, sem):
    n_layer, n_row, n_col, table = dims
    hid_v, len_v, kc, vc, g1, b1, wq, bq, wk, bk, wv, bv, wo, bo, g2, b2, w1, bf1, w2, bf2 = local
    small_sem, big_sem, out_sem, ssem, rsem = sem
    n_chip = n_row // 2
    row = lax.axis_index("row")
    col = lax.axis_index("col")
    chip = row // 2
    par = row % 2
    partner = row + 1 - 2 * par
    batch, width = hid_v.shape
    part = batch // HALVES
    hd = kc.shape[-1]
    keys = kc.shape[2]
    ffb = w1.shape[-1] // n_row
    lanes = ffb // 128
    offs = [2, 1, 3, 0]
    chips = {off: lax.rem(chip + off, n_chip) for off in offs}
    row_order = []
    for off in offs[:-1]:
        row_order += [2 * chips[off] + par, 2 * chips[off] + 1 - par]

    barrier = pltpu.get_barrier_semaphore()
    for t in range(1, n_row):
        pl.semaphore_signal(barrier, inc=1, device_id={"row": lax.rem(row + t, n_row)}, device_id_type=MESH)
    for t in range(1, n_col):
        pl.semaphore_signal(barrier, inc=1, device_id={"col": lax.rem(col + t, n_col)}, device_id_type=MESH)

    small = [(hid_hbm, hid_v), (g1_hbm, g1), (b1_hbm, b1), (len_hbm, len_v), (bq_hbm, bq), (bk_hbm, bk),
             (bv_hbm, bv), (bo_hbm, bo), (g2_hbm, g2), (b2_hbm, b2), (bf1_hbm, bf1), (bf2_hbm, bf2)]
    small_copies = [pltpu.make_async_copy(s, d, small_sem.at[i]) for i, (s, d) in enumerate(small)]
    bigs = [(wq_hbm, wq), (wk_hbm, wk), (wv_hbm, wv), (kc_hbm, kc), (vc_hbm, vc), (wo_hbm, wo), (w1_hbm, w1),
            (w2_hbm, w2)]
    WQ, WK, WV, KC, VC, WO, W1, W2 = range(8)

    def big_copy(i, l):
        s, d = bigs[i]
        src = s.at[l, :, 0] if i in (KC, VC) else s.at[l]
        return pltpu.make_async_copy(src, d.at[l], big_sem.at[l, i])

    for c in small_copies:
        c.start()
    for i in (WQ, WK, WV):
        big_copy(i, 0).start()
    small_copies[0].wait()
    state[...] = hid_v[...]

    def enter():
        pl.semaphore_wait(barrier, n_row - 1 + n_col - 1)

    def rest_of_small():
        for c in small_copies[1:]:
            c.wait()

    def rest_of_bulk():
        for i in (KC, VC, WO, W1, W2):
            big_copy(i, 0).start()
        for l in range(1, n_layer):
            for i in range(8):
                big_copy(i, l).start()

    def remote(h, name, i, src, dst, axis, target):
        at = table[h][name] + i
        return pltpu.make_async_remote_copy(src_ref=src, dst_ref=dst, send_sem=ssem.at[at], recv_sem=rsem.at[at],
                                            device_id={axis: target}, device_id_type=MESH)

    def same_bytes(h, name, i, ref, axis):
        return remote(h, name, i, ref, ref, axis, partner if axis == "row" else lax.rem(col + 1, n_col))

    def got(h, name, i, ref, axis="row"):
        same_bytes(h, name, i, ref, axis).wait_recv()

    def sent(h, name, i, ref, axis="row"):
        same_bytes(h, name, i, ref, axis).wait_send()

    def pick(ref, l):
        rows = ref[...].astype(F32)
        out = rows[0:1]
        for i in range(1, n_layer):
            out = jnp.where(l == i, rows[i:i + 1], out)
        return out

    def pick_slice(ref, l, start, size):
        rows = ref[:, pl.ds(pl.multiple_of(start, size), size)].astype(F32)
        out = rows[0:1]
        for i in range(1, n_layer):
            out = jnp.where(l == i, rows[i:i + 1], out)
        return out

    eye = lax.broadcasted_iota(jnp.int32, (part, 128), 0) == lax.broadcasted_iota(jnp.int32, (part, 128), 1)

    def to_row(column):
        return jnp.sum(jnp.where(eye, column, 0.0), axis=0, keepdims=True)

    def to_column(line):
        return jnp.sum(jnp.where(eye, line, 0.0), axis=1, keepdims=True)

    def local_norm(l, h, name, which, gain, shift):
        st_send, st_recv = halves[h]["st_send"], halves[h]["st_recv"]
        x = state[h * part:(h + 1) * part].astype(F32)
        c = jnp.sum(x, axis=1, keepdims=True) / width
        xc = x - c
        v = jnp.sum(xc * xc, axis=1, keepdims=True) / width
        sub = lax.broadcasted_iota(jnp.int32, (8, 128), 0)
        tile = jnp.where(sub == 0, to_row(c), jnp.where(sub == 1, to_row(v), 0.0))
        st_send[l, which] = tile
        if which == 0 and h == 0:
            pl.when(l == 0)(enter)
        for j in row_order:
            remote(h, name, 0, st_send.at[l, which], st_recv.at[l, which, row], "row", j).start()
        remote(h, name + "p", 0, st_send.at[l, which], st_recv.at[l, which, row], "row", partner).start()
        st_recv[l, which, row] = tile
        if which == 0 and h == 0:
            pl.when(l == 0)(rest_of_small)
        g, b = pick(gain, l), pick(shift, l)
        y = (xc * lax.rsqrt(v + EPS_LN) * g).astype(BF16)
        if h:
            return y
        extra = lax.broadcasted_iota(jnp.int32, (16, 1), 0)
        extra = jnp.where(extra == 0, g, jnp.where(extra == 1, b, 0.0))
        return jnp.concatenate([y, extra.astype(BF16)], axis=0)

    def scale_of(v):
        return (v + EPS_LN) * lax.rsqrt(v + EPS_LN)

    def global_norm(parts):
        m = sum(c for c, _ in parts) / len(parts)
        var = sum(v + (c - m) * (c - m) for c, v in parts) / len(parts)
        r = lax.rsqrt(var + EPS_LN)
        return [(to_column(r * scale_of(v)), to_column(r * (c - m))) for c, v in parts]

    def stats(l, h, which, j):
        tile = halves[h]["st_recv"][l, which, j]
        return tile[0:1], tile[1:2]

    def merge(one, two):
        half = 0.5 * (one[0] - two[0])
        return 0.5 * (one[0] + two[0]), 0.5 * (one[1] + two[1]) + half * half

    def pair_merge(l, h, which):
        here, there = stats(l, h, which, row), stats(l, h, which, partner)
        c_pair, v_pair = merge(here, there)
        r_pair = lax.rsqrt(v_pair + EPS_LN)
        a_own, a_got = to_column(r_pair * scale_of(here[1])), to_column(r_pair * scale_of(there[1]))
        d_own = to_column(r_pair * (here[0] - c_pair))

        def rows(own, other, g_own, g_other):
            return (a_own * own[:part] + a_got * other[:part]) + d_own * (g_own - g_other)

        return rows

    def pair_coefficients(l, h, which):
        return global_norm([merge(stats(l, h, which, 2 * k), stats(l, h, which, 2 * k + 1)) for k in range(n_chip)])

    def col_send(l, h, name, value):
        buf = halves[h][name]
        buf[l, col] = value.astype(BF16)
        for t in (2, 1, 3):
            remote(h, name, 0, buf.at[l, col], buf.at[l, col], "col", lax.rem(col + t, n_col)).start()

    def col_sum(l, h, name, bias):
        buf = halves[h][name]
        got(h, name, 0, buf.at[l, pl.ds(0, n_col - 1)], "col")
        total = buf[l, 0].astype(F32)
        for j in range(1, n_col):
            total = total + buf[l, j].astype(F32)
        rows = slice(h * part, (h + 1) * part)
        state[rows] = (state[rows].astype(F32) + (total + bias)).astype(BF16)
        sent(h, name, 0, buf.at[l, pl.ds(0, n_col - 1)], "col")

    def project(l, h):
        b = halves[h]
        y = local_norm(l, h, "st1", 0, g1, b1)
        if h == 0:
            big_copy(WQ, l).wait()
        res = jnp.dot(y, wq[l], preferred_element_type=F32).astype(BF16)
        for j in range(n_row):
            b["q_send"][l, j] = res[:, j * hd:(j + 1) * hd]
        for j in row_order + [partner]:
            remote(h, "q", 0, b["q_send"].at[l, j], b["q_recv"].at[l, row], "row", j).start()
        b["q_recv"][l, row] = b["q_send"][l, row]
        if h == 0:
            big_copy(WK, l).wait()
            big_copy(WV, l).wait()
        for w, (name, w_ref) in enumerate((("kd", wk), ("vd", wv))):
            res = jnp.dot(y, w_ref[l], preferred_element_type=F32)
            even = jnp.concatenate([res[:, 2 * k * hd:(2 * k + 1) * hd] for k in range(n_chip)], axis=1)
            odd = jnp.concatenate([res[:, (2 * k + 1) * hd:(2 * k + 2) * hd] for k in range(n_chip)], axis=1)
            b["kd_send"][l, w] = jnp.where(par == 0, odd, even).astype(BF16)
            remote(h, name, 0, b["kd_send"].at[l, w], b["kd_recv"].at[l, w], "row", partner).start()
            b["k_mine"][w] = jnp.where(par == 0, even, odd)

    def send_kv(l, h):
        b, first = halves[h], halves[0]
        got(h, "st1p", 0, b["st_recv"].at[l, 0, 0])
        merged = pair_merge(l, h, 0)
        for w, (d_name, name) in enumerate((("kd", "k"), ("vd", "v"))):
            got(h, d_name, 0, b["kd_recv"].at[l, w])
            own, other = b["k_mine"][w], b["kd_recv"][l, w].astype(F32)
            gb_own, gb_other = first["k_mine"][w, part:], first["kd_recv"][l, w, part:].astype(F32)
            both = merged(own, other, gb_own[0:1], gb_other[0:1])
            if h == 0:
                both = jnp.concatenate([both, gb_own + gb_other], axis=0)
            both = both.astype(BF16)
            for k in range(n_chip):
                b["k_send"][l, w, k] = both[:, k * hd:(k + 1) * hd]
            for off in offs[:-1]:
                k = chips[off]
                remote(h, name, 0, b["k_send"].at[l, w, k], b["k_recv"].at[l, w, chip], "row", 2 * k + par).start()
            b["k_recv"][l, w, chip] = b["k_send"][l, w, chip]

    def collect(parts, firsts, coefs, bias, l):
        total = pick_slice(bias, l, row * hd, hd)
        for value, first, (scale, shift) in zip(parts, firsts, coefs):
            gb = first.astype(F32)
            total = total + (scale * value[:part].astype(F32) + (shift * gb[0:1] + gb[1:2]))
        return total

    def attend(l, h):
        b, first = halves[h], halves[0]
        base = h * part
        got(h, "st1", 0, b["st_recv"].at[l, 0, pl.ds(0, n_row - 2)])
        coef = global_norm([stats(l, h, 0, j) for j in range(n_row)])
        coef_pair = pair_coefficients(l, h, 0)
        got(h, "q", 0, b["q_recv"].at[l, pl.ds(0, n_row - 1)])
        q = collect([b["q_recv"][l, j] for j in range(n_row)], [first["q_recv"][l, j, part:] for j in range(n_row)],
                    coef, bq, l)
        q = (q * (hd ** -0.5)).astype(BF16).astype(F32)
        group = 16
        rowi = lax.broadcasted_iota(jnp.int32, (group, 1), 0)
        if h == 0:
            big_copy(KC, l).wait()
        parts = []
        for g in range(part // group):
            q_g = q[g * group:(g + 1) * group]
            lhs = jnp.concatenate([jnp.where(rowi == i, q_g, 0.0) for i in range(group)], axis=1).astype(BF16)
            k_g = jnp.concatenate([kc[l, base + g * group + i] for i in range(group)], axis=1)
            parts.append(lax.dot_general(lhs, k_g, (((1,), (1,)), ((), ())), preferred_element_type=F32))
        scores = jnp.concatenate(parts, axis=0)
        spread = lax.broadcasted_iota(jnp.int32, (part, batch), 0) + base
        spread = spread == lax.broadcasted_iota(jnp.int32, (part, batch), 1)
        lens = jnp.sum(jnp.where(spread, len_v[...], 0), axis=1, keepdims=True)
        scores = jnp.where(lax.broadcasted_iota(jnp.int32, (part, keys), 1) < lens, scores, -jnp.inf)

        def fresh(w, name, bias):
            got(h, name, 0, b["k_recv"].at[l, w, pl.ds(0, n_chip - 1)])
            return collect([b["k_recv"][l, w, k] for k in range(n_chip)],
                           [first["k_recv"][l, w, k, part:] for k in range(n_chip)], coef_pair, bias, l).astype(BF16)

        k_new = fresh(0, "k", bk)
        s_new = jnp.sum(q * k_new.astype(F32), axis=1, keepdims=True)
        peak = jnp.maximum(jnp.max(scores, axis=1, keepdims=True), s_new)
        e = jnp.exp(scores - peak)
        e_new = jnp.exp(s_new - peak)
        mass = jnp.sum(e, axis=1, keepdims=True) + e_new
        prob = (e / mass).astype(BF16).astype(F32)
        prob_new = (e_new / mass).astype(BF16).astype(F32)
        if h == 0:
            big_copy(VC, l).wait()
        outs = []
        for g in range(part // group):
            p_g = prob[g * group:(g + 1) * group]
            lhs = jnp.concatenate([jnp.where(rowi // 2 == i, p_g, 0.0) for i in range(group // 2)],
                                  axis=1).astype(BF16)
            at = base + g * group
            v_g = jnp.concatenate([jnp.concatenate([vc[l, at + 2 * i], vc[l, at + 2 * i + 1]], axis=1)
                                   for i in range(group // 2)], axis=0)
            out = jnp.dot(lhs, v_g, preferred_element_type=F32)
            outs.append(jnp.where(rowi % 2 == 0, out[:, :hd], out[:, hd:]))
        v_new = fresh(1, "v", bv)
        mixed = jnp.concatenate(outs, axis=0) + prob_new * v_new.astype(F32)
        b["ag"][l, row] = mixed.astype(BF16)
        for j in row_order + [partner]:
            remote(h, "ag", 0, b["ag"].at[l, row], b["ag"].at[l, row], "row", j).start()
        b["kv_stage"][l, 0] = k_new
        b["kv_stage"][l, 1] = v_new
        kv_copy(l, h, 0).start()
        kv_copy(l, h, 1).start()

    def kv_copy(l, h, w):
        return pltpu.make_async_copy(halves[h]["kv_stage"].at[l, w], (k_out, v_out)[w].at[l, pl.ds(h * part, part)],
                                     out_sem.at[l, h, w])

    def out_product(l, h):
        ag = halves[h]["ag"]
        if h == 0:
            big_copy(WO, l).wait()
        got(h, "ag", 0, ag.at[l, pl.ds(0, n_row - 1)])
        gathered = jnp.concatenate([ag[l, j] for j in range(n_row)], axis=1)
        col_send(l, h, "wo", jnp.dot(gathered, wo[l], preferred_element_type=F32))

    def up(l, h):
        b, first = halves[h], halves[0]
        col_sum(l, h, "wo", pick(bo, l))
        y2 = local_norm(l, h, "st2", 1, g2, b2)
        if h == 0:
            big_copy(W1, l).wait()

        def block(j):
            return jnp.dot(y2, w1[l, :, pl.ds(pl.multiple_of(j * ffb, ffb), ffb)], preferred_element_type=F32)

        for some in (offs[:2], offs[2:]):
            blocks = [block(2 * chips[off] + 1 - par).astype(BF16) for off in some]
            for off, value in zip(some, blocks):
                b["fd_send"][l, chips[off]] = value
            for off in some:
                k = chips[off]
                remote(h, "fd", k, b["fd_send"].at[l, k], b["fd_recv"].at[l, k], "row", partner).start()
        blocks = [block(2 * chips[off] + par) for off in offs]
        for off, value in zip(offs, blocks):
            b["f_mine"][chips[off]] = value
        got(h, "st2p", 0, b["st_recv"].at[l, 1, 0])
        merged = pair_merge(l, h, 1)
        for off in offs:
            k = chips[off]
            got(h, "fd", k, b["fd_recv"].at[l, k])
            gb_own, gb_other = first["f_mine"][k, part:], first["fd_recv"][l, k, part:].astype(F32)
            both = merged(b["f_mine"][k], b["fd_recv"][l, k].astype(F32), gb_own[0:1], gb_other[0:1]).astype(BF16)
            if h == 0:
                gb = gb_own + gb_other
                gb = jnp.concatenate([gb[0:1], gb[1:2]], axis=1)
                tile = jnp.concatenate([gb[:, i * 128:(i + 1) * 128] for i in range(2 * lanes)], axis=0)
            if off:
                b["fi_send"][l, k] = both
                remote(h, "fi", 0, b["fi_send"].at[l, k], b["fi_recv"].at[l, chip], "row", 2 * k + par).start()
                if h == 0:
                    b["fg_send"][l, k] = tile
                    remote(h, "fg", 0, b["fg_send"].at[l, k], b["fg_recv"].at[l, chip], "row", 2 * k + par).start()
            else:
                b["fi_recv"][l, k] = both
                if h == 0:
                    b["fg_recv"][l, k] = tile

    def activate(l, h):
        b, first = halves[h], halves[0]
        ug = b["ug"]
        got(h, "st2", 0, b["st_recv"].at[l, 1, pl.ds(0, n_row - 2)])
        coef = pair_coefficients(l, h, 1)
        total = pick_slice(bf1, l, row * ffb, ffb)
        if h == 0:
            got(h, "fg", 0, b["fg_recv"].at[l, pl.ds(0, n_chip - 1)])
        got(h, "fi", 0, b["fi_recv"].at[l, pl.ds(0, n_chip - 1)])
        for k in range(n_chip):
            tile = first["fg_recv"][l, k]
            g = jnp.concatenate([tile[i:i + 1] for i in range(lanes)], axis=1)
            shift = jnp.concatenate([tile[lanes + i:lanes + i + 1] for i in range(lanes)], axis=1)
            total = total + (coef[k][0] * b["fi_recv"][l, k].astype(F32) + (coef[k][1] * g + shift))
        ug[l, row] = jnp.maximum(total.astype(BF16), 0)
        for off in offs[:-1]:
            remote(h, "ug", n_chip - off, ug.at[l, row], ug.at[l, row], "row", 2 * chips[off] + par).start()
        remote(h, "ug", 0, ug.at[l, row], ug.at[l, row], "row", partner).start()

    def same(off):
        return 2 * chips[off] + par

    def cross(off):
        return 2 * chips[off] + 1 - par

    def fc2_block(l, h, j):
        return jnp.dot(halves[h]["ug"][l, j], w2[l, pl.ds(pl.multiple_of(j * ffb, ffb), ffb), :],
                       preferred_element_type=F32)

    def pass_on(l, h, off):
        ug = halves[h]["ug"]
        got(h, "ug", off, ug.at[l, same(off)])
        remote(h, "ug", n_chip - 1 + off, ug.at[l, same(off)], ug.at[l, same(off)], "row", partner).start()

    def down_first(l, h):
        if h == 0:
            big_copy(W2, l).wait()
        got(h, "ug", 0, halves[h]["ug"].at[l, partner])
        halves[h]["acc"][...] = fc2_block(l, h, row) + fc2_block(l, h, partner)

    def down_near(l, h):
        pass_on(l, h, 1)
        pass_on(l, h, 3)
        acc = halves[h]["acc"]
        acc[...] = acc[...] + (fc2_block(l, h, same(1)) + fc2_block(l, h, same(3)))

    def down_far(l, h):
        ug, acc = halves[h]["ug"], halves[h]["acc"]
        pass_on(l, h, 2)
        got(h, "ug", n_chip, ug.at[l, cross(1)])
        got(h, "ug", n_chip + 2, ug.at[l, cross(3)])
        acc[...] = acc[...] + (fc2_block(l, h, same(2)) + fc2_block(l, h, cross(1)) + fc2_block(l, h, cross(3)))

    def down_last(l, h):
        got(h, "ug", n_chip + 1, halves[h]["ug"].at[l, cross(2)])
        col_send(l, h, "fo", halves[h]["acc"][...] + fc2_block(l, h, cross(2)))

    def drain(l, h):
        b = halves[h]
        for which, name in ((0, "st1"), (1, "st2")):
            sent(h, name, 0, b["st_recv"].at[l, which, pl.ds(0, n_row - 2)])
            sent(h, name + "p", 0, b["st_recv"].at[l, which, 0])
        sent(h, "q", 0, b["q_recv"].at[l, pl.ds(0, n_row - 1)])
        for w, (d, i) in enumerate((("kd", "k"), ("vd", "v"))):
            sent(h, d, 0, b["kd_send"].at[l, w])
            sent(h, i, 0, b["k_send"].at[l, w, pl.ds(0, n_chip - 1)])
        sent(h, "ag", 0, b["ag"].at[l, pl.ds(0, n_row - 1)])
        for k in range(n_chip):
            sent(h, "fd", k, b["fd_send"].at[l, k])
        sent(h, "fi", 0, b["fi_send"].at[l, pl.ds(0, n_chip - 1)])
        if h == 0:
            sent(h, "fg", 0, b["fg_send"].at[l, pl.ds(0, n_chip - 1)])
        for j in range(n_row - 1):
            sent(h, "ug", j, b["ug"].at[l, j])

    def layer(l, carry):
        for h in range(HALVES):
            pl.when(l > 0)(functools.partial(finish_layer, l - 1, h))
            project(l, h)
        pl.when(l == 0)(rest_of_bulk)
        for stage in (send_kv, attend, out_product, up, activate):
            for h in range(HALVES):
                stage(l, h)
        down_first(l, 0)
        down_first(l, 1)
        down_near(l, 0)
        down_far(l, 0)
        down_near(l, 1)
        down_last(l, 0)
        down_far(l, 1)
        down_last(l, 1)
        for h in range(HALVES):
            drain(l, h)
        return carry

    def finish_layer(l, h):
        col_sum(jnp.maximum(l, 0), h, "fo", pick(bf2, l))

    lax.fori_loop(0, n_layer, layer, 0)
    out_copies = [pltpu.make_async_copy(state.at[pl.ds(h * part, part)], h_out.at[pl.ds(h * part, part)],
                                        out_sem.at[0, h, 2]) for h in range(HALVES)]
    for h in range(HALVES):
        finish_layer(n_layer - 1, h)
        out_copies[h].start()
    for l in range(n_layer):
        for h in range(HALVES):
            kv_copy(l, h, 0).wait()
            kv_copy(l, h, 1).wait()
    for c in out_copies:
        c.wait()


def finish(h, k, v, h_out, k_out, v_out, h_v, k_v, v_v, sem_in, sem_out):
    loads = [pltpu.make_async_copy(s, d, sem_in.at[i]) for i, (s, d) in enumerate(((h, h_v), (k, k_v), (v, v_v)))]
    stores = [pltpu.make_async_copy(s, d, sem_out.at[i])
              for i, (s, d) in enumerate(((h_v, h_out), (k_v, k_out), (v_v, v_out)))]
    for c in loads:
        c.start()
    for c, d in zip(loads, stores):
        c.wait()
        d.start()
    for d in stores:
        d.wait()


def solution(mesh):
    n_row, n_col = mesh.shape["row"], mesh.shape["col"]
    n_chip = n_row // 2
    act_spec = P("dp", "row")
    cache_spec = P(None, "dp", ("col", "row"), None, None)
    fresh_spec = P(None, "dp", ("col", "row"), None)
    in_weight = P(None, "row", "col")
    out_weight = P(None, "col", "row")
    col_vec = P(None, "col")
    row_vec = P(None, "row")
    in_specs = (act_spec, P("dp"), cache_spec, cache_spec, row_vec, row_vec,
                in_weight, col_vec, in_weight, col_vec, in_weight, col_vec,
                out_weight, row_vec, row_vec, row_vec, in_weight, col_vec, out_weight, row_vec)

    def local_step(hidden, cache_len, k_cache, v_cache, ln1_g, ln1_b, w_q, b_q, w_k, b_k, w_v, b_v,
                   w_o, b_o, ln2_g, ln2_b, w_fc1, b_fc1, w_fc2, b_fc2):
        batch, width = hidden.shape
        n_layer, _, _, keys, hd = k_cache.shape
        ff = w_fc1.shape[2]
        ffb = ff // n_row
        table, n_sem = layout(n_chip)
        part = batch // HALVES
        args = (hidden, cache_len.reshape(1, batch), k_cache, v_cache, ln1_g, ln1_b, w_q, b_q, w_k, b_k, w_v, b_v,
                w_o, b_o, ln2_g, ln2_b, w_fc1, b_fc1, w_fc2, b_fc2)

        def vm(shape, dtype=BF16):
            return pltpu.VMEM(shape, dtype)

        local = [vm(a.shape, a.dtype) for a in args]
        local[2] = local[3] = vm((n_layer, batch, keys, hd))

        def half(h):
            rows = part + 16 if h == 0 else part
            gb = (n_layer, n_chip, 2 * ffb // 128, 128)
            shapes = dict(
                q_send=vm((n_layer, n_row, rows, hd)), q_recv=vm((n_layer, n_row, rows, hd)),
                kd_send=vm((n_layer, 2, rows, n_chip * hd)), kd_recv=vm((n_layer, 2, rows, n_chip * hd)),
                k_mine=vm((2, rows, n_chip * hd), F32),
                k_send=vm((n_layer, 2, n_chip, rows, hd)), k_recv=vm((n_layer, 2, n_chip, rows, hd)),
                kv_stage=vm((n_layer, 2, part, hd)), ag=vm((n_layer, n_row, part, hd)),
                st_send=vm((n_layer, 2, 8, 128), F32), st_recv=vm((n_layer, 2, n_row, 8, 128), F32),
                wo=vm((n_layer, n_col, part, width)), fo=vm((n_layer, n_col, part, width)),
                fd_send=vm((n_layer, n_chip, rows, ffb)), fd_recv=vm((n_layer, n_chip, rows, ffb)),
                f_mine=vm((n_chip, rows, ffb), F32),
                fi_send=vm((n_layer, n_chip, part, ffb)), fi_recv=vm((n_layer, n_chip, part, ffb)),
                ug=vm((n_layer, n_row, part, ffb)), acc=vm((part, width), F32))
            if h == 0:
                shapes.update(fg_send=vm(gb, F32), fg_recv=vm(gb, F32))
            return shapes

        dma = pltpu.SemaphoreType.DMA
        scratch = [local, [half(h) for h in range(HALVES)], vm((batch, width)),
                   [dma((12,)), dma((n_layer, 8)), dma((n_layer, HALVES, 3)), dma((n_sem,)), dma((n_sem,))]]
        out_shape = (jax.ShapeDtypeStruct((batch, width), BF16),
                     jax.ShapeDtypeStruct((n_layer, batch, hd), BF16),
                     jax.ShapeDtypeStruct((n_layer, batch, hd), BF16))
        h_out, k_new, v_new = pl.pallas_call(
            functools.partial(kernel, (n_layer, n_row, n_col, table)),
            out_shape=out_shape,
            in_specs=[pl.BlockSpec(memory_space=pl.ANY)] * len(args),
            out_specs=[pl.BlockSpec(memory_space=pl.ANY)] * 3,
            scratch_shapes=scratch,
            compiler_params=pltpu.CompilerParams(collective_id=0, has_side_effects=True,
                                                 vmem_limit_bytes=VLIM),
        )(*args)
        h_out, k_new, v_new = pl.pallas_call(
            finish, out_shape=out_shape,
            in_specs=[pl.BlockSpec(memory_space=pl.ANY)] * 3, out_specs=[pl.BlockSpec(memory_space=pl.ANY)] * 3,
            scratch_shapes=[vm(o.shape) for o in out_shape] + [pltpu.SemaphoreType.DMA((3,))] * 2,
        )(h_out, k_new, v_new)
        return h_out, k_new[:, :, None, :], v_new[:, :, None, :]

    return jax.shard_map(local_step, mesh=mesh, in_specs=in_specs,
                         out_specs=(act_spec, fresh_spec, fresh_spec), check_vma=False)
```

```python
import functools

import jax
import jax.numpy as jnp
from jax import lax
from jax.experimental import pallas as pl
from jax.experimental.pallas import tpu as pltpu
from jax.sharding import PartitionSpec as P

EPS_LN = 1e-5
VLIM = 64 * 1000 * 1000
MESH = pl.DeviceIdType.MESH
F32 = jnp.float32
BF16 = jnp.bfloat16


class Sems:
    def __init__(self):
        self.count = 0

    def take(self, n):
        base = self.count
        self.count += n
        return base


HALVES = 2


def layout():
    recv = dict(st1=1, st1p=1, st2=1, st2p=1, q=1, kd=1, vd=1, k=1, v=1, ag=1, wo=1, fd=2, fi=1, fg=1, ug=5, fo=1)
    send = dict(st1=1, st2=1, q=1, kd=1, k=1, ag=1, wo=1, fd=1, fi=1, fg=1, ug=1, fo=1)
    tables = []
    for names in (send, recv):
        sems = Sems()
        tables.append(([{name: sems.take(n) for name, n in names.items()} for _ in range(HALVES)], sems))
    return [t for t, _ in tables], [c.count for _, c in tables]


SENT_WITH = dict(st1p="st1", st2p="st2", vd="kd", v="k")


def kernel(dims, hid_hbm, len_hbm, kc_hbm, vc_hbm, g1_hbm, b1_hbm, wq_hbm, bq_hbm, wk_hbm, bk_hbm, wv_hbm, bv_hbm,
           wo_hbm, bo_hbm, g2_hbm, b2_hbm, w1_hbm, bf1_hbm, w2_hbm, bf2_hbm,
           h_out, k_out, v_out, local, halves, state, sem):
    n_layer, n_row, n_col, table = dims
    hid_v, len_v, kc, vc, g1, b1, wq, bq, wk, bk, wv, bv, wo, bo, g2, b2, w1, bf1, w2, bf2 = local
    small_sem, big_sem, ssem, rsem = sem
    n_chip = n_row // 2
    row = lax.axis_index("row")
    col = lax.axis_index("col")
    chip = row // 2
    par = row % 2
    partner = row + 1 - 2 * par
    batch, width = hid_v.shape
    part = batch // HALVES
    hd = kc.shape[-1]
    keys = kc.shape[2]
    ffb = w1.shape[-1] // n_row
    lanes = ffb // 128
    offs = [2, 1, 3, 0]
    chips = {off: lax.rem(chip + off, n_chip) for off in offs}
    row_order = []
    for off in offs[:-1]:
        row_order += [2 * chips[off] + par, 2 * chips[off] + 1 - par]

    barrier = pltpu.get_barrier_semaphore()
    for t in range(1, n_row):
        pl.semaphore_signal(barrier, inc=1, device_id={"row": lax.rem(row + t, n_row)}, device_id_type=MESH)
    for t in range(1, n_col):
        pl.semaphore_signal(barrier, inc=1, device_id={"col": lax.rem(col + t, n_col)}, device_id_type=MESH)

    small = [(hid_hbm, hid_v), (g1_hbm, g1), (b1_hbm, b1), (len_hbm, len_v), (bq_hbm, bq), (bk_hbm, bk),
             (bv_hbm, bv), (bo_hbm, bo), (g2_hbm, g2), (b2_hbm, b2), (bf1_hbm, bf1), (bf2_hbm, bf2)]
    small_copies = [pltpu.make_async_copy(s, d, small_sem.at[i]) for i, (s, d) in enumerate(small)]
    bigs = [(wq_hbm, wq), (wk_hbm, wk), (wv_hbm, wv), (kc_hbm, kc), (vc_hbm, vc), (wo_hbm, wo), (w1_hbm, w1),
            (w2_hbm, w2)]
    WQ, WK, WV, KC, VC, WO, W1, W2 = range(8)

    def big_copy(i, l):
        s, d = bigs[i]
        src = s.at[l, :, 0] if i in (KC, VC) else s.at[l]
        return pltpu.make_async_copy(src, d.at[l], big_sem.at[l, i])

    for c in small_copies[:3]:
        c.start()
    for i in (WQ, WK, WV):
        big_copy(i, 0).start()
    for c in small_copies[3:]:
        c.start()
    small_copies[0].wait()
    state[...] = hid_v[...]


    def enter():
        pl.semaphore_wait(barrier, n_row - 1 + n_col - 1)

    def norm_vectors():
        for c in small_copies[1:3]:
            c.wait()

    def rest_of_loads():
        for c in small_copies[3:]:
            c.wait()
        for i in (KC, VC, WO, W1, W2):
            big_copy(i, 0).start()
        for l in range(1, n_layer):
            for i in range(8):
                big_copy(i, l).start()

    def remote(h, name, i, src, dst, axis, target):
        return pltpu.make_async_remote_copy(
            src_ref=src, dst_ref=dst, send_sem=ssem.at[table[0][h][SENT_WITH.get(name, name)]],
            recv_sem=rsem.at[table[1][h][name] + i], device_id={axis: target}, device_id_type=MESH)

    def same_bytes(h, name, i, ref, axis):
        return remote(h, name, i, ref, ref, axis, partner if axis == "row" else lax.rem(col + 1, n_col))

    def got(h, name, i, ref, axis="row"):
        same_bytes(h, name, i, ref, axis).wait_recv()

    def sent(h, name, ref, axis="row"):
        same_bytes(h, name, 0, ref, axis).wait_send()

    def pick(ref, l):
        rows = ref[...].astype(F32)
        out = rows[0:1]
        for i in range(1, n_layer):
            out = jnp.where(l == i, rows[i:i + 1], out)
        return out

    def pick_slice(ref, l, start, size):
        rows = ref[:, pl.ds(pl.multiple_of(start, size), size)].astype(F32)
        out = rows[0:1]
        for i in range(1, n_layer):
            out = jnp.where(l == i, rows[i:i + 1], out)
        return out

    eye = lax.broadcasted_iota(jnp.int32, (part, 128), 0) == lax.broadcasted_iota(jnp.int32, (part, 128), 1)

    def to_row(column):
        return jnp.sum(jnp.where(eye, column, 0.0), axis=0, keepdims=True)

    def to_column(line):
        return jnp.sum(jnp.where(eye, line, 0.0), axis=1, keepdims=True)

    def local_norm(l, h, name, which, gain, shift, entering=False):
        st_send, st_recv = halves[h]["st_send"], halves[h]["st_recv"]
        x = state[h * part:(h + 1) * part].astype(F32)
        c = jnp.sum(x, axis=1, keepdims=True) / width
        xc = x - c
        v = jnp.sum(xc * xc, axis=1, keepdims=True) / width
        sub = lax.broadcasted_iota(jnp.int32, (8, 128), 0)
        tile = jnp.where(sub == 0, to_row(c), jnp.where(sub == 1, to_row(v), 0.0))
        st_send[l, which] = tile
        st_recv[l, which, row] = tile

        def send():
            for j in row_order:
                remote(h, name, 0, st_send.at[l, which], st_recv.at[l, which, row], "row", j).start()
            remote(h, name + "p", 0, st_send.at[l, which], st_recv.at[l, which, row], "row", partner).start()

        if entering:
            norm_vectors()
        else:
            send()
        g, b = pick(gain, l), pick(shift, l)
        y = (xc * lax.rsqrt(v + EPS_LN) * g).astype(BF16)
        if h:
            return y, send
        extra = lax.broadcasted_iota(jnp.int32, (16, 1), 0)
        extra = jnp.where(extra == 0, g, jnp.where(extra == 1, b, 0.0))
        return jnp.concatenate([y, extra.astype(BF16)], axis=0), send

    def scale_of(v):
        return (v + EPS_LN) * lax.rsqrt(v + EPS_LN)

    def global_norm(parts):
        m = sum(c for c, _ in parts) / len(parts)
        var = sum(v + (c - m) * (c - m) for c, v in parts) / len(parts)
        r = lax.rsqrt(var + EPS_LN)
        return [(to_column(r * scale_of(v)), to_column(r * (c - m))) for c, v in parts]

    def stats(l, h, which, j):
        tile = halves[h]["st_recv"][l, which, j]
        return tile[0:1], tile[1:2]

    def merge(one, two):
        half = 0.5 * (one[0] - two[0])
        return 0.5 * (one[0] + two[0]), 0.5 * (one[1] + two[1]) + half * half

    def pair_merge(l, h, which):
        here, there = stats(l, h, which, row), stats(l, h, which, partner)
        c_pair, v_pair = merge(here, there)
        r_pair = lax.rsqrt(v_pair + EPS_LN)
        a_own, a_got = to_column(r_pair * scale_of(here[1])), to_column(r_pair * scale_of(there[1]))
        d_own = to_column(r_pair * (here[0] - c_pair))

        def rows(own, other, g_own, g_other):
            return (a_own * own[:part] + a_got * other[:part]) + d_own * (g_own - g_other)

        return rows

    def pair_coefficients(l, h, which):
        return global_norm([merge(stats(l, h, which, 2 * k), stats(l, h, which, 2 * k + 1)) for k in range(n_chip)])

    def col_send(l, h, name, value):
        buf = halves[h][name]
        buf[l, col] = value.astype(BF16)
        for t in (2, 1, 3):
            remote(h, name, 0, buf.at[l, col], buf.at[l, col], "col", lax.rem(col + t, n_col)).start()

    def col_sum(l, h, name, bias):
        buf = halves[h][name]
        got(h, name, 0, buf.at[l, pl.ds(0, n_col - 1)], "col")
        total = buf[l, 0].astype(F32)
        for j in range(1, n_col):
            total = total + buf[l, j].astype(F32)
        rows = slice(h * part, (h + 1) * part)
        state[rows] = (state[rows].astype(F32) + (total + bias)).astype(BF16)
        sent(h, name, buf.at[l, pl.ds(0, n_col - 1)], "col")

    def project_q(l, h, entering=False):
        b = halves[h]
        y, send_stats = local_norm(l, h, "st1", 0, g1, b1, entering)
        if h == 0:
            big_copy(WQ, l).wait()
        res = jnp.dot(y, wq[l], preferred_element_type=F32).astype(BF16)
        for j in range(n_row):
            b["q_send"][l, j] = res[:, j * hd:(j + 1) * hd]
        b["y"][...] = y
        if entering:
            enter()
            send_stats()

    def send_q(l, h):
        b = halves[h]
        for j in row_order + [partner]:
            remote(h, "q", 0, b["q_send"].at[l, j], b["q_recv"].at[l, row], "row", j).start()
        b["q_recv"][l, row] = b["q_send"][l, row]

    def project_kv(l, h):
        b = halves[h]
        y = b["y"][...]
        if h == 0:
            big_copy(WK, l).wait()
            big_copy(WV, l).wait()
        for w, (name, w_ref) in enumerate((("kd", wk), ("vd", wv))):
            res = jnp.dot(y, w_ref[l], preferred_element_type=F32)
            even = jnp.concatenate([res[:, 2 * k * hd:(2 * k + 1) * hd] for k in range(n_chip)], axis=1)
            odd = jnp.concatenate([res[:, (2 * k + 1) * hd:(2 * k + 2) * hd] for k in range(n_chip)], axis=1)
            b["kd_send"][l, w] = jnp.where(par == 0, odd, even).astype(BF16)
            remote(h, name, 0, b["kd_send"].at[l, w], b["kd_recv"].at[l, w], "row", partner).start()
            b["k_mine"][w] = jnp.where(par == 0, even, odd)

    def send_kv(l, h):
        b, first = halves[h], halves[0]
        got(h, "st1p", 0, b["st_recv"].at[l, 0, 0])
        merged = pair_merge(l, h, 0)
        for w, (d_name, name) in enumerate((("kd", "k"), ("vd", "v"))):
            got(h, d_name, 0, b["kd_recv"].at[l, w])
            own, other = b["k_mine"][w], b["kd_recv"][l, w].astype(F32)
            gb_own, gb_other = first["k_mine"][w, part:], first["kd_recv"][l, w, part:].astype(F32)
            both = merged(own, other, gb_own[0:1], gb_other[0:1])
            if h == 0:
                both = jnp.concatenate([both, gb_own + gb_other], axis=0)
            both = both.astype(BF16)
            for k in range(n_chip):
                b["k_send"][l, w, k] = both[:, k * hd:(k + 1) * hd]
            for off in offs[:-1]:
                k = chips[off]
                remote(h, name, 0, b["k_send"].at[l, w, k], b["k_recv"].at[l, w, chip], "row", 2 * k + par).start()
            b["k_recv"][l, w, chip] = b["k_send"][l, w, chip]

    def collect(parts, firsts, coefs, bias, l):
        total = pick_slice(bias, l, row * hd, hd)
        for value, first, (scale, shift) in zip(parts, firsts, coefs):
            gb = first.astype(F32)
            total = total + (scale * value[:part].astype(F32) + (shift * gb[0:1] + gb[1:2]))
        return total

    def attend(l, h):
        b, first = halves[h], halves[0]
        base = h * part
        got(h, "st1", 0, b["st_recv"].at[l, 0, pl.ds(0, n_row - 2)])
        coef = global_norm([stats(l, h, 0, j) for j in range(n_row)])
        coef_pair = pair_coefficients(l, h, 0)
        got(h, "q", 0, b["q_recv"].at[l, pl.ds(0, n_row - 1)])
        q = collect([b["q_recv"][l, j] for j in range(n_row)], [first["q_recv"][l, j, part:] for j in range(n_row)],
                    coef, bq, l)
        q = (q * (hd ** -0.5)).astype(BF16).astype(F32)
        group = 16
        rowi = lax.broadcasted_iota(jnp.int32, (group, 1), 0)
        if h == 0:
            big_copy(KC, l).wait()
        parts = []
        for g in range(part // group):
            q_g = q[g * group:(g + 1) * group]
            lhs = jnp.concatenate([jnp.where(rowi == i, q_g, 0.0) for i in range(group)], axis=1).astype(BF16)
            k_g = jnp.concatenate([kc[l, base + g * group + i] for i in range(group)], axis=1)
            parts.append(lax.dot_general(lhs, k_g, (((1,), (1,)), ((), ())), preferred_element_type=F32))
        scores = jnp.concatenate(parts, axis=0)
        spread = lax.broadcasted_iota(jnp.int32, (part, batch), 0) + base
        spread = spread == lax.broadcasted_iota(jnp.int32, (part, batch), 1)
        lens = jnp.sum(jnp.where(spread, len_v[...], 0), axis=1, keepdims=True)
        scores = jnp.where(lax.broadcasted_iota(jnp.int32, (part, keys), 1) < lens, scores, -jnp.inf)

        def fresh(w, name, bias):
            got(h, name, 0, b["k_recv"].at[l, w, pl.ds(0, n_chip - 1)])
            return collect([b["k_recv"][l, w, k] for k in range(n_chip)],
                           [first["k_recv"][l, w, k, part:] for k in range(n_chip)], coef_pair, bias, l).astype(BF16)

        k_new = fresh(0, "k", bk)
        s_new = jnp.sum(q * k_new.astype(F32), axis=1, keepdims=True)
        peak = jnp.maximum(jnp.max(scores, axis=1, keepdims=True), s_new)
        e = jnp.exp(scores - peak)
        e_new = jnp.exp(s_new - peak)
        mass = jnp.sum(e, axis=1, keepdims=True) + e_new
        prob = (e / mass).astype(BF16).astype(F32)
        prob_new = (e_new / mass).astype(BF16).astype(F32)
        if h == 0:
            big_copy(VC, l).wait()
        outs = []
        for g in range(part // group):
            p_g = prob[g * group:(g + 1) * group]
            lhs = jnp.concatenate([jnp.where(rowi // 2 == i, p_g, 0.0) for i in range(group // 2)],
                                  axis=1).astype(BF16)
            at = base + g * group
            v_g = jnp.concatenate([jnp.concatenate([vc[l, at + 2 * i], vc[l, at + 2 * i + 1]], axis=1)
                                   for i in range(group // 2)], axis=0)
            out = jnp.dot(lhs, v_g, preferred_element_type=F32)
            outs.append(jnp.where(rowi % 2 == 0, out[:, :hd], out[:, hd:]))
        v_new = fresh(1, "v", bv)
        mixed = jnp.concatenate(outs, axis=0) + prob_new * v_new.astype(F32)
        b["ag"][l, row] = mixed.astype(BF16)
        for j in row_order + [partner]:
            remote(h, "ag", 0, b["ag"].at[l, row], b["ag"].at[l, row], "row", j).start()
        k_out[l, base:base + part] = k_new
        v_out[l, base:base + part] = v_new

    def out_product(l, h):
        ag = halves[h]["ag"]
        if h == 0:
            big_copy(WO, l).wait()
        got(h, "ag", 0, ag.at[l, pl.ds(0, n_row - 1)])
        gathered = jnp.concatenate([ag[l, j] for j in range(n_row)], axis=1)
        col_send(l, h, "wo", jnp.dot(gathered, wo[l], preferred_element_type=F32))

    def up(l, h):
        b, first = halves[h], halves[0]
        col_sum(l, h, "wo", pick(bo, l))
        y2, _ = local_norm(l, h, "st2", 1, g2, b2)
        if h == 0:
            big_copy(W1, l).wait()

        def block(j):
            return jnp.dot(y2, w1[l, :, pl.ds(pl.multiple_of(j * ffb, ffb), ffb)], preferred_element_type=F32)

        for some in (offs[:2], offs[2:]):
            blocks = [block(2 * chips[off] + 1 - par).astype(BF16) for off in some]
            for off, value in zip(some, blocks):
                b["fd_send"][l, chips[off]] = value
            for off in some:
                k = chips[off]
                remote(h, "fd", offs.index(off) // 2, b["fd_send"].at[l, k], b["fd_recv"].at[l, k], "row",
                       partner).start()
        blocks = [block(2 * chips[off] + par) for off in offs]
        for off, value in zip(offs, blocks):
            b["f_mine"][chips[off]] = value
        got(h, "st2p", 0, b["st_recv"].at[l, 1, 0])
        merged = pair_merge(l, h, 1)
        for off in offs:
            k = chips[off]
            if off in (offs[0], offs[2]):
                got(h, "fd", offs.index(off) // 2, b["fd_recv"].at[l, pl.ds(0, 2)])
            gb_own, gb_other = first["f_mine"][k, part:], first["fd_recv"][l, k, part:].astype(F32)
            both = merged(b["f_mine"][k], b["fd_recv"][l, k].astype(F32), gb_own[0:1], gb_other[0:1]).astype(BF16)
            if h == 0:
                gb = gb_own + gb_other
                gb = jnp.concatenate([gb[0:1], gb[1:2]], axis=1)
                tile = jnp.concatenate([gb[:, i * 128:(i + 1) * 128] for i in range(2 * lanes)], axis=0)
            if off:
                b["fi_send"][l, k] = both
                remote(h, "fi", 0, b["fi_send"].at[l, k], b["fi_recv"].at[l, chip], "row", 2 * k + par).start()
                if h == 0:
                    b["fg_send"][l, k] = tile
                    remote(h, "fg", 0, b["fg_send"].at[l, k], b["fg_recv"].at[l, chip], "row", 2 * k + par).start()
            else:
                b["fi_recv"][l, k] = both
                if h == 0:
                    b["fg_recv"][l, k] = tile

    def activate(l, h):
        b, first = halves[h], halves[0]
        ug = b["ug"]
        got(h, "st2", 0, b["st_recv"].at[l, 1, pl.ds(0, n_row - 2)])
        coef = pair_coefficients(l, h, 1)
        total = pick_slice(bf1, l, row * ffb, ffb)
        if h == 0:
            got(h, "fg", 0, b["fg_recv"].at[l, pl.ds(0, n_chip - 1)])
        got(h, "fi", 0, b["fi_recv"].at[l, pl.ds(0, n_chip - 1)])
        for k in range(n_chip):
            tile = first["fg_recv"][l, k]
            g = jnp.concatenate([tile[i:i + 1] for i in range(lanes)], axis=1)
            shift = jnp.concatenate([tile[lanes + i:lanes + i + 1] for i in range(lanes)], axis=1)
            total = total + (coef[k][0] * b["fi_recv"][l, k].astype(F32) + (coef[k][1] * g + shift))
        ug[l, row] = jnp.maximum(total.astype(BF16), 0)
        for off in offs[:-1]:
            remote(h, "ug", 2 - off % 2, ug.at[l, row], ug.at[l, row], "row", 2 * chips[off] + par).start()
        remote(h, "ug", 0, ug.at[l, row], ug.at[l, row], "row", partner).start()

    def same(off):
        return 2 * chips[off] + par

    def cross(off):
        return 2 * chips[off] + 1 - par

    def fc2_block(l, h, j):
        return jnp.dot(halves[h]["ug"][l, j], w2[l, pl.ds(pl.multiple_of(j * ffb, ffb), ffb), :],
                       preferred_element_type=F32)

    def pass_on(l, h, off):
        ug = halves[h]["ug"]
        remote(h, "ug", 4 - off % 2, ug.at[l, same(off)], ug.at[l, same(off)], "row", partner).start()

    def down_first(l, h):
        if h == 0:
            big_copy(W2, l).wait()
        got(h, "ug", 0, halves[h]["ug"].at[l, partner])
        halves[h]["acc"][...] = fc2_block(l, h, row) + fc2_block(l, h, partner)

    def down_near(l, h):
        got(h, "ug", 1, halves[h]["ug"].at[l, pl.ds(0, 2)])
        pass_on(l, h, 1)
        pass_on(l, h, 3)
        acc = halves[h]["acc"]
        acc[...] = acc[...] + (fc2_block(l, h, same(1)) + fc2_block(l, h, same(3)))

    def down_far(l, h):
        ug, acc = halves[h]["ug"], halves[h]["acc"]
        got(h, "ug", 2, ug.at[l, same(2)])
        pass_on(l, h, 2)
        got(h, "ug", 3, ug.at[l, pl.ds(0, 2)])
        acc[...] = acc[...] + (fc2_block(l, h, same(2)) + fc2_block(l, h, cross(1)) + fc2_block(l, h, cross(3)))

    def down_last(l, h):
        got(h, "ug", 4, halves[h]["ug"].at[l, cross(2)])
        col_send(l, h, "fo", halves[h]["acc"][...] + fc2_block(l, h, cross(2)))

    def drain(l, h):
        b = halves[h]
        for which, name in ((0, "st1"), (1, "st2")):
            sent(h, name, b["st_recv"].at[l, which, pl.ds(0, n_row - 1)])
        sent(h, "q", b["q_recv"].at[l, pl.ds(0, n_row - 1)])
        sent(h, "kd", b["kd_send"].at[l])
        sent(h, "k", b["k_send"].at[l, :, pl.ds(0, n_chip - 1)])
        sent(h, "ag", b["ag"].at[l, pl.ds(0, n_row - 1)])
        sent(h, "fd", b["fd_send"].at[l])
        sent(h, "fi", b["fi_send"].at[l, pl.ds(0, n_chip - 1)])
        if h == 0:
            sent(h, "fg", b["fg_send"].at[l, pl.ds(0, n_chip - 1)])
        sent(h, "ug", b["ug"].at[l, pl.ds(0, n_row - 1)])

    def layer(l, carry):
        def later():
            finish_layer(l - 1, 0)
            project_q(l, 0)

        pl.when(l > 0)(later)
        send_q(l, 0)
        project_kv(l, 0)
        pl.when(l > 0)(functools.partial(finish_layer, l - 1, 1))
        project_q(l, 1)
        send_q(l, 1)
        pl.when(l == 0)(rest_of_loads)
        send_kv(l, 0)
        project_kv(l, 1)
        send_kv(l, 1)
        for stage in (attend, out_product, up, activate, down_first):
            for h in range(HALVES):
                stage(l, h)
        down_near(l, 0)
        down_far(l, 0)
        down_last(l, 0)
        down_near(l, 1)
        down_far(l, 1)
        down_last(l, 1)
        for h in range(HALVES):
            drain(l, h)
        return carry

    def finish_layer(l, h):
        col_sum(jnp.maximum(l, 0), h, "fo", pick(bf2, l))

    project_q(0, 0, entering=True)
    lax.fori_loop(0, n_layer, layer, 0)
    for h in range(HALVES):
        finish_layer(n_layer - 1, h)
    h_out[...] = state[...]


def finish(h, k, v, h_out, k_out, v_out, sem):
    copies = [pltpu.make_async_copy(s, d, sem.at[i]) for i, (s, d) in enumerate(((h, h_out), (k, k_out), (v, v_out)))]
    for c in copies:
        c.start()
    for c in copies:
        c.wait()


def solution(mesh):
    n_row, n_col = mesh.shape["row"], mesh.shape["col"]
    n_chip = n_row // 2
    act_spec = P("dp", "row")
    cache_spec = P(None, "dp", ("col", "row"), None, None)
    fresh_spec = P(None, "dp", ("col", "row"), None)
    in_weight = P(None, "row", "col")
    out_weight = P(None, "col", "row")
    col_vec = P(None, "col")
    row_vec = P(None, "row")
    in_specs = (act_spec, P("dp"), cache_spec, cache_spec, row_vec, row_vec,
                in_weight, col_vec, in_weight, col_vec, in_weight, col_vec,
                out_weight, row_vec, row_vec, row_vec, in_weight, col_vec, out_weight, row_vec)

    def local_step(hidden, cache_len, k_cache, v_cache, ln1_g, ln1_b, w_q, b_q, w_k, b_k, w_v, b_v,
                   w_o, b_o, ln2_g, ln2_b, w_fc1, b_fc1, w_fc2, b_fc2):
        batch, width = hidden.shape
        n_layer, _, _, keys, hd = k_cache.shape
        ff = w_fc1.shape[2]
        ffb = ff // n_row
        table, n_sem = layout()
        part = batch // HALVES
        args = (hidden, cache_len.reshape(1, batch), k_cache, v_cache, ln1_g, ln1_b, w_q, b_q, w_k, b_k, w_v, b_v,
                w_o, b_o, ln2_g, ln2_b, w_fc1, b_fc1, w_fc2, b_fc2)

        def vm(shape, dtype=BF16):
            return pltpu.VMEM(shape, dtype)

        local = [vm(a.shape, a.dtype) for a in args]
        local[2] = local[3] = vm((n_layer, batch, keys, hd))

        def half(h):
            rows = part + 16 if h == 0 else part
            gb = (n_layer, n_chip, 2 * ffb // 128, 128)
            shapes = dict(
                q_send=vm((n_layer, n_row, rows, hd)), q_recv=vm((n_layer, n_row, rows, hd)),
                kd_send=vm((n_layer, 2, rows, n_chip * hd)), kd_recv=vm((n_layer, 2, rows, n_chip * hd)),
                k_mine=vm((2, rows, n_chip * hd), F32),
                k_send=vm((n_layer, 2, n_chip, rows, hd)), k_recv=vm((n_layer, 2, n_chip, rows, hd)),
                y=vm((rows, width)), ag=vm((n_layer, n_row, part, hd)),
                st_send=vm((n_layer, 2, 8, 128), F32), st_recv=vm((n_layer, 2, n_row, 8, 128), F32),
                wo=vm((n_layer, n_col, part, width)), fo=vm((n_layer, n_col, part, width)),
                fd_send=vm((n_layer, n_chip, rows, ffb)), fd_recv=vm((n_layer, n_chip, rows, ffb)),
                f_mine=vm((n_chip, rows, ffb), F32),
                fi_send=vm((n_layer, n_chip, part, ffb)), fi_recv=vm((n_layer, n_chip, part, ffb)),
                ug=vm((n_layer, n_row, part, ffb)), acc=vm((part, width), F32))
            if h == 0:
                shapes.update(fg_send=vm(gb, F32), fg_recv=vm(gb, F32))
            return shapes

        dma = pltpu.SemaphoreType.DMA
        scratch = [local, [half(h) for h in range(HALVES)], vm((batch, width)),
                   [dma((12,)), dma((n_layer, 8)), dma((n_sem[0],)), dma((n_sem[1],))]]
        out_shape = (jax.ShapeDtypeStruct((batch, width), BF16),
                     jax.ShapeDtypeStruct((n_layer, batch, hd), BF16),
                     jax.ShapeDtypeStruct((n_layer, batch, hd), BF16))
        kept = pl.pallas_call(
            functools.partial(kernel, (n_layer, n_row, n_col, table)),
            out_shape=[pltpu.VMEM(o.shape, o.dtype) for o in out_shape],
            in_specs=[pl.BlockSpec(memory_space=pl.ANY)] * len(args),
            out_specs=[pl.BlockSpec(memory_space=pltpu.VMEM)] * 3,
            scratch_shapes=scratch,
            compiler_params=pltpu.CompilerParams(collective_id=0, has_side_effects=True, vmem_limit_bytes=VLIM),
        )(*args)
        h_out, k_new, v_new = pl.pallas_call(
            finish, out_shape=out_shape,
            in_specs=[pl.BlockSpec(memory_space=pltpu.VMEM)] * 3, out_specs=[pl.BlockSpec(memory_space=pl.ANY)] * 3,
            scratch_shapes=[pltpu.SemaphoreType.DMA((3,))],
        )(*[pltpu.with_memory_space_constraint(o, pltpu.VMEM) for o in kept])
        return h_out, k_new[:, :, None, :], v_new[:, :, None, :]

    return jax.shard_map(local_step, mesh=mesh, in_specs=in_specs,
                         out_specs=(act_spec, fresh_spec, fresh_spec), check_vma=False)
```

```python
import functools

import jax
import jax.numpy as jnp
from jax import lax
from jax.experimental import pallas as pl
from jax.experimental.pallas import tpu as pltpu
from jax.sharding import PartitionSpec as P

EPS_LN = 1e-5
VLIM = 64 * 1000 * 1000
MESH = pl.DeviceIdType.MESH
F32 = jnp.float32
BF16 = jnp.bfloat16


class Sems:
    def __init__(self):
        self.count = 0

    def take(self, n):
        base = self.count
        self.count += n
        return base


HALVES = 2


def layout():
    recv = dict(st1=1, st1p=1, st2=1, st2p=1, q=1, vd=1, k=1, v=1, ag=1, wo=1, fd=2, fi=1, fg=1, ug=5, fo=1)
    send = dict(st1=1, st2=1, q=1, vd=1, k=1, v=1, ag=1, wo=1, fd=1, fi=1, fg=1, ug=1, fo=1)
    tables = []
    for names in (send, recv):
        sems = Sems()
        tables.append(([{name: sems.take(n) for name, n in names.items()} for _ in range(HALVES)], sems))
    return [t for t, _ in tables], [c.count for _, c in tables]


SENT_WITH = dict(st1p="st1", st2p="st2")


def kernel(dims, hid_hbm, len_hbm, kc_hbm, vc_hbm, g1_hbm, b1_hbm, wq_hbm, bq_hbm, wk_hbm, bk_hbm, wv_hbm, bv_hbm,
           wo_hbm, bo_hbm, g2_hbm, b2_hbm, w1_hbm, bf1_hbm, w2_hbm, bf2_hbm,
           h_out, k_out, v_out, local, halves, state, kt, sem):
    n_layer, n_row, n_col, table = dims
    hid_v, len_v, kc, vc, g1, b1, wq, bq, wk, bk, wv, bv, wo, bo, g2, b2, w1, bf1, w2, bf2 = local
    small_sem, big_sem, ssem, rsem = sem
    n_chip = n_row // 2
    row = lax.axis_index("row")
    col = lax.axis_index("col")
    chip = row // 2
    par = row % 2
    partner = row + 1 - 2 * par
    batch, width = hid_v.shape
    part = batch // HALVES
    hd = kc.shape[-1]
    keys = kc.shape[2]
    ffb = w1.shape[-1] // n_row
    lanes = ffb // 128
    offs = [2, 1, 3, 0]
    chips = {off: lax.rem(chip + off, n_chip) for off in offs}
    row_order = []
    for off in offs[:-1]:
        row_order += [2 * chips[off] + par, 2 * chips[off] + 1 - par]

    barrier = pltpu.get_barrier_semaphore()
    for t in range(1, n_row):
        pl.semaphore_signal(barrier, inc=1, device_id={"row": lax.rem(row + t, n_row)}, device_id_type=MESH)
    for t in range(1, n_col):
        pl.semaphore_signal(barrier, inc=1, device_id={"col": lax.rem(col + t, n_col)}, device_id_type=MESH)

    small = [(hid_hbm, hid_v), (g1_hbm, g1), (b1_hbm, b1), (len_hbm, len_v), (bq_hbm, bq), (bk_hbm, bk),
             (bv_hbm, bv), (bo_hbm, bo), (g2_hbm, g2), (b2_hbm, b2), (bf1_hbm, bf1), (bf2_hbm, bf2)]
    small_copies = [pltpu.make_async_copy(s, d, small_sem.at[i]) for i, (s, d) in enumerate(small)]
    bigs = [(wq_hbm, wq), (wk_hbm, wk), (wv_hbm, wv), (kc_hbm, kc), (vc_hbm, vc), (wo_hbm, wo), (w1_hbm, w1),
            (w2_hbm, w2)]
    WQ, WK, WV, KC, VC, WO, W1, W2 = range(8)

    def big_copy(i, l):
        s, d = bigs[i]
        src = s.at[l, :, 0] if i in (KC, VC) else s.at[l]
        return pltpu.make_async_copy(src, d.at[l], big_sem.at[l, i])

    for c in small_copies[:3]:
        c.start()
    for i in (WQ, WK, WV):
        big_copy(i, 0).start()
    for c in small_copies[3:]:
        c.start()
    small_copies[0].wait()
    state[...] = hid_v[...]


    def enter():
        pl.semaphore_wait(barrier, n_row - 1 + n_col - 1)

    def norm_vectors():
        for c in small_copies[1:3]:
            c.wait()

    def rest_of_loads():
        for c in small_copies[3:]:
            c.wait()
        for i in (KC, VC, WO, W1, W2):
            big_copy(i, 0).start()
        for l in range(1, n_layer):
            for i in range(8):
                big_copy(i, l).start()

    def remote(h, name, i, src, dst, axis, target):
        return pltpu.make_async_remote_copy(
            src_ref=src, dst_ref=dst, send_sem=ssem.at[table[0][h][SENT_WITH.get(name, name)]],
            recv_sem=rsem.at[table[1][h][name] + i], device_id={axis: target}, device_id_type=MESH)

    def same_bytes(h, name, i, ref, axis):
        return remote(h, name, i, ref, ref, axis, partner if axis == "row" else lax.rem(col + 1, n_col))

    def got(h, name, i, ref, axis="row"):
        same_bytes(h, name, i, ref, axis).wait_recv()

    def sent(h, name, ref, axis="row"):
        same_bytes(h, name, 0, ref, axis).wait_send()

    def pick(ref, l):
        rows = ref[...].astype(F32)
        out = rows[0:1]
        for i in range(1, n_layer):
            out = jnp.where(l == i, rows[i:i + 1], out)
        return out

    def pick_slice(ref, l, start, size):
        rows = ref[:, pl.ds(pl.multiple_of(start, size), size)].astype(F32)
        out = rows[0:1]
        for i in range(1, n_layer):
            out = jnp.where(l == i, rows[i:i + 1], out)
        return out

    eye = lax.broadcasted_iota(jnp.int32, (part, 128), 0) == lax.broadcasted_iota(jnp.int32, (part, 128), 1)

    def to_row(column):
        return jnp.sum(jnp.where(eye, column, 0.0), axis=0, keepdims=True)

    def to_column(line):
        return jnp.sum(jnp.where(eye, line, 0.0), axis=1, keepdims=True)

    def local_norm(l, h, name, which, gain, shift, entering=False):
        st_send, st_recv = halves[h]["st_send"], halves[h]["st_recv"]
        x = state[h * part:(h + 1) * part].astype(F32)
        c = jnp.sum(x, axis=1, keepdims=True) / width
        xc = x - c
        v = jnp.sum(xc * xc, axis=1, keepdims=True) / width
        sub = lax.broadcasted_iota(jnp.int32, (8, 128), 0)
        tile = jnp.where(sub == 0, to_row(c), jnp.where(sub == 1, to_row(v), 0.0))
        st_send[l, which] = tile
        st_recv[l, which, row] = tile

        def send():
            for j in row_order:
                remote(h, name, 0, st_send.at[l, which], st_recv.at[l, which, row], "row", j).start()
            remote(h, name + "p", 0, st_send.at[l, which], st_recv.at[l, which, row], "row", partner).start()

        if entering:
            norm_vectors()
        else:
            send()
        g, b = pick(gain, l), pick(shift, l)
        y = (xc * lax.rsqrt(v + EPS_LN) * g).astype(BF16)
        if h:
            return y, send
        extra = lax.broadcasted_iota(jnp.int32, (16, 1), 0)
        extra = jnp.where(extra == 0, g, jnp.where(extra == 1, b, 0.0))
        return jnp.concatenate([y, extra.astype(BF16)], axis=0), send

    def scale_of(v):
        return (v + EPS_LN) * lax.rsqrt(v + EPS_LN)

    def global_norm(parts):
        m = sum(c for c, _ in parts) / len(parts)
        var = sum(v + (c - m) * (c - m) for c, v in parts) / len(parts)
        r = lax.rsqrt(var + EPS_LN)
        return [(to_column(r * scale_of(v)), to_column(r * (c - m))) for c, v in parts]

    def stats(l, h, which, j):
        tile = halves[h]["st_recv"][l, which, j]
        return tile[0:1], tile[1:2]

    def merge(one, two):
        half = 0.5 * (one[0] - two[0])
        return 0.5 * (one[0] + two[0]), 0.5 * (one[1] + two[1]) + half * half

    def pair_merge(l, h, which):
        here, there = stats(l, h, which, row), stats(l, h, which, partner)
        c_pair, v_pair = merge(here, there)
        r_pair = lax.rsqrt(v_pair + EPS_LN)
        a_own, a_got = to_column(r_pair * scale_of(here[1])), to_column(r_pair * scale_of(there[1]))
        d_own = to_column(r_pair * (here[0] - c_pair))

        def rows(own, other, g_own, g_other):
            return (a_own * own[:part] + a_got * other[:part]) + d_own * (g_own - g_other)

        return rows

    def pair_coefficients(l, h, which):
        return global_norm([merge(stats(l, h, which, 2 * k), stats(l, h, which, 2 * k + 1)) for k in range(n_chip)])

    def col_send(l, h, name, value):
        buf = halves[h][name]
        buf[l, col] = value.astype(BF16)
        for t in (2, 1, 3):
            remote(h, name, 0, buf.at[l, col], buf.at[l, col], "col", lax.rem(col + t, n_col)).start()

    def col_sum(l, h, name, bias):
        buf = halves[h][name]
        got(h, name, 0, buf.at[l, pl.ds(0, n_col - 1)], "col")
        total = buf[l, 0].astype(F32)
        for j in range(1, n_col):
            total = total + buf[l, j].astype(F32)
        rows = slice(h * part, (h + 1) * part)
        state[rows] = (state[rows].astype(F32) + (total + bias)).astype(BF16)
        sent(h, name, buf.at[l, pl.ds(0, n_col - 1)], "col")

    def product(l, h, w, weight):
        b = halves[h]
        res = jnp.dot(b["y"][...], weight[l], preferred_element_type=F32).astype(BF16)
        for j in range(n_row):
            b["q_send"][l, w, j] = res[:, j * hd:(j + 1) * hd]

    def send_product(l, h, w):
        b = halves[h]
        for j in row_order + [partner]:
            remote(h, ("q", "k")[w], 0, b["q_send"].at[l, w, j], b["q_recv"].at[l, w, row], "row", j).start()
        b["q_recv"][l, w, row] = b["q_send"][l, w, row]

    def project_q(l, h, entering=False):
        y, send_stats = local_norm(l, h, "st1", 0, g1, b1, entering)
        halves[h]["y"][...] = y
        if h:
            project_v(l, h)
        if h == 0:
            big_copy(WQ, l).wait()
        product(l, h, 0, wq)
        if entering:
            enter()
            send_stats()

    def project_kv(l, h):
        b = halves[h]
        if h == 0:
            big_copy(WK, l).wait()
        product(l, h, 1, wk)
        send_product(l, h, 1)
        if h == 0:
            project_v(l, h)

    def project_v(l, h):
        b = halves[h]
        if h == 0:
            big_copy(WV, l).wait()
        res = jnp.dot(b["y"][...], wv[l], preferred_element_type=F32)
        even = jnp.concatenate([res[:, 2 * k * hd:(2 * k + 1) * hd] for k in range(n_chip)], axis=1)
        odd = jnp.concatenate([res[:, (2 * k + 1) * hd:(2 * k + 2) * hd] for k in range(n_chip)], axis=1)
        b["vd_send"][l] = jnp.where(par == 0, odd, even).astype(BF16)
        remote(h, "vd", 0, b["vd_send"].at[l], b["vd_recv"].at[l], "row", partner).start()
        b["v_mine"][...] = jnp.where(par == 0, even, odd)

    def send_v(l, h):
        b, first = halves[h], halves[0]
        got(h, "st1p", 0, b["st_recv"].at[l, 0, 0])
        merged = pair_merge(l, h, 0)
        got(h, "vd", 0, b["vd_recv"].at[l])
        own, other = b["v_mine"][...], b["vd_recv"][l].astype(F32)
        gb_own, gb_other = first["v_mine"][part:], first["vd_recv"][l, part:].astype(F32)
        both = merged(own, other, gb_own[0:1], gb_other[0:1])
        if h == 0:
            both = jnp.concatenate([both, gb_own + gb_other], axis=0)
        both = both.astype(BF16)
        for k in range(n_chip):
            b["v_send"][l, k] = both[:, k * hd:(k + 1) * hd]
        for off in offs[:-1]:
            k = chips[off]
            remote(h, "v", 0, b["v_send"].at[l, k], b["v_recv"].at[l, chip], "row", 2 * k + par).start()
        b["v_recv"][l, chip] = b["v_send"][l, chip]

    def collect(parts, firsts, coefs, bias, l):
        total = pick_slice(bias, l, row * hd, hd)
        for value, first, (scale, shift) in zip(parts, firsts, coefs):
            gb = first.astype(F32)
            total = total + (scale * value[:part].astype(F32) + (shift * gb[0:1] + gb[1:2]))
        return total

    def ready_q(l, h):
        b, first = halves[h], halves[0]
        got(h, "st1", 0, b["st_recv"].at[l, 0, pl.ds(0, n_row - 2)])
        coef = global_norm([stats(l, h, 0, j) for j in range(n_row)])
        coef_pair = pair_coefficients(l, h, 0)
        got(h, "q", 0, b["q_recv"].at[l, 0, pl.ds(0, n_row - 1)])
        q = collect([b["q_recv"][l, 0, j] for j in range(n_row)],
                    [first["q_recv"][l, 0, j, part:] for j in range(n_row)], coef, bq, l)
        b["q"][...] = (q * (hd ** -0.5)).astype(BF16).astype(F32)
        return coef, coef_pair

    def attend(l, h, coefs):
        coef, coef_pair = coefs
        b, first = halves[h], halves[0]
        base = h * part
        q = b["q"][...]
        group = 16
        rowi = lax.broadcasted_iota(jnp.int32, (group, 1), 0)
        parts = []
        for g in range(part // group):
            q_g = q[g * group:(g + 1) * group]
            lhs = jnp.concatenate([jnp.where(rowi == i, q_g, 0.0) for i in range(group)], axis=1).astype(BF16)
            k_g = jnp.concatenate([kt[base + g * group + i] for i in range(group)], axis=0)
            parts.append(jnp.dot(lhs, k_g, preferred_element_type=F32))
        scores = jnp.concatenate(parts, axis=0)
        spread = lax.broadcasted_iota(jnp.int32, (part, batch), 0) + base
        spread = spread == lax.broadcasted_iota(jnp.int32, (part, batch), 1)
        lens = jnp.sum(jnp.where(spread, len_v[...], 0), axis=1, keepdims=True)
        scores = jnp.where(lax.broadcasted_iota(jnp.int32, (part, keys), 1) < lens, scores, -jnp.inf)

        got(h, "k", 0, b["q_recv"].at[l, 1, pl.ds(0, n_row - 1)])
        k_new = collect([b["q_recv"][l, 1, j] for j in range(n_row)],
                        [first["q_recv"][l, 1, j, part:] for j in range(n_row)], coef, bk, l).astype(BF16)
        s_new = jnp.sum(q * k_new.astype(F32), axis=1, keepdims=True)
        peak = jnp.maximum(jnp.max(scores, axis=1, keepdims=True), s_new)
        e = jnp.exp(scores - peak)
        e_new = jnp.exp(s_new - peak)
        mass = jnp.sum(e, axis=1, keepdims=True) + e_new
        prob = (e / mass).astype(BF16).astype(F32)
        prob_new = (e_new / mass).astype(BF16).astype(F32)
        if h == 0:
            big_copy(VC, l).wait()
        outs = []
        for g in range(part // group):
            p_g = prob[g * group:(g + 1) * group]
            lhs = jnp.concatenate([jnp.where(rowi // 2 == i, p_g, 0.0) for i in range(group // 2)],
                                  axis=1).astype(BF16)
            at = base + g * group
            v_g = jnp.concatenate([jnp.concatenate([vc[l, at + 2 * i], vc[l, at + 2 * i + 1]], axis=1)
                                   for i in range(group // 2)], axis=0)
            out = jnp.dot(lhs, v_g, preferred_element_type=F32)
            outs.append(jnp.where(rowi % 2 == 0, out[:, :hd], out[:, hd:]))
        got(h, "v", 0, b["v_recv"].at[l, pl.ds(0, n_chip - 1)])
        v_new = collect([b["v_recv"][l, k] for k in range(n_chip)],
                        [first["v_recv"][l, k, part:] for k in range(n_chip)], coef_pair, bv, l).astype(BF16)
        mixed = jnp.concatenate(outs, axis=0) + prob_new * v_new.astype(F32)
        b["ag"][l, row] = mixed.astype(BF16)
        for j in row_order + [partner]:
            remote(h, "ag", 0, b["ag"].at[l, row], b["ag"].at[l, row], "row", j).start()
        k_out[l, base:base + part] = k_new
        v_out[l, base:base + part] = v_new

    def out_product(l, h):
        ag = halves[h]["ag"]
        if h == 0:
            big_copy(WO, l).wait()
        got(h, "ag", 0, ag.at[l, pl.ds(0, n_row - 1)])
        gathered = jnp.concatenate([ag[l, j] for j in range(n_row)], axis=1)
        col_send(l, h, "wo", jnp.dot(gathered, wo[l], preferred_element_type=F32))

    def up(l, h):
        b, first = halves[h], halves[0]
        col_sum(l, h, "wo", pick(bo, l))
        y2, _ = local_norm(l, h, "st2", 1, g2, b2)
        if h == 0:
            big_copy(W1, l).wait()

        def block(j):
            return jnp.dot(y2, w1[l, :, pl.ds(pl.multiple_of(j * ffb, ffb), ffb)], preferred_element_type=F32)

        for some in (offs[:2], offs[2:]):
            blocks = [block(2 * chips[off] + 1 - par).astype(BF16) for off in some]
            for off, value in zip(some, blocks):
                b["fd_send"][l, chips[off]] = value
            for off in some:
                k = chips[off]
                remote(h, "fd", offs.index(off) // 2, b["fd_send"].at[l, k], b["fd_recv"].at[l, k], "row",
                       partner).start()
        blocks = [block(2 * chips[off] + par) for off in offs[:-1]]
        for off, value in zip(offs, blocks):
            b["f_mine"][chips[off]] = value
        got(h, "st2p", 0, b["st_recv"].at[l, 1, 0])
        merged = pair_merge(l, h, 1)
        for off in offs:
            k = chips[off]
            if off == 0:
                b["f_mine"][k] = block(2 * k + par)
            if off in (offs[0], offs[2]):
                got(h, "fd", offs.index(off) // 2, b["fd_recv"].at[l, pl.ds(0, 2)])
            gb_own, gb_other = first["f_mine"][k, part:], first["fd_recv"][l, k, part:].astype(F32)
            both = merged(b["f_mine"][k], b["fd_recv"][l, k].astype(F32), gb_own[0:1], gb_other[0:1]).astype(BF16)
            if h == 0:
                gb = gb_own + gb_other
                gb = jnp.concatenate([gb[0:1], gb[1:2]], axis=1)
                tile = jnp.concatenate([gb[:, i * 128:(i + 1) * 128] for i in range(2 * lanes)], axis=0)
            if off:
                b["fi_send"][l, k] = both
                remote(h, "fi", 0, b["fi_send"].at[l, k], b["fi_recv"].at[l, chip], "row", 2 * k + par).start()
                if h == 0:
                    b["fg_send"][l, k] = tile
                    remote(h, "fg", 0, b["fg_send"].at[l, k], b["fg_recv"].at[l, chip], "row", 2 * k + par).start()
            else:
                b["fi_recv"][l, k] = both
                if h == 0:
                    b["fg_recv"][l, k] = tile

    def activate(l, h):
        b, first = halves[h], halves[0]
        ug = b["ug"]
        got(h, "st2", 0, b["st_recv"].at[l, 1, pl.ds(0, n_row - 2)])
        coef = pair_coefficients(l, h, 1)
        total = pick_slice(bf1, l, row * ffb, ffb)
        if h == 0:
            got(h, "fg", 0, b["fg_recv"].at[l, pl.ds(0, n_chip - 1)])
        got(h, "fi", 0, b["fi_recv"].at[l, pl.ds(0, n_chip - 1)])
        for k in range(n_chip):
            tile = first["fg_recv"][l, k]
            g = jnp.concatenate([tile[i:i + 1] for i in range(lanes)], axis=1)
            shift = jnp.concatenate([tile[lanes + i:lanes + i + 1] for i in range(lanes)], axis=1)
            total = total + (coef[k][0] * b["fi_recv"][l, k].astype(F32) + (coef[k][1] * g + shift))
        ug[l, row] = jnp.maximum(total.astype(BF16), 0)
        for off in offs[:-1]:
            remote(h, "ug", 2 - off % 2, ug.at[l, row], ug.at[l, row], "row", 2 * chips[off] + par).start()
        remote(h, "ug", 0, ug.at[l, row], ug.at[l, row], "row", partner).start()

    def same(off):
        return 2 * chips[off] + par

    def cross(off):
        return 2 * chips[off] + 1 - par

    def fc2_block(l, h, j):
        return jnp.dot(halves[h]["ug"][l, j], w2[l, pl.ds(pl.multiple_of(j * ffb, ffb), ffb), :],
                       preferred_element_type=F32)

    def pass_on(l, h, off):
        ug = halves[h]["ug"]
        remote(h, "ug", 4 - off % 2, ug.at[l, same(off)], ug.at[l, same(off)], "row", partner).start()

    def down_first(l, h):
        if h == 0:
            big_copy(W2, l).wait()
        got(h, "ug", 0, halves[h]["ug"].at[l, partner])
        halves[h]["acc"][...] = fc2_block(l, h, row) + fc2_block(l, h, partner)

    def down_near(l, h):
        got(h, "ug", 1, halves[h]["ug"].at[l, pl.ds(0, 2)])
        pass_on(l, h, 1)
        pass_on(l, h, 3)
        acc = halves[h]["acc"]
        acc[...] = acc[...] + (fc2_block(l, h, same(1)) + fc2_block(l, h, same(3)))

    def down_far(l, h):
        ug, acc = halves[h]["ug"], halves[h]["acc"]
        got(h, "ug", 2, ug.at[l, same(2)])
        pass_on(l, h, 2)
        got(h, "ug", 3, ug.at[l, pl.ds(0, 2)])
        acc[...] = acc[...] + (fc2_block(l, h, same(2)) + fc2_block(l, h, cross(1)) + fc2_block(l, h, cross(3)))

    def down_last(l, h):
        got(h, "ug", 4, halves[h]["ug"].at[l, cross(2)])
        col_send(l, h, "fo", halves[h]["acc"][...] + fc2_block(l, h, cross(2)))

    def drain(l, h):
        b = halves[h]
        for which, name in ((0, "st1"), (1, "st2")):
            sent(h, name, b["st_recv"].at[l, which, pl.ds(0, n_row - 1)])
        sent(h, "q", b["q_recv"].at[l, 0, pl.ds(0, n_row - 1)])
        sent(h, "k", b["q_recv"].at[l, 1, pl.ds(0, n_row - 1)])
        sent(h, "vd", b["vd_send"].at[l])
        sent(h, "v", b["v_send"].at[l, pl.ds(0, n_chip - 1)])
        sent(h, "ag", b["ag"].at[l, pl.ds(0, n_row - 1)])
        sent(h, "fd", b["fd_send"].at[l])
        sent(h, "fi", b["fi_send"].at[l, pl.ds(0, n_chip - 1)])
        if h == 0:
            sent(h, "fg", b["fg_send"].at[l, pl.ds(0, n_chip - 1)])
        sent(h, "ug", b["ug"].at[l, pl.ds(0, n_row - 1)])

    def turn_keys(l, h):
        step = 8

        def some(i, carry):
            for j in range(step):
                at = h * part + i * step + j
                kt[at] = kc[l, at].T
            return carry

        if h == 0:
            big_copy(KC, l).wait()
        lax.fori_loop(0, part // step, some, 0)

    def layer(l, carry):
        def later():
            finish_layer(l - 1, 0)
            project_q(l, 0)

        pl.when(l > 0)(later)
        send_product(l, 0, 0)
        project_kv(l, 0)
        pl.when(l == 0)(rest_of_loads)
        send_v(l, 0)
        for h in range(1, HALVES):
            pl.when(l > 0)(functools.partial(finish_layer, l - 1, h))
            project_q(l, h)
            send_product(l, h, 0)
            project_kv(l, h)
        pl.when(l == 0)(functools.partial(turn_keys, 0, 0))
        coefs = ready_q(l, 0)
        send_v(l, HALVES - 1)
        attend(l, 0, coefs)
        pl.when(l == 0)(functools.partial(turn_keys, 0, 1))
        for h in range(1, HALVES):
            attend(l, h, ready_q(l, h))
        for stage in (out_product, up, activate, down_first):
            for h in range(HALVES):
                stage(l, h)
        pl.when(l + 1 < n_layer)(lambda: turn_keys(l + 1, 0))
        for h in range(HALVES):
            down_near(l, h)
            down_far(l, h)
            down_last(l, h)
        for h in range(HALVES):
            drain(l, h)
        pl.when(l + 1 < n_layer)(lambda: turn_keys(l + 1, 1))
        return carry

    def finish_layer(l, h):
        col_sum(jnp.maximum(l, 0), h, "fo", pick(bf2, l))

    project_q(0, 0, entering=True)
    lax.fori_loop(0, n_layer, layer, 0)
    for h in range(HALVES):
        finish_layer(n_layer - 1, h)
    h_out[...] = state[...]


def finish(h, k, v, h_out, k_out, v_out, sem):
    copies = [pltpu.make_async_copy(s, d, sem.at[i]) for i, (s, d) in enumerate(((h, h_out), (k, k_out), (v, v_out)))]
    for c in copies:
        c.start()
    for c in copies:
        c.wait()


def solution(mesh):
    n_row, n_col = mesh.shape["row"], mesh.shape["col"]
    n_chip = n_row // 2
    act_spec = P("dp", "row")
    cache_spec = P(None, "dp", ("col", "row"), None, None)
    fresh_spec = P(None, "dp", ("col", "row"), None)
    in_weight = P(None, "row", "col")
    out_weight = P(None, "col", "row")
    col_vec = P(None, "col")
    row_vec = P(None, "row")
    in_specs = (act_spec, P("dp"), cache_spec, cache_spec, row_vec, row_vec,
                in_weight, col_vec, in_weight, col_vec, in_weight, col_vec,
                out_weight, row_vec, row_vec, row_vec, in_weight, col_vec, out_weight, row_vec)

    def local_step(hidden, cache_len, k_cache, v_cache, ln1_g, ln1_b, w_q, b_q, w_k, b_k, w_v, b_v,
                   w_o, b_o, ln2_g, ln2_b, w_fc1, b_fc1, w_fc2, b_fc2):
        batch, width = hidden.shape
        n_layer, _, _, keys, hd = k_cache.shape
        ff = w_fc1.shape[2]
        ffb = ff // n_row
        table, n_sem = layout()
        part = batch // HALVES
        args = (hidden, cache_len.reshape(1, batch), k_cache, v_cache, ln1_g, ln1_b, w_q, b_q, w_k, b_k, w_v, b_v,
                w_o, b_o, ln2_g, ln2_b, w_fc1, b_fc1, w_fc2, b_fc2)

        def vm(shape, dtype=BF16):
            return pltpu.VMEM(shape, dtype)

        local = [vm(a.shape, a.dtype) for a in args]
        local[2] = local[3] = vm((n_layer, batch, keys, hd))

        def half(h):
            rows = part + 16 if h == 0 else part
            gb = (n_layer, n_chip, 2 * ffb // 128, 128)
            shapes = dict(
                q_send=vm((n_layer, 2, n_row, rows, hd)), q_recv=vm((n_layer, 2, n_row, rows, hd)),
                vd_send=vm((n_layer, rows, n_chip * hd)), vd_recv=vm((n_layer, rows, n_chip * hd)),
                v_mine=vm((rows, n_chip * hd), F32),
                v_send=vm((n_layer, n_chip, rows, hd)), v_recv=vm((n_layer, n_chip, rows, hd)),
                y=vm((rows, width)), q=vm((part, hd), F32), ag=vm((n_layer, n_row, part, hd)),
                st_send=vm((n_layer, 2, 8, 128), F32), st_recv=vm((n_layer, 2, n_row, 8, 128), F32),
                wo=vm((n_layer, n_col, part, width)), fo=vm((n_layer, n_col, part, width)),
                fd_send=vm((n_layer, n_chip, rows, ffb)), fd_recv=vm((n_layer, n_chip, rows, ffb)),
                f_mine=vm((n_chip, rows, ffb), F32),
                fi_send=vm((n_layer, n_chip, part, ffb)), fi_recv=vm((n_layer, n_chip, part, ffb)),
                ug=vm((n_layer, n_row, part, ffb)), acc=vm((part, width), F32))
            if h == 0:
                shapes.update(fg_send=vm(gb, F32), fg_recv=vm(gb, F32))
            return shapes

        dma = pltpu.SemaphoreType.DMA
        scratch = [local, [half(h) for h in range(HALVES)], vm((batch, width)), vm((batch, hd, keys)),
                   [dma((12,)), dma((n_layer, 8)), dma((n_sem[0],)), dma((n_sem[1],))]]
        out_shape = (jax.ShapeDtypeStruct((batch, width), BF16),
                     jax.ShapeDtypeStruct((n_layer, batch, hd), BF16),
                     jax.ShapeDtypeStruct((n_layer, batch, hd), BF16))
        kept = pl.pallas_call(
            functools.partial(kernel, (n_layer, n_row, n_col, table)),
            out_shape=[pltpu.VMEM(o.shape, o.dtype) for o in out_shape],
            in_specs=[pl.BlockSpec(memory_space=pl.ANY)] * len(args),
            out_specs=[pl.BlockSpec(memory_space=pltpu.VMEM)] * 3,
            scratch_shapes=scratch,
            compiler_params=pltpu.CompilerParams(collective_id=0, has_side_effects=True, vmem_limit_bytes=VLIM),
        )(*args)
        h_out, k_new, v_new = pl.pallas_call(
            finish, out_shape=out_shape,
            in_specs=[pl.BlockSpec(memory_space=pltpu.VMEM)] * 3, out_specs=[pl.BlockSpec(memory_space=pl.ANY)] * 3,
            scratch_shapes=[pltpu.SemaphoreType.DMA((3,))],
        )(*[pltpu.with_memory_space_constraint(o, pltpu.VMEM) for o in kept])
        return h_out, k_new[:, :, None, :], v_new[:, :, None, :]

    return jax.shard_map(local_step, mesh=mesh, in_specs=in_specs,
                         out_specs=(act_spec, fresh_spec, fresh_spec), check_vma=False)
```

```python
import functools

import jax
import jax.numpy as jnp
from jax import lax
from jax.experimental import pallas as pl
from jax.experimental.pallas import tpu as pltpu
from jax.sharding import PartitionSpec as P

EPS_LN = 1e-5
VLIM = 64 * 1000 * 1000
MESH = pl.DeviceIdType.MESH
F32 = jnp.float32
BF16 = jnp.bfloat16


class Sems:
    def __init__(self):
        self.count = 0

    def take(self, n):
        base = self.count
        self.count += n
        return base


HALVES = 2


def layout():
    recv = dict(st1=1, st1p=1, st2=1, st2p=1, q=1, vd=1, k=1, v=1, ag=1, wo=1, fd=2, fi=1, fg=1, ug=5, fo=1)
    send = dict(st1=1, st2=1, q=1, vd=1, k=1, v=1, ag=1, wo=1, fd=1, fi=1, fg=1, ug=1, fo=1)
    tables = []
    for names in (send, recv):
        sems = Sems()
        tables.append(([{name: sems.take(n) for name, n in names.items()} for _ in range(HALVES)], sems))
    return [t for t, _ in tables], [c.count for _, c in tables]


SENT_WITH = dict(st1p="st1", st2p="st2")


def kernel(dims, hid_hbm, len_hbm, kc_hbm, vc_hbm, g1_hbm, b1_hbm, wq_hbm, bq_hbm, wk_hbm, bk_hbm, wv_hbm, bv_hbm,
           wo_hbm, bo_hbm, g2_hbm, b2_hbm, w1_hbm, bf1_hbm, w2_hbm, bf2_hbm,
           h_out, k_out, v_out, local, halves, state, kt, sem):
    n_layer, n_row, n_col, table = dims
    hid_v, len_v, kc, vc, g1, b1, wq, bq, wk, bk, wv, bv, wo, bo, g2, b2, w1, bf1, w2, bf2 = local
    small_sem, big_sem, ssem, rsem = sem
    n_chip = n_row // 2
    row = lax.axis_index("row")
    col = lax.axis_index("col")
    chip = row // 2
    par = row % 2
    partner = row + 1 - 2 * par
    batch, width = hid_v.shape
    part = batch // HALVES
    hd = kc.shape[-1]
    keys = kc.shape[2]
    ffb = w1.shape[-1] // n_row
    lanes = ffb // 128
    offs = [2, 1, 3, 0]
    chips = {off: lax.rem(chip + off, n_chip) for off in offs}
    row_order = []
    for off in offs[:-1]:
        row_order += [2 * chips[off] + par, 2 * chips[off] + 1 - par]

    barrier = pltpu.get_barrier_semaphore()
    for t in range(1, n_row):
        pl.semaphore_signal(barrier, inc=1, device_id={"row": lax.rem(row + t, n_row)}, device_id_type=MESH)
    for t in range(1, n_col):
        pl.semaphore_signal(barrier, inc=1, device_id={"col": lax.rem(col + t, n_col)}, device_id_type=MESH)

    small = [(hid_hbm, hid_v), (g1_hbm, g1), (b1_hbm, b1), (len_hbm, len_v), (bq_hbm, bq), (bk_hbm, bk),
             (bv_hbm, bv), (bo_hbm, bo), (g2_hbm, g2), (b2_hbm, b2), (bf1_hbm, bf1), (bf2_hbm, bf2)]
    small_copies = [pltpu.make_async_copy(s, d, small_sem.at[i]) for i, (s, d) in enumerate(small)]
    bigs = [(wq_hbm, wq), (wk_hbm, wk), (wv_hbm, wv), (kc_hbm, kc), (vc_hbm, vc), (wo_hbm, wo), (w1_hbm, w1),
            (w2_hbm, w2)]
    WQ, WK, WV, KC, VC, WO, W1, W2 = range(8)

    def big_copy(i, l):
        s, d = bigs[i]
        src = s.at[l, :, 0] if i in (KC, VC) else s.at[l]
        return pltpu.make_async_copy(src, d.at[l], big_sem.at[l, i])

    for c in small_copies[:3]:
        c.start()
    for i in (WQ, WK, WV):
        big_copy(i, 0).start()
    for c in small_copies[3:]:
        c.start()
    small_copies[0].wait()
    state[...] = hid_v[...]


    def enter():
        pl.semaphore_wait(barrier, n_row - 1 + n_col - 1)

    def norm_vectors():
        for c in small_copies[1:3]:
            c.wait()

    def rest_of_loads():
        for c in small_copies[3:]:
            c.wait()
        for i in (KC, VC, WO, W1, W2):
            big_copy(i, 0).start()
        for l in range(1, n_layer):
            for i in range(8):
                big_copy(i, l).start()

    def remote(h, name, i, src, dst, axis, target):
        return pltpu.make_async_remote_copy(
            src_ref=src, dst_ref=dst, send_sem=ssem.at[table[0][h][SENT_WITH.get(name, name)]],
            recv_sem=rsem.at[table[1][h][name] + i], device_id={axis: target}, device_id_type=MESH)

    def same_bytes(h, name, i, ref, axis):
        return remote(h, name, i, ref, ref, axis, partner if axis == "row" else lax.rem(col + 1, n_col))

    def got(h, name, i, ref, axis="row"):
        same_bytes(h, name, i, ref, axis).wait_recv()

    def sent(h, name, ref, axis="row"):
        same_bytes(h, name, 0, ref, axis).wait_send()

    def pick(ref, l):
        rows = ref[...].astype(F32)
        out = rows[0:1]
        for i in range(1, n_layer):
            out = jnp.where(l == i, rows[i:i + 1], out)
        return out

    def pick_slice(ref, l, start, size):
        rows = ref[:, pl.ds(pl.multiple_of(start, size), size)].astype(F32)
        out = rows[0:1]
        for i in range(1, n_layer):
            out = jnp.where(l == i, rows[i:i + 1], out)
        return out

    eye = lax.broadcasted_iota(jnp.int32, (part, 128), 0) == lax.broadcasted_iota(jnp.int32, (part, 128), 1)

    def to_row(column):
        return jnp.sum(jnp.where(eye, column, 0.0), axis=0, keepdims=True)

    def to_column(line):
        return jnp.sum(jnp.where(eye, line, 0.0), axis=1, keepdims=True)

    def local_norm(l, h, name, which, gain, shift, entering=False):
        st_send, st_recv = halves[h]["st_send"], halves[h]["st_recv"]
        x = state[h * part:(h + 1) * part].astype(F32)
        c = jnp.sum(x, axis=1, keepdims=True) / width
        xc = x - c
        v = jnp.sum(xc * xc, axis=1, keepdims=True) / width
        sub = lax.broadcasted_iota(jnp.int32, (8, 128), 0)
        tile = jnp.where(sub == 0, to_row(c), jnp.where(sub == 1, to_row(v), 0.0))
        st_send[l, which] = tile
        st_recv[l, which, row] = tile

        def send():
            for j in row_order:
                remote(h, name, 0, st_send.at[l, which], st_recv.at[l, which, row], "row", j).start()
            remote(h, name + "p", 0, st_send.at[l, which], st_recv.at[l, which, row], "row", partner).start()

        if entering:
            norm_vectors()
        else:
            send()
        g, b = pick(gain, l), pick(shift, l)
        y = (xc * lax.rsqrt(v + EPS_LN) * g).astype(BF16)
        if h:
            return y, send
        extra = lax.broadcasted_iota(jnp.int32, (16, 1), 0)
        extra = jnp.where(extra == 0, g, jnp.where(extra == 1, b, 0.0))
        return jnp.concatenate([y, extra.astype(BF16)], axis=0), send

    def scale_of(v):
        return (v + EPS_LN) * lax.rsqrt(v + EPS_LN)

    def global_norm(parts):
        m = sum(c for c, _ in parts) / len(parts)
        var = sum(v + (c - m) * (c - m) for c, v in parts) / len(parts)
        r = lax.rsqrt(var + EPS_LN)
        return [(to_column(r * scale_of(v)), to_column(r * (c - m))) for c, v in parts]

    def stats(l, h, which, j):
        tile = halves[h]["st_recv"][l, which, j]
        return tile[0:1], tile[1:2]

    def merge(one, two):
        half = 0.5 * (one[0] - two[0])
        return 0.5 * (one[0] + two[0]), 0.5 * (one[1] + two[1]) + half * half

    def pair_merge(l, h, which):
        here, there = stats(l, h, which, row), stats(l, h, which, partner)
        c_pair, v_pair = merge(here, there)
        r_pair = lax.rsqrt(v_pair + EPS_LN)
        a_own, a_got = to_column(r_pair * scale_of(here[1])), to_column(r_pair * scale_of(there[1]))
        d_own = to_column(r_pair * (here[0] - c_pair))

        def rows(own, other, g_own, g_other):
            return (a_own * own[:part] + a_got * other[:part]) + d_own * (g_own - g_other)

        return rows

    def pair_coefficients(l, h, which):
        return global_norm([merge(stats(l, h, which, 2 * k), stats(l, h, which, 2 * k + 1)) for k in range(n_chip)])

    def col_send(l, h, name, value):
        buf = halves[h][name]
        buf[l, col] = value.astype(BF16)
        for t in (2, 1, 3):
            remote(h, name, 0, buf.at[l, col], buf.at[l, col], "col", lax.rem(col + t, n_col)).start()

    def col_sum(l, h, name, bias):
        buf = halves[h][name]
        got(h, name, 0, buf.at[l, pl.ds(0, n_col - 1)], "col")
        total = buf[l, 0].astype(F32)
        for j in range(1, n_col):
            total = total + buf[l, j].astype(F32)
        rows = slice(h * part, (h + 1) * part)
        state[rows] = (state[rows].astype(F32) + (total + bias)).astype(BF16)
        sent(h, name, buf.at[l, pl.ds(0, n_col - 1)], "col")

    def product(l, h, w, weight):
        b = halves[h]
        res = jnp.dot(b["y"][...], weight[l], preferred_element_type=F32).astype(BF16)
        for j in range(n_row):
            b["q_send"][l, w, j] = res[:, j * hd:(j + 1) * hd]

    def send_product(l, h, w):
        b = halves[h]
        for j in row_order + [partner]:
            remote(h, ("q", "k")[w], 0, b["q_send"].at[l, w, j], b["q_recv"].at[l, w, row], "row", j).start()
        b["q_recv"][l, w, row] = b["q_send"][l, w, row]

    def project_q(l, h, entering=False):
        y, send_stats = local_norm(l, h, "st1", 0, g1, b1, entering)
        halves[h]["y"][...] = y
        if h:
            project_v(l, h)
        if h == 0:
            big_copy(WQ, l).wait()
        product(l, h, 0, wq)
        if entering:
            enter()
            send_stats()

    def project_kv(l, h):
        b = halves[h]
        if h == 0:
            big_copy(WK, l).wait()
        product(l, h, 1, wk)
        send_product(l, h, 1)
        if h == 0:
            project_v(l, h)

    def project_v(l, h):
        b = halves[h]
        if h == 0:
            big_copy(WV, l).wait()
        res = jnp.dot(b["y"][...], wv[l], preferred_element_type=F32)
        even = jnp.concatenate([res[:, 2 * k * hd:(2 * k + 1) * hd] for k in range(n_chip)], axis=1)
        odd = jnp.concatenate([res[:, (2 * k + 1) * hd:(2 * k + 2) * hd] for k in range(n_chip)], axis=1)
        b["vd_send"][l] = jnp.where(par == 0, odd, even).astype(BF16)
        remote(h, "vd", 0, b["vd_send"].at[l], b["vd_recv"].at[l], "row", partner).start()
        b["v_mine"][...] = jnp.where(par == 0, even, odd)

    def send_v(l, h):
        b, first = halves[h], halves[0]
        got(h, "st1p", 0, b["st_recv"].at[l, 0, 0])
        merged = pair_merge(l, h, 0)
        got(h, "vd", 0, b["vd_recv"].at[l])
        own, other = b["v_mine"][...], b["vd_recv"][l].astype(F32)
        gb_own, gb_other = first["v_mine"][part:], first["vd_recv"][l, part:].astype(F32)
        both = merged(own, other, gb_own[0:1], gb_other[0:1])
        if h == 0:
            both = jnp.concatenate([both, gb_own + gb_other], axis=0)
        both = both.astype(BF16)
        for k in range(n_chip):
            b["v_send"][l, k] = both[:, k * hd:(k + 1) * hd]
        for off in offs[:-1]:
            k = chips[off]
            remote(h, "v", 0, b["v_send"].at[l, k], b["v_recv"].at[l, chip], "row", 2 * k + par).start()
        b["v_recv"][l, chip] = b["v_send"][l, chip]

    def collect(parts, firsts, coefs, bias, l):
        total = pick_slice(bias, l, row * hd, hd)
        for value, first, (scale, shift) in zip(parts, firsts, coefs):
            gb = first.astype(F32)
            total = total + (scale * value[:part].astype(F32) + (shift * gb[0:1] + gb[1:2]))
        return total

    def ready_q(l, h):
        b, first = halves[h], halves[0]
        got(h, "st1", 0, b["st_recv"].at[l, 0, pl.ds(0, n_row - 2)])
        coef = global_norm([stats(l, h, 0, j) for j in range(n_row)])
        coef_pair = pair_coefficients(l, h, 0)
        got(h, "q", 0, b["q_recv"].at[l, 0, pl.ds(0, n_row - 1)])
        q = collect([b["q_recv"][l, 0, j] for j in range(n_row)],
                    [first["q_recv"][l, 0, j, part:] for j in range(n_row)], coef, bq, l)
        b["q"][...] = (q * (hd ** -0.5)).astype(BF16).astype(F32)
        return coef, coef_pair

    def attend(l, h, coefs):
        coef, coef_pair = coefs
        b, first = halves[h], halves[0]
        base = h * part
        q = b["q"][...]
        group = 16
        rowi = lax.broadcasted_iota(jnp.int32, (group, 1), 0)
        parts = []
        for g in range(part // group):
            q_g = q[g * group:(g + 1) * group]
            lhs = jnp.concatenate([jnp.where(rowi == i, q_g, 0.0) for i in range(group)], axis=1).astype(BF16)
            k_g = jnp.concatenate([kt[base + g * group + i] for i in range(group)], axis=0)
            parts.append(jnp.dot(lhs, k_g, preferred_element_type=F32))
        scores = jnp.concatenate(parts, axis=0)
        spread = lax.broadcasted_iota(jnp.int32, (part, batch), 0) + base
        spread = spread == lax.broadcasted_iota(jnp.int32, (part, batch), 1)
        lens = jnp.sum(jnp.where(spread, len_v[...], 0), axis=1, keepdims=True)
        scores = jnp.where(lax.broadcasted_iota(jnp.int32, (part, keys), 1) < lens, scores, -jnp.inf)

        got(h, "k", 0, b["q_recv"].at[l, 1, pl.ds(0, n_row - 1)])
        k_new = collect([b["q_recv"][l, 1, j] for j in range(n_row)],
                        [first["q_recv"][l, 1, j, part:] for j in range(n_row)], coef, bk, l).astype(BF16)
        s_new = jnp.sum(q * k_new.astype(F32), axis=1, keepdims=True)
        peak = jnp.maximum(jnp.max(scores, axis=1, keepdims=True), s_new)
        e = jnp.exp(scores - peak)
        e_new = jnp.exp(s_new - peak)
        mass = jnp.sum(e, axis=1, keepdims=True) + e_new
        prob = (e / mass).astype(BF16).astype(F32)
        prob_new = (e_new / mass).astype(BF16).astype(F32)
        if h == 0:
            big_copy(VC, l).wait()
        outs = []
        for g in range(part // group):
            p_g = prob[g * group:(g + 1) * group]
            lhs = jnp.concatenate([jnp.where(rowi // 2 == i, p_g, 0.0) for i in range(group // 2)],
                                  axis=1).astype(BF16)
            at = base + g * group
            v_g = jnp.concatenate([jnp.concatenate([vc[l, at + 2 * i], vc[l, at + 2 * i + 1]], axis=1)
                                   for i in range(group // 2)], axis=0)
            out = jnp.dot(lhs, v_g, preferred_element_type=F32)
            outs.append(jnp.where(rowi % 2 == 0, out[:, :hd], out[:, hd:]))
        got(h, "v", 0, b["v_recv"].at[l, pl.ds(0, n_chip - 1)])
        v_new = collect([b["v_recv"][l, k] for k in range(n_chip)],
                        [first["v_recv"][l, k, part:] for k in range(n_chip)], coef_pair, bv, l).astype(BF16)
        mixed = jnp.concatenate(outs, axis=0) + prob_new * v_new.astype(F32)
        b["ag"][l, row] = mixed.astype(BF16)
        for j in row_order + [partner]:
            remote(h, "ag", 0, b["ag"].at[l, row], b["ag"].at[l, row], "row", j).start()
        k_out[l, base:base + part] = k_new
        v_out[l, base:base + part] = v_new

    def out_product(l, h):
        ag = halves[h]["ag"]
        if h == 0:
            big_copy(WO, l).wait()
        got(h, "ag", 0, ag.at[l, pl.ds(0, n_row - 1)])
        gathered = jnp.concatenate([ag[l, j] for j in range(n_row)], axis=1)
        col_send(l, h, "wo", jnp.dot(gathered, wo[l], preferred_element_type=F32))

    def up(l, h):
        b, first = halves[h], halves[0]
        col_sum(l, h, "wo", pick(bo, l))
        y2, _ = local_norm(l, h, "st2", 1, g2, b2)
        if h == 0:
            big_copy(W1, l).wait()

        def block(j):
            return jnp.dot(y2, w1[l, :, pl.ds(pl.multiple_of(j * ffb, ffb), ffb)], preferred_element_type=F32)

        for some in (offs[:2], offs[2:]):
            blocks = [block(2 * chips[off] + 1 - par).astype(BF16) for off in some]
            for off, value in zip(some, blocks):
                b["fd_send"][l, chips[off]] = value
            for off in some:
                k = chips[off]
                remote(h, "fd", offs.index(off) // 2, b["fd_send"].at[l, k], b["fd_recv"].at[l, k], "row",
                       partner).start()
        blocks = [block(2 * chips[off] + par) for off in offs[:-1]]
        for off, value in zip(offs, blocks):
            b["f_mine"][chips[off]] = value
        got(h, "st2p", 0, b["st_recv"].at[l, 1, 0])
        merged = pair_merge(l, h, 1)
        for off in offs:
            k = chips[off]
            if off == 0:
                b["f_mine"][k] = block(2 * k + par)
            if off in (offs[0], offs[2]):
                got(h, "fd", offs.index(off) // 2, b["fd_recv"].at[l, pl.ds(0, 2)])
            gb_own, gb_other = first["f_mine"][k, part:], first["fd_recv"][l, k, part:].astype(F32)
            both = merged(b["f_mine"][k], b["fd_recv"][l, k].astype(F32), gb_own[0:1], gb_other[0:1]).astype(BF16)
            if h == 0:
                gb = gb_own + gb_other
                gb = jnp.concatenate([gb[0:1], gb[1:2]], axis=1)
                tile = jnp.concatenate([gb[:, i * 128:(i + 1) * 128] for i in range(2 * lanes)], axis=0)
            if off:
                b["fi_send"][l, k] = both
                remote(h, "fi", 0, b["fi_send"].at[l, k], b["fi_recv"].at[l, chip], "row", 2 * k + par).start()
                if h == 0:
                    b["fg_send"][l, k] = tile
                    remote(h, "fg", 0, b["fg_send"].at[l, k], b["fg_recv"].at[l, chip], "row", 2 * k + par).start()
            else:
                b["fi_recv"][l, k] = both
                if h == 0:
                    b["fg_recv"][l, k] = tile

    def activate(l, h):
        b, first = halves[h], halves[0]
        ug = b["ug"]
        got(h, "st2", 0, b["st_recv"].at[l, 1, pl.ds(0, n_row - 2)])
        coef = pair_coefficients(l, h, 1)
        total = pick_slice(bf1, l, row * ffb, ffb)
        if h == 0:
            got(h, "fg", 0, b["fg_recv"].at[l, pl.ds(0, n_chip - 1)])
        got(h, "fi", 0, b["fi_recv"].at[l, pl.ds(0, n_chip - 1)])
        for k in range(n_chip):
            tile = first["fg_recv"][l, k]
            g = jnp.concatenate([tile[i:i + 1] for i in range(lanes)], axis=1)
            shift = jnp.concatenate([tile[lanes + i:lanes + i + 1] for i in range(lanes)], axis=1)
            total = total + (coef[k][0] * b["fi_recv"][l, k].astype(F32) + (coef[k][1] * g + shift))
        ug[l, row] = jnp.maximum(total.astype(BF16), 0)
        for off in offs[:-1]:
            remote(h, "ug", 2 - off % 2, ug.at[l, row], ug.at[l, row], "row", 2 * chips[off] + par).start()
        remote(h, "ug", 0, ug.at[l, row], ug.at[l, row], "row", partner).start()

    def same(off):
        return 2 * chips[off] + par

    def cross(off):
        return 2 * chips[off] + 1 - par

    def fc2_block(l, h, j):
        return jnp.dot(halves[h]["ug"][l, j], w2[l, pl.ds(pl.multiple_of(j * ffb, ffb), ffb), :],
                       preferred_element_type=F32)

    def pass_on(l, h, off):
        ug = halves[h]["ug"]
        remote(h, "ug", 4 - off % 2, ug.at[l, same(off)], ug.at[l, same(off)], "row", partner).start()

    def down_first(l, h):
        if h == 0:
            big_copy(W2, l).wait()
        got(h, "ug", 0, halves[h]["ug"].at[l, partner])
        halves[h]["acc"][...] = fc2_block(l, h, row) + fc2_block(l, h, partner)

    def down_near(l, h):
        got(h, "ug", 1, halves[h]["ug"].at[l, pl.ds(0, 2)])
        pass_on(l, h, 1)
        pass_on(l, h, 3)
        acc = halves[h]["acc"]
        acc[...] = acc[...] + (fc2_block(l, h, same(1)) + fc2_block(l, h, same(3)))

    def down_far(l, h):
        ug, acc = halves[h]["ug"], halves[h]["acc"]
        got(h, "ug", 2, ug.at[l, same(2)])
        pass_on(l, h, 2)
        got(h, "ug", 3, ug.at[l, pl.ds(0, 2)])
        acc[...] = acc[...] + (fc2_block(l, h, same(2)) + fc2_block(l, h, cross(1)) + fc2_block(l, h, cross(3)))

    def down_last(l, h):
        got(h, "ug", 4, halves[h]["ug"].at[l, cross(2)])
        col_send(l, h, "fo", halves[h]["acc"][...] + fc2_block(l, h, cross(2)))

    def drain(l, h):
        b = halves[h]
        for which, name in ((0, "st1"), (1, "st2")):
            sent(h, name, b["st_recv"].at[l, which, pl.ds(0, n_row - 1)])
        sent(h, "q", b["q_recv"].at[l, 0, pl.ds(0, n_row - 1)])
        sent(h, "k", b["q_recv"].at[l, 1, pl.ds(0, n_row - 1)])
        sent(h, "vd", b["vd_send"].at[l])
        sent(h, "v", b["v_send"].at[l, pl.ds(0, n_chip - 1)])
        sent(h, "ag", b["ag"].at[l, pl.ds(0, n_row - 1)])
        sent(h, "fd", b["fd_send"].at[l])
        sent(h, "fi", b["fi_send"].at[l, pl.ds(0, n_chip - 1)])
        if h == 0:
            sent(h, "fg", b["fg_send"].at[l, pl.ds(0, n_chip - 1)])
        sent(h, "ug", b["ug"].at[l, pl.ds(0, n_row - 1)])

    def turn_keys(l, h):
        step = 16

        def some(i, carry):
            for j in range(step):
                at = h * part + i * step + j
                kt[at] = kc[l, at].T
            return carry

        if h == 0:
            big_copy(KC, l).wait()
        lax.fori_loop(0, part // step, some, 0)

    def layer(l, carry):
        def later():
            finish_layer(l - 1, 0)
            project_q(l, 0)

        pl.when(l > 0)(later)
        send_product(l, 0, 0)
        project_kv(l, 0)
        pl.when(l == 0)(rest_of_loads)
        send_v(l, 0)
        for h in range(1, HALVES):
            pl.when(l > 0)(functools.partial(finish_layer, l - 1, h))
            project_q(l, h)
            send_product(l, h, 0)
            project_kv(l, h)
        pl.when(l == 0)(functools.partial(turn_keys, 0, 0))
        coefs = ready_q(l, 0)
        send_v(l, HALVES - 1)
        attend(l, 0, coefs)
        pl.when(l == 0)(functools.partial(turn_keys, 0, 1))
        for h in range(1, HALVES):
            attend(l, h, ready_q(l, h))
        for stage in (out_product, up, activate, down_first):
            for h in range(HALVES):
                stage(l, h)
        pl.when(l + 1 < n_layer)(lambda: turn_keys(l + 1, 0))
        for h in range(HALVES):
            down_near(l, h)
            down_far(l, h)
            down_last(l, h)
        for h in range(HALVES):
            drain(l, h)
        pl.when(l + 1 < n_layer)(lambda: turn_keys(l + 1, 1))
        return carry

    def finish_layer(l, h):
        col_sum(jnp.maximum(l, 0), h, "fo", pick(bf2, l))

    project_q(0, 0, entering=True)
    lax.fori_loop(0, n_layer, layer, 0)
    for h in range(HALVES):
        finish_layer(n_layer - 1, h)
    h_out[...] = state[...]


def finish(h, k, v, h_out, k_out, v_out, sem):
    copies = [pltpu.make_async_copy(s, d, sem.at[i]) for i, (s, d) in enumerate(((h, h_out), (k, k_out), (v, v_out)))]
    for c in copies:
        c.start()
    for c in copies:
        c.wait()


def solution(mesh):
    n_row, n_col = mesh.shape["row"], mesh.shape["col"]
    n_chip = n_row // 2
    act_spec = P("dp", "row")
    cache_spec = P(None, "dp", ("col", "row"), None, None)
    fresh_spec = P(None, "dp", ("col", "row"), None)
    in_weight = P(None, "row", "col")
    out_weight = P(None, "col", "row")
    col_vec = P(None, "col")
    row_vec = P(None, "row")
    in_specs = (act_spec, P("dp"), cache_spec, cache_spec, row_vec, row_vec,
                in_weight, col_vec, in_weight, col_vec, in_weight, col_vec,
                out_weight, row_vec, row_vec, row_vec, in_weight, col_vec, out_weight, row_vec)

    def local_step(hidden, cache_len, k_cache, v_cache, ln1_g, ln1_b, w_q, b_q, w_k, b_k, w_v, b_v,
                   w_o, b_o, ln2_g, ln2_b, w_fc1, b_fc1, w_fc2, b_fc2):
        batch, width = hidden.shape
        n_layer, _, _, keys, hd = k_cache.shape
        ff = w_fc1.shape[2]
        ffb = ff // n_row
        table, n_sem = layout()
        part = batch // HALVES
        args = (hidden, cache_len.reshape(1, batch), k_cache, v_cache, ln1_g, ln1_b, w_q, b_q, w_k, b_k, w_v, b_v,
                w_o, b_o, ln2_g, ln2_b, w_fc1, b_fc1, w_fc2, b_fc2)

        def vm(shape, dtype=BF16):
            return pltpu.VMEM(shape, dtype)

        local = [vm(a.shape, a.dtype) for a in args]
        local[2] = local[3] = vm((n_layer, batch, keys, hd))

        def half(h):
            rows = part + 16 if h == 0 else part
            gb = (n_layer, n_chip, 2 * ffb // 128, 128)
            shapes = dict(
                q_send=vm((n_layer, 2, n_row, rows, hd)), q_recv=vm((n_layer, 2, n_row, rows, hd)),
                vd_send=vm((n_layer, rows, n_chip * hd)), vd_recv=vm((n_layer, rows, n_chip * hd)),
                v_mine=vm((rows, n_chip * hd), F32),
                v_send=vm((n_layer, n_chip, rows, hd)), v_recv=vm((n_layer, n_chip, rows, hd)),
                y=vm((rows, width)), q=vm((part, hd), F32), ag=vm((n_layer, n_row, part, hd)),
                st_send=vm((n_layer, 2, 8, 128), F32), st_recv=vm((n_layer, 2, n_row, 8, 128), F32),
                wo=vm((n_layer, n_col, part, width)), fo=vm((n_layer, n_col, part, width)),
                fd_send=vm((n_layer, n_chip, rows, ffb)), fd_recv=vm((n_layer, n_chip, rows, ffb)),
                f_mine=vm((n_chip, rows, ffb), F32),
                fi_send=vm((n_layer, n_chip, part, ffb)), fi_recv=vm((n_layer, n_chip, part, ffb)),
                ug=vm((n_layer, n_row, part, ffb)), acc=vm((part, width), F32))
            if h == 0:
                shapes.update(fg_send=vm(gb, F32), fg_recv=vm(gb, F32))
            return shapes

        dma = pltpu.SemaphoreType.DMA
        scratch = [local, [half(h) for h in range(HALVES)], vm((batch, width)), vm((batch, hd, keys)),
                   [dma((12,)), dma((n_layer, 8)), dma((n_sem[0],)), dma((n_sem[1],))]]
        out_shape = (jax.ShapeDtypeStruct((batch, width), BF16),
                     jax.ShapeDtypeStruct((n_layer, batch, hd), BF16),
                     jax.ShapeDtypeStruct((n_layer, batch, hd), BF16))
        kept = pl.pallas_call(
            functools.partial(kernel, (n_layer, n_row, n_col, table)),
            out_shape=[pltpu.VMEM(o.shape, o.dtype) for o in out_shape],
            in_specs=[pl.BlockSpec(memory_space=pl.ANY)] * len(args),
            out_specs=[pl.BlockSpec(memory_space=pltpu.VMEM)] * 3,
            scratch_shapes=scratch,
            compiler_params=pltpu.CompilerParams(collective_id=0, has_side_effects=True, vmem_limit_bytes=VLIM),
        )(*args)
        h_out, k_new, v_new = pl.pallas_call(
            finish, out_shape=out_shape,
            in_specs=[pl.BlockSpec(memory_space=pltpu.VMEM)] * 3, out_specs=[pl.BlockSpec(memory_space=pl.ANY)] * 3,
            scratch_shapes=[pltpu.SemaphoreType.DMA((3,))],
        )(*[pltpu.with_memory_space_constraint(o, pltpu.VMEM) for o in kept])
        return h_out, k_new[:, :, None, :], v_new[:, :, None, :]

    return jax.shard_map(local_step, mesh=mesh, in_specs=in_specs,
                         out_specs=(act_spec, fresh_spec, fresh_spec), check_vma=False)
```
